32 devices in a mesh: base: 16 (over z, x, core), chan: 2 (over y).
Axes of the slice: x: 2, y: 2, z: 4, core: 2. Of those that a mesh axis runs over, the one named last changes fastest.
Arguments:
- image0: float32 [2048, 2048], P(('base', 'chan')), may hold values from -6 to 6
- interp: float32 [16, 2, 256, 8, 256], P('base', 'chan'), may hold values from -0.375 to 0.375
- vis_weight: float32 [16, 2, 256, 8], P('base', 'chan'), may hold values from 0.2 to 5
- counts: int32 [16, 2, 256], P('base', 'chan'), may hold values from 1 to 8
- tile_index: int32 [16, 2, 256], P('base', 'chan'), may hold values from 0 to 511
Outputs:
- image_out: float32 [2048, 2048], P(('base', 'chan'))
- estimates: float32 [3], replicated
The draws below stay inside these ranges and needn't reach their ends.
Inputs may be any that keep to these rules, and one draw needn't show every extreme that they name: `tile_index`: slot s of a device belongs to the spectrum block of device s // 8 of base+chan, base index major; the entry numbers the tile within that block. `counts`: visibility v of a slot is live when v < count.
All inputs are finite; a program needn't handle non-finite values.
Results may differ from the reference program's by a relative error of at most 0.00023.
Values sent between devices are 32-bit elements; how exact they have to be, the bound alone decides.
A program may use at most 128 MiB of HBM per device.

```python
import math
import jax
import jax.numpy as jnp
from jax import lax

N = 2048
TILE_V = 8
TILE_U = 32
VCAP = 8
TOUCH = 256
ITERS = 3
CAP = 8
TILES_OWN = 512
N_BASE = 16
N_CHAN = 2


def place_ends(values, stream_key, smallest, top_value):
    longest = values.shape.index(max(values.shape))
    spots = []
    for shift in (0, 1):
        where = [jax.random.randint(jax.random.fold_in(stream_key, axis), (), 0, length) for axis, length in enumerate(values.shape)]
        where[longest] = (where[longest] + shift) % values.shape[longest]
        spots.append(tuple(where))
    return values.at[spots[0]].set(smallest).at[spots[1]].set(top_value)


def shard_levels(stream_key, dims, shards, smallest, top_value):
    gain, own = 1.0, jax.random.fold_in(stream_key, 6)
    for dim, parts in shards:
        heights = jnp.exp(jax.random.uniform(jax.random.fold_in(own, dim), (parts,), jnp.float32, smallest / len(shards), top_value / len(shards)))
        gain = gain * jnp.repeat(heights, dims[dim] // parts).reshape([-1 if axis == dim else 1 for axis in range(len(dims))])
    return gain


def scatter_about(stream_key, extent, spread, most, cuts=(), kind=jnp.bfloat16):
    values = jax.random.normal(stream_key, extent, jnp.float32) * spread
    if len(cuts) > 0:
        values = shard_levels(stream_key, extent, cuts, -0.22, 0.18) * values
    return jnp.clip(values, min=-most, max=most).astype(kind)


def setup_inputs(seed: int = 0) -> dict:
    splits = jax.random.split(jax.random.key(seed), 6)
    image0 = scatter_about(splits[0], (N, N), 1.0, 6.0, ((0, 32),), jnp.float32)
    interp = scatter_about(splits[1], (N_BASE, N_CHAN, TOUCH, VCAP, TILE_V * TILE_U), (TILE_V * TILE_U) ** -0.5, 0.375, ((0, 16), (1, 2)), jnp.float32)
    vis_weight = jnp.clip(jnp.exp(math.log(5.0) - 3.218876 * jax.random.uniform(splits[2], (N_BASE, N_CHAN, TOUCH, VCAP), jnp.float32) ** shard_levels(splits[2], (N_BASE, N_CHAN, TOUCH, VCAP), ((0, 16), (1, 2)), -0.2, 0.2)), 0.2, 5.0)
    counts = place_ends(jax.random.randint(splits[3], (N_BASE, N_CHAN, TOUCH), 1, VCAP + 1), jax.random.fold_in(splits[3], 1), 1, VCAP).astype(jnp.int32)
    tile_index = place_ends(jax.random.randint(splits[4], (N_BASE, N_CHAN, TOUCH), 0, TILES_OWN), jax.random.fold_in(splits[4], 1), 0, TILES_OWN - 1).astype(jnp.int32)
    return {"image0": image0, "interp": interp, "vis_weight": vis_weight, "counts": counts, "tile_index": tile_index}


PRECISION_LEVEL = lax.Precision.HIGHEST

def spectrum_tiles(image):
    devices = N_BASE * N_CHAN
    spectrum = jnp.fft.fft2(image, norm='ortho')
    planes = []
    for plane in (jnp.real(spectrum), jnp.imag(spectrum)):
        held = plane.T.reshape(devices, N // devices // TILE_V, TILE_V, N // TILE_U, TILE_U)
        planes.append(held.transpose(0, 1, 3, 2, 4).reshape(devices * TILES_OWN, TILE_V * TILE_U))
    return jnp.stack(planes, axis=1)

def image_of(grid):
    devices = N_BASE * N_CHAN
    planes = []
    for member in range(2):
        held = grid[:, member, :].reshape(devices, N // devices // TILE_V, N // TILE_U, TILE_V, TILE_U)
        planes.append(held.transpose(0, 1, 3, 2, 4).reshape(N, N).T)
    spectrum = lax.complex(planes[0], planes[1])
    return jnp.real(jnp.fft.ifft2(spectrum, norm='ortho'))

def apply_normal(image, sample_weights, masked_weight, global_index):
    tiles = spectrum_tiles(image)

    def accumulate(grid, pieces):
        slot_weight_table, slot_valid_mask, slot_index = pieces
        sample_values = tiles[slot_index]
        visible_samples = jnp.einsum('gnz,gez->gen', slot_weight_table, sample_values, precision=PRECISION_LEVEL) * slot_valid_mask[:, None, :]
        gridded_plane = jnp.einsum('hbi,hyb->hyi', slot_weight_table, visible_samples, precision=PRECISION_LEVEL)
        return (grid.at[slot_index].add(gridded_plane), None)
    grid, unused = lax.scan(accumulate, jnp.zeros_like(tiles), (sample_weights, masked_weight, global_index))
    return image_of(grid)

def reference(image0, interp, vis_weight, counts, tile_index):
    devices = N_BASE * N_CHAN
    sample_weights = interp.reshape(devices, TOUCH, VCAP, TILE_V * TILE_U)
    live = (jnp.arange(VCAP, dtype=jnp.int32)[None, None, :] < counts.reshape(devices, TOUCH, 1)).astype(jnp.float32)
    masked_weight = vis_weight.reshape(devices, TOUCH, VCAP) * live
    owner = (jnp.arange(TOUCH, dtype=jnp.int32) // CAP).astype(jnp.int32)
    global_index = (owner[None, :] * TILES_OWN + tile_index.reshape(devices, TOUCH)).astype(jnp.int32)
    current = image0 / jnp.sqrt(jnp.sum(image0 * image0))
    found = []
    for iteration in range(ITERS):
        image = apply_normal(current, sample_weights, masked_weight, global_index)
        norm_value = jnp.sqrt(jnp.sum(image * image))
        found.append(norm_value)
        current = image / norm_value
    return (N * current, jnp.stack(found))
```

```python
import math

import jax
import jax.numpy as jnp
import numpy as np
from jax import lax
from jax.experimental import pallas as pl
from jax.experimental.pallas import tpu as pltpu
from jax.sharding import PartitionSpec as P

TILE_V = 8
TILE_U = 32
ITERS = 3


PRECISION_LEVEL = lax.Precision.HIGHEST


def split_length(length):
    outer_len = 2 ** ((length.bit_length() - 1) // 2)
    return (outer_len, length // outer_len)


def angle_table(count_a, count_b, modulus, sign):
    left = jnp.arange(count_a, dtype=jnp.int32)[:, None]
    right = jnp.arange(count_b, dtype=jnp.int32)[None, :]
    angle = sign * 2.0 * math.pi / modulus * (left * right % modulus).astype(jnp.float32)
    return (jnp.cos(angle), jnp.sin(angle))


def transform_rows(real_part, imag_part, sign):
    row_count, length = real_part.shape
    outer_len, inner_len = split_length(length)
    cos_q, sin_q = angle_table(inner_len, inner_len, inner_len, sign)
    cos_t, sin_t = angle_table(inner_len, outer_len, length, sign)
    cos_p, sin_p = angle_table(outer_len, outer_len, outer_len, sign)
    real_in = real_part.reshape(row_count, inner_len, outer_len)
    first_re = jnp.einsum("kq,rqp->rkp", cos_q, real_in, precision=PRECISION_LEVEL)
    first_im = jnp.einsum("kq,rqp->rkp", sin_q, real_in, precision=PRECISION_LEVEL)
    if imag_part is not None:
        imag_in = imag_part.reshape(row_count, inner_len, outer_len)
        first_re = first_re - jnp.einsum("kq,rqp->rkp", sin_q, imag_in, precision=PRECISION_LEVEL)
        first_im = first_im + jnp.einsum("kq,rqp->rkp", cos_q, imag_in, precision=PRECISION_LEVEL)
    turned_re = first_re * cos_t - first_im * sin_t
    turned_im = first_re * sin_t + first_im * cos_t
    last_re = jnp.einsum("jp,rkp->rjk", cos_p, turned_re, precision=PRECISION_LEVEL) - jnp.einsum(
        "jp,rkp->rjk", sin_p, turned_im, precision=PRECISION_LEVEL
    )
    last_im = jnp.einsum("jp,rkp->rjk", cos_p, turned_im, precision=PRECISION_LEVEL) + jnp.einsum(
        "jp,rkp->rjk", sin_p, turned_re, precision=PRECISION_LEVEL
    )
    factor = 1.0 / math.sqrt(length)
    return (
        last_re.reshape(row_count, length) * factor,
        last_im.reshape(row_count, length) * factor,
    )


def transpose_global(real_part, imag_part):
    row_count, length = real_part.shape
    n_base = lax.axis_size("base")
    n_chan = lax.axis_size("chan")
    width = length // (n_base * n_chan)
    moved = (
        lax.all_to_all(
            lax.all_to_all(
                real_part.reshape(1, row_count, n_base, n_chan, width),
                "base",
                split_axis=2,
                concat_axis=0,
                tiled=True,
            ),
            "chan",
            split_axis=3,
            concat_axis=1,
            tiled=True,
        ),
        lax.all_to_all(
            lax.all_to_all(
                imag_part.reshape(1, row_count, n_base, n_chan, width),
                "base",
                split_axis=2,
                concat_axis=0,
                tiled=True,
            ),
            "chan",
            split_axis=3,
            concat_axis=1,
            tiled=True,
        ),
    )
    return (moved[0].reshape(length, width).T, moved[1].reshape(length, width).T)


def to_tiles(plane):
    row_count, length = plane.shape
    shaped = plane.reshape(row_count // TILE_V, TILE_V, length // TILE_U, TILE_U)
    return shaped.transpose(0, 2, 1, 3).reshape(-1, TILE_V * TILE_U)


def from_tiles(tiles, row_count, length):
    shaped = tiles.reshape(row_count // TILE_V, length // TILE_U, TILE_V, TILE_U)
    return shaped.transpose(0, 2, 1, 3).reshape(row_count, length)


def slot_work(sample_weights, masked_weight, sample_values):
    visible_samples = (
        jnp.einsum("gnz,gez->gen", sample_weights, sample_values, precision=PRECISION_LEVEL)
        * masked_weight[:, None, :]
    )
    return jnp.einsum("hbi,hyb->hyi", sample_weights, visible_samples, precision=PRECISION_LEVEL)


def total_squares(image):
    return lax.psum(jnp.sum(image * image), ("base", "chan"))


def general_device(image0, interp, vis_weight, counts, tile_index):
    n_base = lax.axis_size("base")
    n_chan = lax.axis_size("chan")
    row_count, length = image0.shape
    touch = tile_index.shape[2]
    slots_each = touch // (n_base * n_chan)
    vcap = interp.shape[3]
    cells = interp.shape[4]
    tiles_own = row_count // TILE_V * (length // TILE_U)
    live = (jnp.arange(vcap, dtype=jnp.int32)[None, :] < counts.reshape(touch, 1)).astype(
        jnp.float32
    )
    masked_weight = vis_weight.reshape(touch, vcap) * live
    sample_weights = interp.reshape(touch, vcap, cells)
    wanted = lax.all_to_all(
        lax.all_to_all(
            tile_index.reshape(n_base, n_chan, slots_each),
            "base",
            split_axis=0,
            concat_axis=0,
            tiled=True,
        ),
        "chan",
        split_axis=1,
        concat_axis=1,
        tiled=True,
    ).reshape(touch)
    onehot = (jnp.arange(tiles_own, dtype=jnp.int32)[:, None] == wanted[None, :]).astype(
        jnp.float32
    )
    moved = (
        lax.all_to_all(
            lax.all_to_all(
                sample_weights.reshape(n_base, n_chan, slots_each, vcap, cells),
                "base",
                split_axis=0,
                concat_axis=0,
                tiled=True,
            ),
            "chan",
            split_axis=1,
            concat_axis=1,
            tiled=True,
        ),
        lax.all_to_all(
            lax.all_to_all(
                masked_weight.reshape(n_base, n_chan, slots_each, vcap),
                "base",
                split_axis=0,
                concat_axis=0,
                tiled=True,
            ),
            "chan",
            split_axis=1,
            concat_axis=1,
            tiled=True,
        ),
    )
    sample_weights = moved[0].reshape(touch, vcap, cells)
    masked_weight = moved[1].reshape(touch, vcap)
    found = []
    current = image0 / jnp.sqrt(total_squares(image0))
    for iteration in range(ITERS):
        real_part, imag_part = transform_rows(current, None, -1.0)
        real_part, imag_part = transpose_global(real_part, imag_part)
        real_part, imag_part = transform_rows(real_part, imag_part, -1.0)
        tiles = jnp.stack([to_tiles(real_part), to_tiles(imag_part)], axis=1)
        sample_values = jnp.take(tiles, wanted, axis=0)
        gridded_plane = slot_work(sample_weights, masked_weight, sample_values)
        summed = jnp.einsum("ts,skc->tkc", onehot, gridded_plane, precision=PRECISION_LEVEL)
        real_part = from_tiles(summed[:, 0, :], row_count, length)
        imag_part = from_tiles(summed[:, 1, :], row_count, length)
        real_part, imag_part = transform_rows(real_part, imag_part, 1.0)
        real_part, imag_part = transpose_global(real_part, imag_part)
        real_part, imag_part = transform_rows(real_part, imag_part, 1.0)
        norm_value = jnp.sqrt(total_squares(real_part))
        found.append(norm_value)
        current = real_part / norm_value
    return (float(length) * current, jnp.stack(found))


F32 = jnp.float32
BF16 = jnp.bfloat16
VMEM_SPEC = pl.BlockSpec(memory_space=pltpu.VMEM)
SMEM_SPEC = pl.BlockSpec(memory_space=pltpu.SMEM)
BIG = pltpu.CompilerParams(vmem_limit_bytes=48 * 1024 * 1024)


def halves(value):
    high = value.astype(BF16)
    return high, (value - high.astype(F32)).astype(BF16)


def np_halves(table):
    high = np.asarray(table, np.float32).astype(jnp.bfloat16)
    low = (np.asarray(table, np.float64) - high.astype(np.float64)).astype(jnp.bfloat16)
    return high, low


def triple_dot(left, right, dims):
    def one(a, b):
        return lax.dot_general(a, b, (dims, ((), ())), preferred_element_type=F32)

    return one(left[0], right[0]) + (one(left[0], right[1]) + one(left[1], right[0]))


def fft_list(items, sign):
    count = len(items)
    if count == 1:
        return items
    even = fft_list(items[0::2], sign)
    odd = fft_list(items[1::2], sign)
    low, high = [], []
    for k in range(count // 2):
        re, im = odd[k]
        if k == 0:
            t_re, t_im = re, im
        elif 4 * k == count:
            t_re, t_im = (im, -re) if sign < 0 else (-im, re)
        else:
            angle = sign * 2.0 * math.pi * k / count
            c, s = math.cos(angle), math.sin(angle)
            t_re, t_im = re * c - im * s, re * s + im * c
        e_re, e_im = even[k]
        low.append((e_re + t_re, e_im + t_im))
        high.append((e_re - t_re, e_im - t_im))
    return low + high


ANY_SPEC = pl.BlockSpec(memory_space=pl.ANY)
NT = ((1,), (1,))
NN = ((1,), (0,))


def turn(re, im, c, s):
    return re * c - im * s, re * s + im * c


def swap_halves(x0, x1):
    half = x0.shape[1] // 2
    left = lax.broadcasted_iota(jnp.int32, x0.shape, 1) < half
    return (
        jnp.where(left, x0, pltpu.roll(x1, half, 1)),
        jnp.where(left, pltpu.roll(x0, half, 1), x1),
    )


def move(table, parts, dims=NN):
    def one(part):
        return lax.dot_general(table, part, (dims, ((), ())), preferred_element_type=F32)

    return one(parts[0]) + one(parts[1])


def chip_of(p):
    z, x, core, y = p // 8, (p // 4) % 2, (p // 2) % 2, p % 2
    w = 3 * x + y - 2 * x * y
    return 4 * w + z + (w % 2) * (3 - 2 * z), core


def device_of(chip, core):
    w, at = chip // 4, chip % 4
    z = at + (w % 2) * (3 - 2 * at)
    x = w // 2
    y = w % 2 + x - 2 * x * (w % 2)
    return ((z * 2 + x) * 2 + core) * 2 + y


def turned_block(block):
    rows, lanes = block.shape

    def anti(size):
        total = lax.broadcasted_iota(jnp.int32, (size, size), 0) + lax.broadcasted_iota(
            jnp.int32, (size, size), 1
        )
        return (total == size - 1).astype(F32).astype(BF16)

    half = move(anti(rows), halves(block))
    high, low = halves(half)
    table = anti(lanes)

    def one(part):
        return jnp.dot(part, table, preferred_element_type=F32)

    return one(high) + one(low)


def lanes_of(shape):
    return lax.broadcasted_iota(jnp.int32, shape, 1)


def onto_first(low, high):
    lane = lanes_of(low.shape)
    value = jnp.where(lane % 8 > 0, pltpu.roll(high, 9, 1), pltpu.roll(low, 1, 1))
    return jnp.where(lane >= 8, value, pltpu.roll(value, 1, 0))


def onto_second(low, high):
    lane = lanes_of(low.shape)
    size = low.shape[1]
    value = jnp.where(lane % 8 < 7, pltpu.roll(low, size - 9, 1), pltpu.roll(high, size - 1, 1))
    return jnp.where(lane < size - 8, value, pltpu.roll(value, low.shape[0] - 1, 0))


def main_kernel(
    n,
    n_chan,
    held_ref,
    w_hbm,
    x_ref,
    rtc,
    rts,
    rfh,
    rfl,
    rih,
    ril,
    tc,
    ts,
    cfh,
    cfl,
    cih,
    cil,
    perm_ref,
    y_ref,
    norm_ref,
    b_ref,
    send1,
    recv1,
    send2,
    recv2,
    recv_w,
    recv_x,
    mark_send,
    mark_recv,
    wh,
    wl,
    wm,
    oh,
    oht,
    own_h,
    own_l,
    g_h,
    g_l,
    h_h,
    h_l,
    grid,
    came,
    edge_send,
    edge_last,
    u_ref,
    w_sem,
    x_sem,
    d1_sem,
    d2_sem,
    m_sem,
    core_sem,
    ring_sem,
    own_sem,
):
    base, chan = lax.axis_index("base"), lax.axis_index("chan")
    me = base * n_chan + chan
    chip, core = chip_of(me)
    chips = n // 2
    rows = 32
    partner = device_of(chip, 1 - core)
    around = device_of((chip + chips + 2 * core - 1) % chips, 1 - core)
    first_edge = jnp.logical_and(core == 0, chip == 0)
    last_edge = jnp.logical_and(core == 1, chip == chips - 1)

    def place(p):
        return (p // n_chan, p % n_chan)

    def remote(src, dst, sems, out_index, in_index, peer):
        return pltpu.make_async_remote_copy(
            src_ref=src,
            dst_ref=dst,
            send_sem=sems.at[out_index],
            recv_sem=sems.at[in_index],
            device_id=place(peer),
            device_id_type=pl.DeviceIdType.MESH,
        )

    def block_of(p):
        its_chip, its_core = chip_of(p)
        return its_chip + its_core * (n - 1 - 2 * its_chip)

    def weights_to(p, arrives):
        return remote(w_hbm.at[block_of(p)], recv_w.at[arrives], w_sem, (0, p), (1, arrives), p)

    def extras_to(p, arrives):
        return remote(x_ref.at[block_of(p)], recv_x.at[arrives], x_sem, (0, p), (1, arrives), p)

    def first_to(p, arrives):
        its_chip, its_core = chip_of(p)
        return remote(
            send1.at[its_chip * 2 + its_core], recv1.at[arrives], d1_sem, (0, p), (1, arrives), p
        )

    def second_to(p, arrives):
        its_chip, its_core = chip_of(arrives)
        return remote(
            send2.at[p], recv2.at[its_chip * 2 + its_core], d2_sem, (0, p), (1, arrives), p
        )

    def mark_to(k):
        return lambda p, arrives: remote(
            mark_send.at[k], mark_recv.at[k, arrives], m_sem, (k, 0, p), (k, 1, arrives), p
        )

    def start_all(make, low=1, high=n):
        def body(step, carry):
            make((me + step) % n, me).start()
            return carry

        lax.fori_loop(low, high, body, 0)

    def sent_all(make):
        def body(step, carry):
            make((me + step) % n, me).wait_send()
            return carry

        lax.fori_loop(1, n, body, 0)

    def came_all(make, low=1, high=n):
        def body(step, carry):
            p = (me + step) % n
            make(p, p).wait_recv()
            return carry

        lax.fori_loop(low, high, body, 0)

    def put_mark(k, total):
        mark_send[k] = jnp.full((1, 128), total, F32)
        mark_recv[k, me] = jnp.full((1, 128), total, F32)
        start_all(mark_to(k))

    def get_mark(k):
        came_all(mark_to(k))
        total = mark_recv[k, 0]
        for d in range(1, n):
            total = total + mark_recv[k, d]
        return jnp.sqrt(total)

    own_w = pltpu.make_async_copy(w_hbm.at[block_of(me)], recv_w.at[me], own_sem.at[0])
    own_w.start()
    start_all(extras_to)
    recv_x[me] = x_ref[block_of(me)]
    start_all(weights_to, 1, 4)

    total = jnp.zeros((8, 128), F32)
    for at in range(0, held_ref.shape[1], 512):
        part = held_ref[:, at : at + 512]
        square = part * part
        b_ref[:, at : at + 512] = triple_dot((rfh[...], rfl[...]), halves(part), NN)
        for lane in range(0, 512, 128):
            for row in range(0, 64, 8):
                total = total + square[row : row + 8, lane : lane + 128]
    put_mark(0, jnp.sum(total))

    def row_chunk(i, carry):
        at = pl.multiple_of(i * 8, 8)
        items = [[None, None] for _ in range(n)]
        for pair in range(n // 2):
            lanes = slice(pair * 128, (pair + 1) * 128)
            for part in range(2):
                x0 = b_ref[pl.ds(at + part * 64, 8), lanes]
                x1 = b_ref[pl.ds(at + part * 64 + rows, 8), lanes]
                items[2 * pair][part], items[2 * pair + 1][part] = swap_halves(x0, x1)
        items = [
            turn(*items[q], tc_q, ts_q)
            for q, (tc_q, ts_q) in enumerate(
                (rtc[q, pl.ds(at, 8), :], rts[q, pl.ds(at, 8), :]) for q in range(n)
            )
        ]
        items = fft_list(items, -1.0)
        row = lax.broadcasted_iota(jnp.int32, (8, 128), 0) + at
        lane = lanes_of((8, 128))
        alone = jnp.logical_and(row == 0, lane < 64)
        items[0] = (items[0][0], jnp.where(alone, items[n // 2][0], items[0][1]))
        its_core = i // 2
        to = pl.multiple_of((i % 2) * 8, 8)
        for o in range(n // 2):
            send1[o * 2 + its_core, pl.ds(to, 8), :] = items[o][0]
            send1[o * 2 + its_core, pl.ds(to + 16, 8), :] = items[o][1]
        return carry

    lax.fori_loop(0, 4, row_chunk, 0)
    recv1[me] = send1[chip * 2 + core]
    start_all(first_to)
    start_all(weights_to, 4, n)

    came_all(extras_to)
    numbers = recv_x[0, :, 256:]
    for d in range(1, n):
        numbers = numbers + recv_x[d, :, 256:]
    numbers = jnp.where(core == 0, numbers, 511.0 - numbers)
    for g in range(8):
        wm[g] = (
            recv_x[4 * g, :, :256]
            + recv_x[4 * g + 1, :, :256]
            + recv_x[4 * g + 2, :, :256]
            + recv_x[4 * g + 3, :, :256]
        )
    wide = jnp.broadcast_to(numbers, (256, 256))
    tall = wide.T
    for at in range(0, 512, 256):
        down = (lax.broadcasted_iota(jnp.int32, (256, 256), 0) + at).astype(F32)
        along = (lanes_of((256, 256)) + at).astype(F32)
        oht[at : at + 256, :] = (wide == down).astype(F32).astype(BF16)
        oh[:, at : at + 256] = (tall == along).astype(F32).astype(BF16)

    came_all(first_to)
    inverse = 1.0 / get_mark(0)

    def block(i, half):
        return 2 * core + i + 4 * half

    def forward(i, carry):
        at = pl.multiple_of(i * 8, 8)
        items = fft_list(
            [
                (
                    recv1[d, pl.ds(at, 8), :] * inverse,
                    recv1[d, pl.ds(at + 16, 8), :] * inverse,
                )
                for d in range(n)
            ],
            -1.0,
        )
        for k in range(n):
            re, im = turn(*items[k], tc[k : k + 1, :], ts[k : k + 1, :])
            u_ref[k * 8 : k * 8 + 8, :128] = re
            u_ref[k * 8 : k * 8 + 8, 128:] = im
        out = triple_dot((cfh[...], cfl[...]), halves(u_ref[...]), NT)
        for part in range(2):
            for half in range(2):
                start = part * 128 + half * 64
                came[0, part, block(i, half)] = out[start : start + 64]
        return carry

    lax.fori_loop(0, 2, forward, 0)

    def raised(block_before):
        return onto_first(block_before, block_before)

    @pl.when(first_edge)
    def _():
        z_re, z_im = came[0, 0, 0], came[0, 1, 0]
        f_re = raised(turned_block(z_re))
        f_im = -raised(turned_block(z_im))
        first = lanes_of(z_re.shape) % 8 == 0
        came[0, 0, 0] = jnp.where(first, 0.5 * (z_re + f_re), z_re)
        came[0, 1, 0] = jnp.where(first, 0.5 * (z_im + f_im), z_im)
        edge_send[0] = 0.5 * (z_im - f_im)
        edge_send[1] = -0.5 * (z_re - f_re)

    @pl.when(jnp.logical_and(core == 0, chip > 0))
    def _():
        edge_send[0] = came[0, 0, 0]
        edge_send[1] = came[0, 1, 0]

    def half_copy(half, its_core, peer):
        at = pl.ds(2 * its_core + 4 * half, 2)
        return remote(
            came.at[0, :, at], came.at[0, :, at], core_sem, (0, half, 0), (0, half, 1), peer
        )

    for half in range(2):
        half_copy(half, core, partner).start()

    edge_copy = remote(edge_send, came.at[0, :, 8], ring_sem, (0, 0), (0, 1), around)

    @pl.when(core == 0)
    def _():
        edge_copy.start()

    def make_ready(g, carry):
        def one(j, carry):
            d = 4 * g + j

            @pl.when(d != me)
            def _():
                weights_to(d, d).wait_recv()

            @pl.when(d == me)
            def _():
                own_w.wait()

            return carry

        lax.fori_loop(0, 4, one, 0)
        value = recv_w[pl.ds(4 * g, 4)].reshape(256, 256)
        for part, ref in zip(halves(value), (wh, wl)):
            ref[g] = jnp.dot(part, perm_ref[core], preferred_element_type=F32).astype(BF16)
        return carry

    lax.fori_loop(0, 8, make_ready, 0)

    def keep(a, part, value):
        high, low = halves(value)
        at = pl.ds(pl.multiple_of(a * 64, 64), 64)
        own_h[part, at, :] = high
        own_l[part, at, :] = low

    for half in range(2):
        half_copy(half, 1 - core, partner).wait_recv()

    @pl.when(core == 0)
    def _():
        def one(a, carry):
            for part in range(2):
                keep(a, part, came[0, part, a])
            return carry

        lax.fori_loop(0, 8, one, 0)

    @pl.when(core == 1)
    def _():
        edge_copy.wait_recv()

        def one(a, carry):
            for part in range(2):
                keep(a, part, onto_second(came[0, part, a], came[0, part, a + 1]))
            return carry

        lax.fori_loop(0, 8, one, 0)

    row_of = lax.broadcasted_iota(jnp.int32, (64, 256), 0) % 32
    slot_of = lanes_of((64, 256)) // 8

    def partner_copy(k, its_core, peer):
        return remote(
            grid.at[k], came.at[k + 1, :, pl.ds(its_core, 8)], core_sem, (k + 1, 0, 0), (k + 1, 0, 1), peer
        )

    def ring_copy(k, its_core, peer):
        return remote(
            grid.at[k, :, 7 * its_core],
            came.at[k + 1, :, 8 * (1 - its_core)],
            ring_sem,
            (k + 1, 0),
            (k + 1, 1),
            peer,
        )

    def apply(k):
        for part in range(2):
            for own, out in ((own_h, g_h), (own_l, g_l)):
                out[part] = jnp.dot(
                    oh[...], own[part], preferred_element_type=F32
                ).astype(BF16).reshape(8, 32, 256)

        def group(g, carry):
            left = tuple(
                jnp.concatenate([ref[0, g], ref[1, g]], axis=0) for ref in (g_h, g_l)
            )
            weights = (wh[g], wl[g])
            seen = triple_dot(left, weights, NT)
            seen = jnp.where(row_of == slot_of, seen * wm[g], 0.0)
            high, low = halves(triple_dot(halves(seen), weights, NN))
            for ref, value in ((h_h, high), (h_l, low)):
                ref[0, g] = value[:32]
                ref[1, g] = value[32:]
            return carry

        lax.fori_loop(0, 8, group, 0)
        for part in range(2):
            grid[k, part] = move(
                oht[...], (h_h[part].reshape(256, 256), h_l[part].reshape(256, 256))
            ).reshape(8, 64, 256)
        partner_copy(k, core, partner).start()
        ring_copy(k, core, around).start()
        partner_copy(k, 1 - core, partner).wait_recv()
        ring_copy(k, 1 - core, around).wait_recv()

    def close_edge(k):
        @pl.when(jnp.logical_or(first_edge, last_edge))
        def _():
            came[k + 1, 0, 8 * core] = turned_block(grid[k, 0, 7 * core])
            came[k + 1, 1, 8 * core] = -turned_block(grid[k, 1, 7 * core])

    def iteration(k, scale):
        apply(k)
        close_edge(k)
        total = jnp.zeros((64, 256), F32)

        def combine(onto):
            def one(a, total):
                for part in range(2):
                    value = grid[k, part, a] + onto(came[k + 1, part, a], came[k + 1, part, a + 1])
                    value = value * scale
                    keep(a, part, value)
                    total = total + value * value
                return total

            return lax.fori_loop(0, 8, one, total)

        total = lax.cond(core == 0, lambda: combine(onto_first), lambda: combine(onto_second))
        put_mark(k + 1, jnp.sum(total))

    half_scale = jnp.full((1, 256), 0.5, F32)

    def two_lanes(value):
        return jnp.concatenate([value, value], axis=1)

    iteration(0, half_scale)
    n1 = [None]

    def second():
        apply(1)
        close_edge(1)
        norm = two_lanes(get_mark(1))
        n1[0] = norm
        scale = 0.5 / norm
        total = jnp.zeros((64, 256), F32)

        def combine(onto):
            def one(a, total):
                for part in range(2):
                    value = grid[1, part, a] + onto(came[2, part, a], came[2, part, a + 1])
                    value = value * scale
                    keep(a, part, value)
                    total = total + value * value
                return total

            return lax.fori_loop(0, 8, one, total)

        total = lax.cond(core == 0, lambda: combine(onto_first), lambda: combine(onto_second))
        put_mark(2, jnp.sum(total))

    second()
    apply(2)
    n2 = two_lanes(get_mark(2))
    scale = 1.0 / n2


    @pl.when(first_edge)
    def _():
        up = raised(came[3, 0, 0]), raised(came[3, 1, 0])
        edge_last[0] = up[0] + raised(turned_block(up[0]))
        edge_last[1] = up[1] - raised(turned_block(up[1]))

    @pl.when(first_edge)
    def _():
        came[3, 0, 0] = turned_block(grid[2, 0, 0])
        came[3, 1, 0] = -turned_block(grid[2, 1, 0])

    def last_sum(j, total):
        a = 2 * core + j % 2 + 4 * (j // 2)

        @pl.when(core == 0)
        def _():
            for part in range(2):
                value = grid[2, part, a] + onto_first(came[3, part, a], came[3, part, a + 1])
                grid[0, part, a] = value * scale

        @pl.when(core == 1)
        def _():
            for part in range(2):
                value = came[3, part, a] + onto_first(grid[2, part, a - 1], grid[2, part, a])
                grid[0, part, a] = value * scale

        for part in range(2):
            value = grid[0, part, a]
            total = total + value * value
        return total

    partner_copy(0, core, partner).wait_send()
    ring_copy(0, core, around).wait_send()
    total = 0.5 * lax.fori_loop(0, 4, last_sum, jnp.zeros((64, 256), F32))
    mark_total = jnp.sum(total)
    h0_re, h0_im = grid[0, 0, 0], grid[0, 1, 0]
    alone = jnp.logical_and(lanes_of((64, 256)) % 8 == 0, first_edge)
    z_re = jnp.where(alone, 0.5 * (h0_re - edge_last[1] * scale), h0_re)
    z_im = jnp.where(alone, 0.5 * (h0_im + edge_last[0] * scale), h0_im)

    @pl.when(first_edge)
    def _():
        grid[0, 0, 0] = z_re
        grid[0, 1, 0] = z_im

    change = z_re * z_re + z_im * z_im - 0.5 * (h0_re * h0_re + h0_im * h0_im)
    put_mark(3, mark_total + jnp.sum(jnp.where(alone, change, 0.0)))

    def backward(i, carry):
        at = pl.multiple_of(i * 8, 8)
        held = jnp.concatenate(
            [grid[0, part, block(i, half)] for part in range(2) for half in range(2)], axis=0
        )
        u_ref[...] = triple_dot(halves(held.T), (cih[...], cil[...]), NN)
        items = []
        for k in range(n):
            re = u_ref[k * 8 : k * 8 + 8, :128]
            im = u_ref[k * 8 : k * 8 + 8, 128:]
            items.append(turn(re, im, tc[k : k + 1, :], -ts[k : k + 1, :]))
        items = fft_list(items, 1.0)
        for d in range(n):
            send2[d, pl.ds(at, 8), :] = items[d][0]
            send2[d, pl.ds(at + 16, 8), :] = items[d][1]
        return carry

    lax.fori_loop(0, 2, backward, 0)
    recv2[chip * 2 + core] = send2[me]
    start_all(second_to)
    came_all(second_to)

    def back_chunk(i, carry):
        at = pl.multiple_of(i * 8, 8)
        its_core = i // 2
        to = pl.multiple_of((i % 2) * 8, 8)
        items = [
            (recv2[o * 2 + its_core, pl.ds(to, 8), :], recv2[o * 2 + its_core, pl.ds(to + 16, 8), :])
            for o in range(n // 2)
        ]
        row = lax.broadcasted_iota(jnp.int32, (8, 128), 0) + at
        lane = lanes_of((8, 128))
        extra = jnp.where(jnp.logical_and(row == 0, lane < 64), items[0][1], 0.0)
        even = fft_list(items, 1.0)
        odd = []
        for o, (re, im) in enumerate(items):
            angle = 2.0 * math.pi * o / n
            odd.append((re, im) if o == 0 else turn(re, im, math.cos(angle), math.sin(angle)))
        odd = fft_list(odd, 1.0)
        items = []
        for k in range(n // 2):
            items.append((even[k][0] + extra, even[k][1]))
            items.append((odd[k][0] - extra, odd[k][1]))
        items = [
            turn(*items[q], rtc[q, pl.ds(at, 8), :], -rts[q, pl.ds(at, 8), :]) for q in range(n)
        ]
        for pair in range(n // 2):
            lanes = slice(pair * 128, (pair + 1) * 128)
            for part in range(2):
                x0, x1 = swap_halves(items[2 * pair][part], items[2 * pair + 1][part])
                b_ref[pl.ds(at + part * 64, 8), lanes] = x0
                b_ref[pl.ds(at + part * 64 + rows, 8), lanes] = x1
        return carry

    lax.fori_loop(0, 4, back_chunk, 0)
    n3 = get_mark(3)
    factor = float(held_ref.shape[1]) / n3
    factor = jnp.concatenate([factor] * 4, axis=1)
    for at in range(0, held_ref.shape[1], 512):
        part = triple_dot((rih[...], ril[...]), halves(b_ref[:, at : at + 512]), NN)
        y_ref[:, at : at + 512] = part * factor
    norm_ref[0:1, :] = n1[0][:, :128]
    norm_ref[1:2, :] = n2[:, :128]
    norm_ref[2:3, :] = n3

    sent_all(extras_to)
    sent_all(weights_to)
    sent_all(first_to)
    sent_all(second_to)
    for k in range(4):
        sent_all(mark_to(k))
    for half in range(2):
        half_copy(half, core, partner).wait_send()

    @pl.when(core == 0)
    def _():
        edge_copy.wait_send()

    for k in (1, 2):
        partner_copy(k, core, partner).wait_send()
        ring_copy(k, core, around).wait_send()


def tables(n, row_count, length):
    half = row_count // 2
    scale = 1.0 / math.sqrt(length)
    local = np.arange(row_count)
    angle = -2.0 * np.pi * np.outer(local, local) / row_count
    c, s = np.cos(angle) * scale, np.sin(angle) * scale
    two = np.eye(2)
    col_f = np.block([[np.kron(two, c), np.kron(two, -s)], [np.kron(two, s), np.kron(two, c)]])
    col_i = col_f
    row_f = np.concatenate([c, s], axis=0)
    row_i = np.concatenate([c, s], axis=1)
    index = np.arange(n)
    turns = -2.0 * np.pi * np.outer(index, np.tile(local, 2)) / length
    u = np.arange(half)[:, None] + half * (np.arange(2 * row_count)[None, :] // row_count)
    row_turns = -2.0 * np.pi * index[:, None, None] * u[None] / length
    return col_f, col_i, row_f, row_i, turns, row_turns


def fast_device(image0, interp, vis_weight, counts, tile_index):
    n_chan = lax.axis_size("chan")
    n = lax.axis_size("base") * n_chan
    me = lax.axis_index("base") * n_chan + lax.axis_index("chan")
    row_count, length = image0.shape
    touch = tile_index.shape[2]
    each = touch // n
    vcap, cells = interp.shape[3:]
    col_f, col_i, row_f, row_i, turns, row_turns = tables(n, row_count, length)
    cfh, cfl = np_halves(col_f)
    cih, cil = np_halves(col_i)
    rfh, rfl = np_halves(row_f)
    rih, ril = np_halves(row_i)
    tc, ts = np.cos(turns).astype(np.float32), np.sin(turns).astype(np.float32)
    rtc = np.cos(row_turns).astype(np.float32)
    rts = np.sin(row_turns).astype(np.float32)
    order = np.arange(cells).reshape(TILE_V, TILE_U).T.reshape(-1)
    perm = np.zeros((2, cells, cells), np.float32)
    perm[0, order, np.arange(cells)] = 1.0
    perm[1] = perm[0][:, ::-1]
    perm = perm.astype(jnp.bfloat16)

    live = (jnp.arange(vcap, dtype=jnp.int32)[None, :] < counts.reshape(touch, 1)).astype(F32)
    masked = (vis_weight.reshape(touch, vcap) * live).reshape(n, each * vcap)
    numbers = tile_index.reshape(n, each).astype(F32)
    lane = jnp.arange(cells, dtype=jnp.int32)[None, :]
    spread = cells // (each * vcap)
    masked = jnp.where(lane // (each * vcap) == me % spread, jnp.tile(masked, (1, spread)), 0.0)
    numbers = jnp.where(lane // each == me, jnp.tile(numbers, (1, cells // each)), 0.0)
    extras = jnp.concatenate([masked, numbers], axis=1).reshape(n, 1, 2 * cells)
    matrices = interp.reshape(n, each * vcap, cells)
    held = image0.reshape(row_count, length // n, n).transpose(1, 2, 0).reshape(length // n, -1)

    def dma(*shape):
        return pltpu.SemaphoreType.DMA(shape)

    message = (n, 32, 128)
    wide = (8, 64, 256)
    held, norms = pl.pallas_call(
        lambda *refs: main_kernel(n, n_chan, *refs),
        out_shape=[
            jax.ShapeDtypeStruct((length // n, n * row_count), F32),
            jax.ShapeDtypeStruct((8, 128), F32),
        ],
        in_specs=[VMEM_SPEC, ANY_SPEC] + [VMEM_SPEC] * 14,
        out_specs=[VMEM_SPEC] * 2,
        scratch_shapes=[
            pltpu.VMEM((2 * row_count, length), F32),
            pltpu.VMEM(message, F32),
            pltpu.VMEM(message, F32),
            pltpu.VMEM(message, F32),
            pltpu.VMEM(message, F32),
            pltpu.VMEM((n, each * vcap, cells), F32),
            pltpu.VMEM((n, 1, 2 * cells), F32),
            pltpu.VMEM((4, 1, 128), F32),
            pltpu.VMEM((4, n, 1, 128), F32),
            pltpu.VMEM((8, cells, cells), BF16),
            pltpu.VMEM((8, cells, cells), BF16),
            pltpu.VMEM((8, 1, cells), F32),
            pltpu.VMEM((touch, 512), BF16),
            pltpu.VMEM((512, touch), BF16),
            pltpu.VMEM((2, 512, cells), BF16),
            pltpu.VMEM((2, 512, cells), BF16),
            pltpu.VMEM((2, 8, 32, cells), BF16),
            pltpu.VMEM((2, 8, 32, cells), BF16),
            pltpu.VMEM((2, 8, 32, cells), BF16),
            pltpu.VMEM((2, 8, 32, cells), BF16),
            pltpu.VMEM((3, 2, 8, 64, cells), F32),
            pltpu.VMEM((4, 2, 9, 64, cells), F32),
            pltpu.VMEM((2, 64, cells), F32),
            pltpu.VMEM((2, 64, cells), F32),
            pltpu.VMEM((256, 256), F32),
            dma(2, n),
            dma(2, n),
            dma(2, n),
            dma(2, n),
            dma(4, 2, n),
            dma(4, 2, 2),
            dma(4, 2),
            dma(1),
        ],
        compiler_params=pltpu.CompilerParams(
            has_side_effects=True, vmem_limit_bytes=48 * 1024 * 1024
        ),
    )(held, matrices, extras, rtc, rts, rfh, rfl, rih, ril, tc, ts, cfh, cfl, cih, cil, perm)
    image = held.reshape(length // n, n, row_count).transpose(2, 0, 1).reshape(row_count, length)
    return image, norms[:3, 0]


def per_device(image0, interp, vis_weight, counts, tile_index):
    n = lax.axis_size("base") * lax.axis_size("chan")
    row_count, length = image0.shape
    vcap, cells = interp.shape[3:]
    touch = tile_index.shape[2]
    fits = (n, row_count, length // row_count) == (TILE_U, 64, TILE_U)
    if fits and (vcap, cells, touch % 256) == (8, 256, 0) and touch // n == 8:
        return fast_device(image0, interp, vis_weight, counts, tile_index)
    return general_device(image0, interp, vis_weight, counts, tile_index)


def solution(mesh):
    placed = (
        P(("base", "chan"), None),
        P("base", "chan", None, None, None),
        P("base", "chan", None, None),
        P("base", "chan", None),
        P("base", "chan", None),
    )
    return jax.shard_map(
        per_device,
        mesh=mesh,
        in_specs=placed,
        out_specs=(P(("base", "chan"), None), P()),
        check_vma=False,
    )
```

```python
import math

import jax
import jax.numpy as jnp
import numpy as np
from jax import lax
from jax.experimental import pallas as pl
from jax.experimental.pallas import tpu as pltpu
from jax.sharding import PartitionSpec as P

TILE_V = 8
TILE_U = 32
ITERS = 3


PRECISION_LEVEL = lax.Precision.HIGHEST


def split_length(length):
    outer_len = 2 ** ((length.bit_length() - 1) // 2)
    return (outer_len, length // outer_len)


def angle_table(count_a, count_b, modulus, sign):
    left = jnp.arange(count_a, dtype=jnp.int32)[:, None]
    right = jnp.arange(count_b, dtype=jnp.int32)[None, :]
    angle = sign * 2.0 * math.pi / modulus * (left * right % modulus).astype(jnp.float32)
    return (jnp.cos(angle), jnp.sin(angle))


def transform_rows(real_part, imag_part, sign):
    row_count, length = real_part.shape
    outer_len, inner_len = split_length(length)
    cos_q, sin_q = angle_table(inner_len, inner_len, inner_len, sign)
    cos_t, sin_t = angle_table(inner_len, outer_len, length, sign)
    cos_p, sin_p = angle_table(outer_len, outer_len, outer_len, sign)
    real_in = real_part.reshape(row_count, inner_len, outer_len)
    first_re = jnp.einsum("kq,rqp->rkp", cos_q, real_in, precision=PRECISION_LEVEL)
    first_im = jnp.einsum("kq,rqp->rkp", sin_q, real_in, precision=PRECISION_LEVEL)
    if imag_part is not None:
        imag_in = imag_part.reshape(row_count, inner_len, outer_len)
        first_re = first_re - jnp.einsum("kq,rqp->rkp", sin_q, imag_in, precision=PRECISION_LEVEL)
        first_im = first_im + jnp.einsum("kq,rqp->rkp", cos_q, imag_in, precision=PRECISION_LEVEL)
    turned_re = first_re * cos_t - first_im * sin_t
    turned_im = first_re * sin_t + first_im * cos_t
    last_re = jnp.einsum("jp,rkp->rjk", cos_p, turned_re, precision=PRECISION_LEVEL) - jnp.einsum(
        "jp,rkp->rjk", sin_p, turned_im, precision=PRECISION_LEVEL
    )
    last_im = jnp.einsum("jp,rkp->rjk", cos_p, turned_im, precision=PRECISION_LEVEL) + jnp.einsum(
        "jp,rkp->rjk", sin_p, turned_re, precision=PRECISION_LEVEL
    )
    factor = 1.0 / math.sqrt(length)
    return (
        last_re.reshape(row_count, length) * factor,
        last_im.reshape(row_count, length) * factor,
    )


def transpose_global(real_part, imag_part):
    row_count, length = real_part.shape
    n_base = lax.axis_size("base")
    n_chan = lax.axis_size("chan")
    width = length // (n_base * n_chan)
    moved = (
        lax.all_to_all(
            lax.all_to_all(
                real_part.reshape(1, row_count, n_base, n_chan, width),
                "base",
                split_axis=2,
                concat_axis=0,
                tiled=True,
            ),
            "chan",
            split_axis=3,
            concat_axis=1,
            tiled=True,
        ),
        lax.all_to_all(
            lax.all_to_all(
                imag_part.reshape(1, row_count, n_base, n_chan, width),
                "base",
                split_axis=2,
                concat_axis=0,
                tiled=True,
            ),
            "chan",
            split_axis=3,
            concat_axis=1,
            tiled=True,
        ),
    )
    return (moved[0].reshape(length, width).T, moved[1].reshape(length, width).T)


def to_tiles(plane):
    row_count, length = plane.shape
    shaped = plane.reshape(row_count // TILE_V, TILE_V, length // TILE_U, TILE_U)
    return shaped.transpose(0, 2, 1, 3).reshape(-1, TILE_V * TILE_U)


def from_tiles(tiles, row_count, length):
    shaped = tiles.reshape(row_count // TILE_V, length // TILE_U, TILE_V, TILE_U)
    return shaped.transpose(0, 2, 1, 3).reshape(row_count, length)


def slot_work(sample_weights, masked_weight, sample_values):
    visible_samples = (
        jnp.einsum("gnz,gez->gen", sample_weights, sample_values, precision=PRECISION_LEVEL)
        * masked_weight[:, None, :]
    )
    return jnp.einsum("hbi,hyb->hyi", sample_weights, visible_samples, precision=PRECISION_LEVEL)


def total_squares(image):
    return lax.psum(jnp.sum(image * image), ("base", "chan"))


def general_device(image0, interp, vis_weight, counts, tile_index):
    n_base = lax.axis_size("base")
    n_chan = lax.axis_size("chan")
    row_count, length = image0.shape
    touch = tile_index.shape[2]
    slots_each = touch // (n_base * n_chan)
    vcap = interp.shape[3]
    cells = interp.shape[4]
    tiles_own = row_count // TILE_V * (length // TILE_U)
    live = (jnp.arange(vcap, dtype=jnp.int32)[None, :] < counts.reshape(touch, 1)).astype(
        jnp.float32
    )
    masked_weight = vis_weight.reshape(touch, vcap) * live
    sample_weights = interp.reshape(touch, vcap, cells)
    wanted = lax.all_to_all(
        lax.all_to_all(
            tile_index.reshape(n_base, n_chan, slots_each),
            "base",
            split_axis=0,
            concat_axis=0,
            tiled=True,
        ),
        "chan",
        split_axis=1,
        concat_axis=1,
        tiled=True,
    ).reshape(touch)
    onehot = (jnp.arange(tiles_own, dtype=jnp.int32)[:, None] == wanted[None, :]).astype(
        jnp.float32
    )
    moved = (
        lax.all_to_all(
            lax.all_to_all(
                sample_weights.reshape(n_base, n_chan, slots_each, vcap, cells),
                "base",
                split_axis=0,
                concat_axis=0,
                tiled=True,
            ),
            "chan",
            split_axis=1,
            concat_axis=1,
            tiled=True,
        ),
        lax.all_to_all(
            lax.all_to_all(
                masked_weight.reshape(n_base, n_chan, slots_each, vcap),
                "base",
                split_axis=0,
                concat_axis=0,
                tiled=True,
            ),
            "chan",
            split_axis=1,
            concat_axis=1,
            tiled=True,
        ),
    )
    sample_weights = moved[0].reshape(touch, vcap, cells)
    masked_weight = moved[1].reshape(touch, vcap)
    found = []
    current = image0 / jnp.sqrt(total_squares(image0))
    for iteration in range(ITERS):
        real_part, imag_part = transform_rows(current, None, -1.0)
        real_part, imag_part = transpose_global(real_part, imag_part)
        real_part, imag_part = transform_rows(real_part, imag_part, -1.0)
        tiles = jnp.stack([to_tiles(real_part), to_tiles(imag_part)], axis=1)
        sample_values = jnp.take(tiles, wanted, axis=0)
        gridded_plane = slot_work(sample_weights, masked_weight, sample_values)
        summed = jnp.einsum("ts,skc->tkc", onehot, gridded_plane, precision=PRECISION_LEVEL)
        real_part = from_tiles(summed[:, 0, :], row_count, length)
        imag_part = from_tiles(summed[:, 1, :], row_count, length)
        real_part, imag_part = transform_rows(real_part, imag_part, 1.0)
        real_part, imag_part = transpose_global(real_part, imag_part)
        real_part, imag_part = transform_rows(real_part, imag_part, 1.0)
        norm_value = jnp.sqrt(total_squares(real_part))
        found.append(norm_value)
        current = real_part / norm_value
    return (float(length) * current, jnp.stack(found))


F32 = jnp.float32
BF16 = jnp.bfloat16
VMEM_SPEC = pl.BlockSpec(memory_space=pltpu.VMEM)
SMEM_SPEC = pl.BlockSpec(memory_space=pltpu.SMEM)
BIG = pltpu.CompilerParams(vmem_limit_bytes=48 * 1024 * 1024)


def halves(value):
    high = value.astype(BF16)
    return high, (value - high.astype(F32)).astype(BF16)


def np_halves(table):
    high = np.asarray(table, np.float32).astype(jnp.bfloat16)
    low = (np.asarray(table, np.float64) - high.astype(np.float64)).astype(jnp.bfloat16)
    return high, low


def triple_dot(left, right, dims):
    def one(a, b):
        return lax.dot_general(a, b, (dims, ((), ())), preferred_element_type=F32)

    return one(left[0], right[0]) + (one(left[0], right[1]) + one(left[1], right[0]))


def fft_list(items, sign):
    count = len(items)
    if count == 1:
        return items
    even = fft_list(items[0::2], sign)
    odd = fft_list(items[1::2], sign)
    low, high = [], []
    for k in range(count // 2):
        re, im = odd[k]
        if k == 0:
            t_re, t_im = re, im
        elif 4 * k == count:
            t_re, t_im = (im, -re) if sign < 0 else (-im, re)
        else:
            angle = sign * 2.0 * math.pi * k / count
            c, s = math.cos(angle), math.sin(angle)
            t_re, t_im = re * c - im * s, re * s + im * c
        e_re, e_im = even[k]
        low.append((e_re + t_re, e_im + t_im))
        high.append((e_re - t_re, e_im - t_im))
    return low + high


HBM_SPEC = pl.BlockSpec(memory_space=pltpu.HBM)
NT = ((1,), (1,))
NN = ((1,), (0,))


def turn(re, im, c, s):
    return re * c - im * s, re * s + im * c


def swap_halves(x0, x1):
    half = x0.shape[1] // 2
    left = lax.broadcasted_iota(jnp.int32, x0.shape, 1) < half
    return (
        jnp.where(left, x0, pltpu.roll(x1, half, 1)),
        jnp.where(left, pltpu.roll(x0, half, 1), x1),
    )


def move(table, parts, dims=NN):
    def one(part):
        return lax.dot_general(table, part, (dims, ((), ())), preferred_element_type=F32)

    return one(parts[0]) + one(parts[1])


def bit_of(p, bit):
    return lax.rem(lax.div(p, 2**bit), 2)


def walk(z, w):
    odd = lax.rem(w, 2)
    return 4 * w + z + odd * (3 - 2 * z)


def chip_of(p):
    x, y = bit_of(p, 2), bit_of(p, 0)
    return walk(lax.div(p, 8), 3 * x + y - 2 * x * y), bit_of(p, 1)


def device_of(chip, core):
    w, at = lax.div(chip, 4), lax.rem(chip, 4)
    odd = lax.rem(w, 2)
    z = at + odd * (3 - 2 * at)
    x = lax.div(w, 2)
    y = odd + x - 2 * x * odd
    return ((z * 2 + x) * 2 + core) * 2 + y


def crossed(p, step, bits):
    value = p + step
    for bit in range(bits):
        value = value - 2 ** (bit + 1) * bit_of(p, bit) * bit_of(step, bit)
    return value


def turned_block(block):
    rows, lanes = block.shape

    def anti(size):
        total = lax.broadcasted_iota(jnp.int32, (size, size), 0) + lax.broadcasted_iota(
            jnp.int32, (size, size), 1
        )
        return (total == size - 1).astype(F32).astype(BF16)

    half = move(anti(rows), halves(block))
    high, low = halves(half)
    table = anti(lanes)

    def one(part):
        return jnp.dot(part, table, preferred_element_type=F32)

    return one(high) + one(low)


def lanes_of(shape):
    return lax.broadcasted_iota(jnp.int32, shape, 1)


def onto_first(low, high):
    lane = lanes_of((low.shape[0], 128))
    column = lane & 7
    high = [pltpu.roll(high[:, at : at + 128], 9, 1) for at in (0, 128)]
    low = [pltpu.roll(low[:, at : at + 128], 1, 1) for at in (0, 128)]
    left = jnp.where(
        column > 0,
        jnp.where(lane < 8, high[1], high[0]),
        jnp.where(lane < 8, low[1], low[0]),
    )
    right = jnp.where(
        column > 0,
        jnp.where(lane < 8, high[0], high[1]),
        jnp.where(lane < 8, low[0], low[1]),
    )
    left = jnp.where(lane >= 8, left, pltpu.roll(left, 1, 0))
    return jnp.concatenate([left, right], axis=1)


def onto_second(low, high):
    rows = low.shape[0]
    lane = lanes_of((rows, 128))
    column = lane & 7
    low = [pltpu.roll(low[:, at : at + 128], 119, 1) for at in (0, 128)]
    high = [pltpu.roll(high[:, at : at + 128], 127, 1) for at in (0, 128)]
    left = jnp.where(
        column < 7,
        jnp.where(lane >= 120, low[1], low[0]),
        jnp.where(lane >= 120, high[1], high[0]),
    )
    right = jnp.where(
        column < 7,
        jnp.where(lane >= 120, low[0], low[1]),
        jnp.where(lane >= 120, high[0], high[1]),
    )
    right = jnp.where(lane < 120, right, pltpu.roll(right, rows - 1, 0))
    return jnp.concatenate([left, right], axis=1)


def main_kernel(
    n,
    n_chan,
    image_hbm,
    w_hbm,
    weight_hbm,
    count_hbm,
    tile_hbm,
    turns_hbm,
    square_hbm,
    tct_hbm,
    row_f_hbm,
    row_i_hbm,
    y_ref,
    norm_ref,
    image,
    tall_ref,
    weight_ref,
    count_ref,
    tile_ref,
    turns,
    square,
    tct,
    row_f,
    row_i,
    x_ref,
    b_ref,
    send1,
    recv1,
    send2,
    recv2,
    recv_w,
    recv_x,
    mark_send,
    mark_recv,
    wh,
    wl,
    th,
    tl,
    wm,
    oh,
    oht,
    own_h,
    own_l,
    g_h,
    g_l,
    h_h,
    h_l,
    grid,
    came,
    edge_send,
    edge_last,
    u_ref,
    w_send,
    w_recv,
    x_sem,
    d1_sem,
    d2_sem,
    m_sem,
    core_sem,
    ring_sem,
    own_sem,
):
    base, chan = lax.axis_index("base"), lax.axis_index("chan")
    me = base * n_chan + chan
    chip, core = chip_of(me)
    chips = n // 2
    rows = 32
    partner = device_of(chip, 1 - core)
    around = device_of(lax.rem(chip + chips + 2 * core - 1, chips), 1 - core)
    first_edge = jnp.logical_and(core == 0, chip == 0)
    last_edge = jnp.logical_and(core == 1, chip == chips - 1)

    def place(p):
        return (lax.div(p, n_chan), lax.rem(p, n_chan))

    def remote(src, dst, sems, out_index, in_index, peer):
        return pltpu.make_async_remote_copy(
            src_ref=src,
            dst_ref=dst,
            send_sem=sems.at[out_index],
            recv_sem=sems.at[in_index],
            device_id=place(peer),
            device_id_type=pl.DeviceIdType.MESH,
        )

    def block_of(p):
        its_chip, its_core = chip_of(p)
        return its_chip + its_core * (n - 1 - 2 * its_chip)

    def weights_to(p, arrives):
        return pltpu.make_async_remote_copy(
            src_ref=w_hbm.at[block_of(p)],
            dst_ref=recv_w.at[arrives],
            send_sem=w_send.at[0],
            recv_sem=w_recv.at[arrives],
            device_id=place(p),
            device_id_type=pl.DeviceIdType.MESH,
        )

    def extras_to(p, arrives):
        return remote(x_ref.at[block_of(p)], recv_x.at[arrives], x_sem, 0, 1, p)

    def first_to(p, arrives):
        its_chip, its_core = chip_of(p)
        return remote(send1.at[its_chip * 2 + its_core], recv1.at[arrives], d1_sem, 0, 1, p)

    def second_to(p, arrives):
        its_chip, its_core = chip_of(arrives)
        return remote(send2.at[p], recv2.at[its_chip * 2 + its_core], d2_sem, 0, 1, p)

    def mark_to(k):
        return lambda p, arrives: remote(
            mark_send.at[k], mark_recv.at[k, arrives], m_sem, (k, 0), (k, 1), p
        )

    def start_all(make, low=1, high=n):
        def body(step, carry):
            make(crossed(me, step, 5), me).start()
            return carry

        lax.fori_loop(low, high, body, 0)

    others = pl.ds(0, n - 1)

    def all_of(sent, landed, sems, out_index, in_index):
        return remote(sent.at[others], landed.at[others], sems, out_index, in_index, partner)

    all_weights = pltpu.make_async_remote_copy(
        src_ref=w_hbm.at[others],
        dst_ref=recv_w.at[others],
        send_sem=w_send.at[0],
        recv_sem=w_recv.at[0],
        device_id=place(partner),
        device_id_type=pl.DeviceIdType.MESH,
    )
    all_extras = all_of(x_ref, recv_x, x_sem, 0, 1)
    all_first = all_of(send1, recv1, d1_sem, 0, 1)
    all_second = all_of(send2, recv2, d2_sem, 0, 1)

    def all_marks(k):
        return all_of(mark_recv.at[k], mark_recv.at[k], m_sem, (k, 0), (k, 1))

    def put_mark(k, total):
        mark_send[k] = total
        mark_recv[k, me] = total
        start_all(mark_to(k))

    def get_mark(k):
        all_marks(k).wait_recv()
        return jnp.sqrt(jnp.sum(mark_recv[k], axis=0))

    def spread_sum(value):
        return jnp.full((1, 128), jnp.sum(value), F32)

    barrier = pltpu.get_barrier_semaphore()

    def greet(step, carry):
        peer = crossed(me, step, 5)
        pl.semaphore_signal(
            barrier, inc=1, device_id=place(peer), device_id_type=pl.DeviceIdType.MESH
        )
        return carry

    lax.fori_loop(1, n, greet, 0)
    own_w = pltpu.make_async_copy(w_hbm.at[block_of(me)], recv_w.at[me], own_sem.at[0])
    loads = [
        pltpu.make_async_copy(src, dst, own_sem.at[1 + at])
        for at, (src, dst) in enumerate(
            (
                (image_hbm, image),
                (row_f_hbm, row_f),
                (turns_hbm, turns),
                (weight_hbm, weight_ref),
                (count_hbm, count_ref),
                (tile_hbm, tile_ref),
                (square_hbm, square),
                (tct_hbm, tct),
                (row_i_hbm, row_i),
            )
        )
    ]
    for load in loads:
        load.start()
    own_w.start()
    for load in loads:
        load.wait()
    rtc, rts = turns.at[0], turns.at[1]
    tc, ts = tct.at[0], tct.at[1]
    cfh, cfl = square.at[0], square.at[1]
    cih, cil = cfh, cfl

    total = jnp.zeros((8, 128), F32)
    for lane in range(0, image.shape[1], 128):
        part = image[:, lane : lane + 128]
        tall_ref[lane : lane + 128, :] = part.T
        square_of = part * part
        for row in range(0, 64, 8):
            total = total + square_of[row : row + 8]
    for at in range(0, n, 8):
        part = jnp.concatenate(
            [tall_ref[pl.ds(at + q, 64, stride=n), :] for q in range(8)], axis=1
        )
        b_ref[:, at * 64 : at * 64 + 512] = triple_dot((row_f[0], row_f[1]), halves(part), NN)

    def row_chunk(i, carry):
        at = pl.multiple_of(i * 8, 8)
        items = [[None, None] for _ in range(n)]
        for pair in range(n // 2):
            lanes = slice(pair * 128, (pair + 1) * 128)
            for part in range(2):
                x0 = b_ref[pl.ds(at + part * 64, 8), lanes]
                x1 = b_ref[pl.ds(at + part * 64 + rows, 8), lanes]
                items[2 * pair][part], items[2 * pair + 1][part] = swap_halves(x0, x1)
        items = [
            turn(*items[q], tc_q, ts_q)
            for q, (tc_q, ts_q) in enumerate(
                (rtc[q, pl.ds(at, 8), :], rts[q, pl.ds(at, 8), :]) for q in range(n)
            )
        ]
        items = fft_list(items, -1.0)
        row = lax.broadcasted_iota(jnp.int32, (8, 128), 0) + at
        lane = lanes_of((8, 128))
        alone = jnp.logical_and(row == 0, lane < 64)
        items[0] = (items[0][0], jnp.where(alone, items[n // 2][0], items[0][1]))
        its_core = lax.div(i, 2)
        to = pl.multiple_of(lax.rem(i, 2) * 8, 8)
        for o in range(n // 2):
            send1[o * 2 + its_core, pl.ds(to, 8), :] = items[o][0]
            send1[o * 2 + its_core, pl.ds(to + 16, 8), :] = items[o][1]
        return carry

    vis = lax.broadcasted_iota(jnp.int32, (8, 256), 0)
    live = jnp.where(vis < count_ref[...], weight_ref[...], 0.0)
    tile = jnp.broadcast_to(tile_ref[...].astype(F32), (8, 256))
    squares = jnp.full((8, 256), jnp.sum(total), F32)
    slots = jnp.concatenate([live, tile, squares, jnp.zeros((104, 256), F32)], axis=0).T
    x_ref[...] = slots.reshape(n, 8, 128)
    recv_x[me] = x_ref[block_of(me)]
    lax.fori_loop(0, 4, row_chunk, 0)
    recv1[me] = send1[chip * 2 + core]

    pl.semaphore_wait(barrier, n - 1)
    start_all(extras_to)
    start_all(first_to)
    start_all(weights_to)

    all_extras.wait_recv()
    slots = recv_x[...].reshape(256, 128)
    inverse = jnp.full((1, 128), jnp.sum(recv_x[:, 0:1, 16:17]), F32)
    inverse = 1.0 / jnp.sqrt(inverse)
    tall = jnp.broadcast_to(slots[:, 8:9], (256, 256))
    tall = jnp.where(core == 0, tall, 511.0 - tall)
    wide = tall.T
    for at in range(0, 512, 256):
        down = (lax.broadcasted_iota(jnp.int32, (256, 256), 0) + at).astype(F32)
        along = (lanes_of((256, 256)) + at).astype(F32)
        oht[at : at + 256, :] = (wide == down).astype(F32).astype(BF16)
        oh[:, at : at + 256] = (tall == along).astype(F32).astype(BF16)
    spread = lax.broadcasted_iota(jnp.int32, (128, 256), 0) == (lanes_of((128, 256)) & 7)
    spread = spread.astype(F32).astype(BF16)
    high, low = halves(slots)
    rest = (slots - high.astype(F32) - low.astype(F32)).astype(BF16)
    value = jnp.dot(high, spread, preferred_element_type=F32) + (
        jnp.dot(low, spread, preferred_element_type=F32)
        + jnp.dot(rest, spread, preferred_element_type=F32)
    )
    slot = (lax.broadcasted_iota(jnp.int32, (256, 256), 0) & 31)
    wm[...] = jnp.where(slot == lax.shift_right_logical(lanes_of((256, 256)), 3), value, 0.0).reshape(8, 32, 256)

    all_first.wait_recv()

    def block(i, half):
        return 2 * core + i + 4 * half

    def forward(i, carry):
        at = pl.multiple_of(i * 8, 8)
        items = fft_list(
            [
                (
                    recv1[d, pl.ds(at, 8), :] * inverse,
                    recv1[d, pl.ds(at + 16, 8), :] * inverse,
                )
                for d in range(n)
            ],
            -1.0,
        )
        for k in range(n):
            re, im = turn(*items[k], tc[k : k + 1, :], ts[k : k + 1, :])
            u_ref[k * 8 : k * 8 + 8, :128] = re
            u_ref[k * 8 : k * 8 + 8, 128:] = im
        out = triple_dot((cfh[...], cfl[...]), halves(u_ref[...]), NT)
        for part in range(2):
            for half in range(2):
                start = part * 128 + half * 64
                came[0, part, block(i, half)] = out[start : start + 64]
        return carry

    lax.fori_loop(0, 2, forward, 0)

    def raised(block_before):
        return onto_first(block_before, block_before)

    @pl.when(first_edge)
    def _():
        z_re, z_im = came[0, 0, 0], came[0, 1, 0]
        f_re = raised(turned_block(z_re))
        f_im = -raised(turned_block(z_im))
        first = (lanes_of(z_re.shape) & 7) == 0
        came[0, 0, 0] = jnp.where(first, 0.5 * (z_re + f_re), z_re)
        came[0, 1, 0] = jnp.where(first, 0.5 * (z_im + f_im), z_im)
        edge_send[0] = 0.5 * (z_im - f_im)
        edge_send[1] = -0.5 * (z_re - f_re)

    @pl.when(jnp.logical_and(core == 0, chip > 0))
    def _():
        edge_send[0] = came[0, 0, 0]
        edge_send[1] = came[0, 1, 0]

    def half_copy(half, its_core, peer):
        at = pl.ds(2 * its_core + 4 * half, 2)
        return remote(
            came.at[0, :, at], came.at[0, :, at], core_sem, (0, half, 0), (0, half, 1), peer
        )

    for half in range(2):
        half_copy(half, core, partner).start()

    edge_copy = remote(edge_send, came.at[0, :, 8], ring_sem, (0, 0), (0, 1), around)

    @pl.when(core == 0)
    def _():
        edge_copy.start()

    def keep(a, part, value):
        high, low = halves(value)
        at = pl.ds(pl.multiple_of(a * 64, 64), 64)
        own_h[part, at, :] = high
        own_l[part, at, :] = low

    for half in range(2):
        half_copy(half, 1 - core, partner).wait_recv()

    @pl.when(core == 0)
    def _():
        def one(a, carry):
            for part in range(2):
                keep(a, part, came[0, part, a])
            return carry

        lax.fori_loop(0, 8, one, 0)

    @pl.when(core == 1)
    def _():
        edge_copy.wait_recv()

        def one(a, carry):
            for part in range(2):
                keep(a, part, onto_second(came[0, part, a], came[0, part, a + 1]))
            return carry

        lax.fori_loop(0, 8, one, 0)

    def partner_copy(k, a, its_core, peer):
        return remote(
            grid.at[k, :, a],
            came.at[k + 1, :, a + its_core],
            core_sem,
            (k + 1, a, 0),
            (k + 1, a, 1),
            peer,
        )

    def partner_sent(k):
        for a in range(8):
            partner_copy(k, a, core, partner).wait_send()

    def ring_copy(k, its_core, peer):
        return remote(
            grid.at[k, :, 7 * its_core],
            came.at[k + 1, :, 8 * (1 - its_core)],
            ring_sem,
            (k + 1, 0),
            (k + 1, 1),
            peer,
        )

    def make_ready(g):
        def one(j, carry):
            d = 4 * g + j

            @pl.when(d != me)
            def _():
                weights_to(d, d).wait_recv()

            @pl.when(d == me)
            def _():
                own_w.wait()

            return carry

        lax.fori_loop(0, 4, one, 0)
        value = recv_w[pl.ds(4 * g, 4)].reshape(256, 256)
        for part, ref, flat in zip(halves(value), (wh, wl), (th, tl)):
            moved = jnp.dot(part, square[2 + core], preferred_element_type=F32)
            ref[g] = moved.astype(BF16)
            flat[g] = moved.T.astype(BF16)

    def apply(k, inverse=None):
        for part in range(2):
            for own, out in ((own_h, g_h), (own_l, g_l)):
                out[part] = jnp.dot(
                    oh[...], own[part], preferred_element_type=F32
                ).astype(BF16).reshape(8, 32, 256)

        def group(step, carry):
            g = step
            if k == 0:
                g = crossed(lax.div(me, 4), step, 3)
                make_ready(g)
            left = tuple(
                jnp.concatenate([ref[0, g], ref[1, g]], axis=0) for ref in (g_h, g_l)
            )
            weights = (wh[g], wl[g])
            seen = triple_dot(left, (th[g], tl[g]), NN)
            weight = wm[g]
            if inverse is not None:
                weight = weight * inverse * inverse
            seen = seen * jnp.concatenate([weight, weight], axis=0)
            high, low = halves(triple_dot(halves(seen), weights, NN))
            for ref, value in ((h_h, high), (h_l, low)):
                ref[0, g] = value[:32]
                ref[1, g] = value[32:]
            return carry

        lax.fori_loop(0, 8, group, 0, unroll=1 if k == 0 else 4)
        for part in range(2):
            grid[k, part] = move(
                oht[...], (h_h[part].reshape(256, 256), h_l[part].reshape(256, 256))
            ).reshape(8, 64, 256)
        ring_copy(k, core, around).start()

        def one(a, carry):
            partner_copy(k, a, core, partner).start()
            return carry

        lax.fori_loop(0, 8, one, 0)

    def close_edge(k):
        ring_copy(k, 1 - core, around).wait_recv()

        @pl.when(jnp.logical_or(first_edge, last_edge))
        def _():
            came[k + 1, 0, 8 * core] = turned_block(grid[k, 0, 7 * core])
            came[k + 1, 1, 8 * core] = -turned_block(grid[k, 1, 7 * core])

    def combine(k):
        def run(onto, start, last):
            def block(a, total):
                for part in range(2):
                    value = grid[k, part, a] + onto(came[k + 1, part, a], came[k + 1, part, a + 1])
                    value = 0.5 * value
                    keep(a, part, value)
                    if k == 0:
                        total = total + value * value
                return total

            def one(step, total):
                partner_copy(k, step + 1, 1 - core, partner).wait_recv()
                return block(step + start, total)

            partner_copy(k, 0, 1 - core, partner).wait_recv()
            total = lax.fori_loop(0, 7, one, jnp.zeros((64, 256), F32))
            close_edge(k)
            return block(last, total)

        return lax.cond(
            core == 0, lambda: run(onto_first, 1, 0), lambda: run(onto_second, 0, 7)
        )

    def two_lanes(value):
        return jnp.concatenate([value, value], axis=1)

    apply(0)
    put_mark(0, spread_sum(combine(0)))
    apply(1)
    combine(1)
    n1 = get_mark(0)
    inverse = two_lanes(1.0 / n1)
    apply(2, inverse)
    for a in range(8):
        partner_copy(2, a, 1 - core, partner).wait_recv()
    ring_copy(2, 1 - core, around).wait_recv()


    @pl.when(first_edge)
    def _():
        up = raised(came[3, 0, 0]), raised(came[3, 1, 0])
        edge_last[0] = up[0] + raised(turned_block(up[0]))
        edge_last[1] = up[1] - raised(turned_block(up[1]))

    @pl.when(first_edge)
    def _():
        came[3, 0, 0] = turned_block(grid[2, 0, 0])
        came[3, 1, 0] = -turned_block(grid[2, 1, 0])

    def last_sum(j, total):
        a = 2 * core + lax.rem(j, 2) + 4 * lax.div(j, 2)

        @pl.when(core == 0)
        def _():
            for part in range(2):
                value = grid[2, part, a] + onto_first(came[3, part, a], came[3, part, a + 1])
                grid[0, part, a] = value

        @pl.when(core == 1)
        def _():
            for part in range(2):
                value = came[3, part, a] + onto_first(grid[2, part, a - 1], grid[2, part, a])
                grid[0, part, a] = value

        for part in range(2):
            value = grid[0, part, a]
            total = total + value * value
        return total

    partner_sent(0)
    ring_copy(0, core, around).wait_send()
    total = 0.5 * lax.fori_loop(0, 4, last_sum, jnp.zeros((64, 256), F32))
    h0_re, h0_im = grid[0, 0, 0], grid[0, 1, 0]
    alone = jnp.logical_and((lanes_of((64, 256)) & 7) == 0, first_edge)
    z_re = jnp.where(alone, 0.5 * (h0_re - edge_last[1]), h0_re)
    z_im = jnp.where(alone, 0.5 * (h0_im + edge_last[0]), h0_im)

    @pl.when(first_edge)
    def _():
        grid[0, 0, 0] = z_re
        grid[0, 1, 0] = z_im


    def backward(i, carry):
        at = pl.multiple_of(i * 8, 8)
        held = jnp.concatenate(
            [grid[0, part, block(i, half)] for part in range(2) for half in range(2)], axis=0
        )
        u_ref[...] = triple_dot(halves(held.T), (cih[...], cil[...]), NN)
        items = []
        for k in range(n):
            re = u_ref[k * 8 : k * 8 + 8, :128]
            im = u_ref[k * 8 : k * 8 + 8, 128:]
            items.append(turn(re, im, tc[k : k + 1, :], -ts[k : k + 1, :]))
        items = fft_list(items, 1.0)
        for d in range(n):
            send2[d, pl.ds(at, 8), :] = items[d][0]
            send2[d, pl.ds(at + 16, 8), :] = items[d][1]
        return carry

    lax.fori_loop(0, 2, backward, 0)
    recv2[chip * 2 + core] = send2[me]
    start_all(second_to)
    change = z_re * z_re + z_im * z_im - 0.5 * (h0_re * h0_re + h0_im * h0_im)
    third = spread_sum(total + jnp.where(alone, change, 0.0))

    def second_sum(i, sums):
        at = pl.ds(pl.multiple_of(i * 64, 64), 64)
        for part in range(2):
            value = own_h[part, at, :].astype(F32) + own_l[part, at, :].astype(F32)
            value = value * inverse
            sums = sums + value * value
        return sums

    second = spread_sum(lax.fori_loop(0, 8, second_sum, jnp.zeros((64, 256), F32)))
    put_mark(1, jnp.where(lanes_of((1, 128)) < 64, second, third))
    all_extras.wait_send()
    all_weights.wait_send()
    all_first.wait_send()
    all_marks(0).wait_send()
    for half in range(2):
        half_copy(half, core, partner).wait_send()

    @pl.when(core == 0)
    def _():
        edge_copy.wait_send()

    for k in (1, 2):
        partner_sent(k)
        ring_copy(k, core, around).wait_send()
    all_second.wait_recv()

    def back_chunk(i, carry):
        at = pl.multiple_of(i * 8, 8)
        its_core = lax.div(i, 2)
        to = pl.multiple_of(lax.rem(i, 2) * 8, 8)
        items = [
            (recv2[o * 2 + its_core, pl.ds(to, 8), :], recv2[o * 2 + its_core, pl.ds(to + 16, 8), :])
            for o in range(n // 2)
        ]
        row = lax.broadcasted_iota(jnp.int32, (8, 128), 0) + at
        lane = lanes_of((8, 128))
        extra = jnp.where(jnp.logical_and(row == 0, lane < 64), items[0][1], 0.0)
        even = fft_list(items, 1.0)
        odd = []
        for o, (re, im) in enumerate(items):
            angle = 2.0 * math.pi * o / n
            odd.append((re, im) if o == 0 else turn(re, im, math.cos(angle), math.sin(angle)))
        odd = fft_list(odd, 1.0)
        items = []
        for k in range(n // 2):
            items.append((even[k][0] + extra, even[k][1]))
            items.append((odd[k][0] - extra, odd[k][1]))
        items = [
            turn(*items[q], rtc[q, pl.ds(at, 8), :], -rts[q, pl.ds(at, 8), :]) for q in range(n)
        ]
        for pair in range(n // 2):
            lanes = slice(pair * 128, (pair + 1) * 128)
            for part in range(2):
                x0, x1 = swap_halves(items[2 * pair][part], items[2 * pair + 1][part])
                b_ref[pl.ds(at + part * 64, 8), lanes] = x0
                b_ref[pl.ds(at + part * 64 + rows, 8), lanes] = x1
        return carry

    lax.fori_loop(0, 4, back_chunk, 0)
    both = get_mark(1)
    n2, n3 = jnp.full((1, 128), both[0, 0], F32), jnp.full((1, 128), both[0, 64], F32)
    factor = float(image.shape[1]) / n3
    factor = jnp.concatenate([factor] * 4, axis=1)
    for at in range(0, n, 8):
        lanes = slice(at * 64, at * 64 + 512)
        part = triple_dot((row_i[0], row_i[1]), halves(b_ref[:, lanes]), NN) * factor
        for q in range(8):
            tall_ref[pl.ds(at + q, 64, stride=n), :] = part[:, q * 64 : q * 64 + 64]
    for lane in range(0, image.shape[1], 128):
        y_ref[:, lane : lane + 128] = tall_ref[lane : lane + 128, :].T
    norm_ref[0:1, :] = n1
    norm_ref[1:2, :] = n2
    norm_ref[2:3, :] = n3 * n1 / n2
    all_second.wait_send()
    all_marks(1).wait_send()


def tables(n, row_count, length):
    half = row_count // 2
    scale = 1.0 / math.sqrt(length)
    local = np.arange(row_count)
    angle = -2.0 * np.pi * np.outer(local, local) / row_count
    c, s = np.cos(angle) * scale, np.sin(angle) * scale
    two = np.eye(2)
    col_f = np.block([[np.kron(two, c), np.kron(two, -s)], [np.kron(two, s), np.kron(two, c)]])
    col_i = col_f
    row_f = np.concatenate([c, s], axis=0)
    row_i = np.concatenate([c, s], axis=1)
    index = np.arange(n)
    turns = -2.0 * np.pi * np.outer(index, np.tile(local, 2)) / length
    u = np.arange(half)[:, None] + half * (np.arange(2 * row_count)[None, :] // row_count)
    row_turns = -2.0 * np.pi * index[:, None, None] * u[None] / length
    return col_f, col_i, row_f, row_i, turns, row_turns


def fast_device(image0, interp, vis_weight, counts, tile_index):
    n_chan = lax.axis_size("chan")
    n = lax.axis_size("base") * n_chan
    row_count, length = image0.shape
    touch = tile_index.shape[2]
    each = touch // n
    vcap, cells = interp.shape[3:]
    col_f, col_i, row_f, row_i, turns, row_turns = tables(n, row_count, length)
    cfh, cfl = np_halves(col_f)
    rows_f, rows_i = np.stack(np_halves(row_f)), np.stack(np_halves(row_i))
    column_turns = np.stack([np.cos(turns), np.sin(turns)]).astype(np.float32)
    row_turns = np.stack([np.cos(row_turns), np.sin(row_turns)]).astype(np.float32)
    order = np.arange(cells).reshape(TILE_V, TILE_U).T.reshape(-1)
    perm = np.zeros((2, cells, cells), np.float32)
    perm[0, order, np.arange(cells)] = 1.0
    perm[1] = perm[0][:, ::-1]
    perm = perm.astype(jnp.bfloat16)
    square = np.concatenate([np.stack([cfh, cfl]), perm])
    matrices = interp.reshape(n, each * vcap, cells)
    weight = vis_weight.reshape(touch, vcap).T
    count = counts.reshape(1, touch)
    tile = tile_index.reshape(1, touch)

    def dma(*shape):
        return pltpu.SemaphoreType.DMA(shape)

    message = (n, 32, 128)
    wide = (8, 64, 256)
    image, norms = pl.pallas_call(
        lambda *refs: main_kernel(n, n_chan, *refs),
        out_shape=[
            jax.ShapeDtypeStruct((row_count, length), F32),
            jax.ShapeDtypeStruct((8, 128), F32),
        ],
        in_specs=[HBM_SPEC] * 10,
        out_specs=[VMEM_SPEC] * 2,
        scratch_shapes=[
            pltpu.VMEM((row_count, length), F32),
            pltpu.VMEM((length, row_count), F32),
            pltpu.VMEM(weight.shape, F32),
            pltpu.VMEM(count.shape, jnp.int32),
            pltpu.VMEM(tile.shape, jnp.int32),
            pltpu.VMEM(row_turns.shape, F32),
            pltpu.VMEM(square.shape, BF16),
            pltpu.VMEM(column_turns.shape, F32),
            pltpu.VMEM(rows_f.shape, BF16),
            pltpu.VMEM(rows_i.shape, BF16),
            pltpu.VMEM((n, 8, 128), F32),
            pltpu.VMEM((2 * row_count, length), F32),
            pltpu.VMEM(message, F32),
            pltpu.VMEM(message, F32),
            pltpu.VMEM(message, F32),
            pltpu.VMEM(message, F32),
            pltpu.VMEM((n, each * vcap, cells), F32),
            pltpu.VMEM((n, 8, 128), F32),
            pltpu.VMEM((2, 1, 128), F32),
            pltpu.VMEM((2, n, 1, 128), F32),
            pltpu.VMEM((8, cells, cells), BF16),
            pltpu.VMEM((8, cells, cells), BF16),
            pltpu.VMEM((8, cells, cells), BF16),
            pltpu.VMEM((8, cells, cells), BF16),
            pltpu.VMEM((8, 32, cells), F32),
            pltpu.VMEM((touch, 512), BF16),
            pltpu.VMEM((512, touch), BF16),
            pltpu.VMEM((2, 512, cells), BF16),
            pltpu.VMEM((2, 512, cells), BF16),
            pltpu.VMEM((2, 8, 32, cells), BF16),
            pltpu.VMEM((2, 8, 32, cells), BF16),
            pltpu.VMEM((2, 8, 32, cells), BF16),
            pltpu.VMEM((2, 8, 32, cells), BF16),
            pltpu.VMEM((3, 2, 8, 64, cells), F32),
            pltpu.VMEM((4, 2, 9, 64, cells), F32),
            pltpu.VMEM((2, 64, cells), F32),
            pltpu.VMEM((2, 64, cells), F32),
            pltpu.VMEM((256, 256), F32),
            dma(1),
            dma(n),
            dma(2),
            dma(2),
            dma(2),
            dma(4, 2),
            dma(4, 8, 2),
            dma(4, 2),
            dma(10),
        ],
        compiler_params=pltpu.CompilerParams(
            has_side_effects=True, collective_id=0, vmem_limit_bytes=67043328
        ),
    )(
        image0,
        matrices,
        weight,
        count,
        tile,
        jnp.asarray(row_turns),
        jnp.asarray(square),
        column_turns,
        rows_f,
        rows_i,
    )
    return image, norms[:3, 0]


def per_device(image0, interp, vis_weight, counts, tile_index):
    n = lax.axis_size("base") * lax.axis_size("chan")
    row_count, length = image0.shape
    vcap, cells = interp.shape[3:]
    touch = tile_index.shape[2]
    fits = (n, row_count, length // row_count) == (TILE_U, 64, TILE_U)
    if fits and (vcap, cells, touch % 256) == (8, 256, 0) and touch // n == 8:
        return fast_device(image0, interp, vis_weight, counts, tile_index)
    return general_device(image0, interp, vis_weight, counts, tile_index)


def solution(mesh):
    placed = (
        P(("base", "chan"), None),
        P("base", "chan", None, None, None),
        P("base", "chan", None, None),
        P("base", "chan", None),
        P("base", "chan", None),
    )
    return jax.shard_map(
        per_device,
        mesh=mesh,
        in_specs=placed,
        out_specs=(P(("base", "chan"), None), P()),
        check_vma=False,
    )
```

```python
import math

import jax
import jax.numpy as jnp
import numpy as np
from jax import lax
from jax.experimental import pallas as pl
from jax.experimental.pallas import tpu as pltpu
from jax.sharding import PartitionSpec as P

TILE_V = 8
TILE_U = 32
ITERS = 3


PRECISION_LEVEL = lax.Precision.HIGHEST


def split_length(length):
    outer_len = 2 ** ((length.bit_length() - 1) // 2)
    return (outer_len, length // outer_len)


def angle_table(count_a, count_b, modulus, sign):
    left = jnp.arange(count_a, dtype=jnp.int32)[:, None]
    right = jnp.arange(count_b, dtype=jnp.int32)[None, :]
    angle = sign * 2.0 * math.pi / modulus * (left * right % modulus).astype(jnp.float32)
    return (jnp.cos(angle), jnp.sin(angle))


def transform_rows(real_part, imag_part, sign):
    row_count, length = real_part.shape
    outer_len, inner_len = split_length(length)
    cos_q, sin_q = angle_table(inner_len, inner_len, inner_len, sign)
    cos_t, sin_t = angle_table(inner_len, outer_len, length, sign)
    cos_p, sin_p = angle_table(outer_len, outer_len, outer_len, sign)
    real_in = real_part.reshape(row_count, inner_len, outer_len)
    first_re = jnp.einsum("kq,rqp->rkp", cos_q, real_in, precision=PRECISION_LEVEL)
    first_im = jnp.einsum("kq,rqp->rkp", sin_q, real_in, precision=PRECISION_LEVEL)
    if imag_part is not None:
        imag_in = imag_part.reshape(row_count, inner_len, outer_len)
        first_re = first_re - jnp.einsum("kq,rqp->rkp", sin_q, imag_in, precision=PRECISION_LEVEL)
        first_im = first_im + jnp.einsum("kq,rqp->rkp", cos_q, imag_in, precision=PRECISION_LEVEL)
    turned_re = first_re * cos_t - first_im * sin_t
    turned_im = first_re * sin_t + first_im * cos_t
    last_re = jnp.einsum("jp,rkp->rjk", cos_p, turned_re, precision=PRECISION_LEVEL) - jnp.einsum(
        "jp,rkp->rjk", sin_p, turned_im, precision=PRECISION_LEVEL
    )
    last_im = jnp.einsum("jp,rkp->rjk", cos_p, turned_im, precision=PRECISION_LEVEL) + jnp.einsum(
        "jp,rkp->rjk", sin_p, turned_re, precision=PRECISION_LEVEL
    )
    factor = 1.0 / math.sqrt(length)
    return (
        last_re.reshape(row_count, length) * factor,
        last_im.reshape(row_count, length) * factor,
    )


def transpose_global(real_part, imag_part):
    row_count, length = real_part.shape
    n_base = lax.axis_size("base")
    n_chan = lax.axis_size("chan")
    width = length // (n_base * n_chan)
    moved = (
        lax.all_to_all(
            lax.all_to_all(
                real_part.reshape(1, row_count, n_base, n_chan, width),
                "base",
                split_axis=2,
                concat_axis=0,
                tiled=True,
            ),
            "chan",
            split_axis=3,
            concat_axis=1,
            tiled=True,
        ),
        lax.all_to_all(
            lax.all_to_all(
                imag_part.reshape(1, row_count, n_base, n_chan, width),
                "base",
                split_axis=2,
                concat_axis=0,
                tiled=True,
            ),
            "chan",
            split_axis=3,
            concat_axis=1,
            tiled=True,
        ),
    )
    return (moved[0].reshape(length, width).T, moved[1].reshape(length, width).T)


def to_tiles(plane):
    row_count, length = plane.shape
    shaped = plane.reshape(row_count // TILE_V, TILE_V, length // TILE_U, TILE_U)
    return shaped.transpose(0, 2, 1, 3).reshape(-1, TILE_V * TILE_U)


def from_tiles(tiles, row_count, length):
    shaped = tiles.reshape(row_count // TILE_V, length // TILE_U, TILE_V, TILE_U)
    return shaped.transpose(0, 2, 1, 3).reshape(row_count, length)


def slot_work(sample_weights, masked_weight, sample_values):
    visible_samples = (
        jnp.einsum("gnz,gez->gen", sample_weights, sample_values, precision=PRECISION_LEVEL)
        * masked_weight[:, None, :]
    )
    return jnp.einsum("hbi,hyb->hyi", sample_weights, visible_samples, precision=PRECISION_LEVEL)


def total_squares(image):
    return lax.psum(jnp.sum(image * image), ("base", "chan"))


def general_device(image0, interp, vis_weight, counts, tile_index):
    n_base = lax.axis_size("base")
    n_chan = lax.axis_size("chan")
    row_count, length = image0.shape
    touch = tile_index.shape[2]
    slots_each = touch // (n_base * n_chan)
    vcap = interp.shape[3]
    cells = interp.shape[4]
    tiles_own = row_count // TILE_V * (length // TILE_U)
    live = (jnp.arange(vcap, dtype=jnp.int32)[None, :] < counts.reshape(touch, 1)).astype(
        jnp.float32
    )
    masked_weight = vis_weight.reshape(touch, vcap) * live
    sample_weights = interp.reshape(touch, vcap, cells)
    wanted = lax.all_to_all(
        lax.all_to_all(
            tile_index.reshape(n_base, n_chan, slots_each),
            "base",
            split_axis=0,
            concat_axis=0,
            tiled=True,
        ),
        "chan",
        split_axis=1,
        concat_axis=1,
        tiled=True,
    ).reshape(touch)
    onehot = (jnp.arange(tiles_own, dtype=jnp.int32)[:, None] == wanted[None, :]).astype(
        jnp.float32
    )
    moved = (
        lax.all_to_all(
            lax.all_to_all(
                sample_weights.reshape(n_base, n_chan, slots_each, vcap, cells),
                "base",
                split_axis=0,
                concat_axis=0,
                tiled=True,
            ),
            "chan",
            split_axis=1,
            concat_axis=1,
            tiled=True,
        ),
        lax.all_to_all(
            lax.all_to_all(
                masked_weight.reshape(n_base, n_chan, slots_each, vcap),
                "base",
                split_axis=0,
                concat_axis=0,
                tiled=True,
            ),
            "chan",
            split_axis=1,
            concat_axis=1,
            tiled=True,
        ),
    )
    sample_weights = moved[0].reshape(touch, vcap, cells)
    masked_weight = moved[1].reshape(touch, vcap)
    found = []
    current = image0 / jnp.sqrt(total_squares(image0))
    for iteration in range(ITERS):
        real_part, imag_part = transform_rows(current, None, -1.0)
        real_part, imag_part = transpose_global(real_part, imag_part)
        real_part, imag_part = transform_rows(real_part, imag_part, -1.0)
        tiles = jnp.stack([to_tiles(real_part), to_tiles(imag_part)], axis=1)
        sample_values = jnp.take(tiles, wanted, axis=0)
        gridded_plane = slot_work(sample_weights, masked_weight, sample_values)
        summed = jnp.einsum("ts,skc->tkc", onehot, gridded_plane, precision=PRECISION_LEVEL)
        real_part = from_tiles(summed[:, 0, :], row_count, length)
        imag_part = from_tiles(summed[:, 1, :], row_count, length)
        real_part, imag_part = transform_rows(real_part, imag_part, 1.0)
        real_part, imag_part = transpose_global(real_part, imag_part)
        real_part, imag_part = transform_rows(real_part, imag_part, 1.0)
        norm_value = jnp.sqrt(total_squares(real_part))
        found.append(norm_value)
        current = real_part / norm_value
    return (float(length) * current, jnp.stack(found))


F32 = jnp.float32
BF16 = jnp.bfloat16
VMEM_SPEC = pl.BlockSpec(memory_space=pltpu.VMEM)
SMEM_SPEC = pl.BlockSpec(memory_space=pltpu.SMEM)
BIG = pltpu.CompilerParams(vmem_limit_bytes=48 * 1024 * 1024)


def halves(value):
    high = value.astype(BF16)
    return high, (value - high.astype(F32)).astype(BF16)


def np_halves(table):
    high = np.asarray(table, np.float32).astype(jnp.bfloat16)
    low = (np.asarray(table, np.float64) - high.astype(np.float64)).astype(jnp.bfloat16)
    return high, low


def triple_dot(left, right, dims):
    def one(a, b):
        return lax.dot_general(a, b, (dims, ((), ())), preferred_element_type=F32)

    return one(left[0], right[0]) + (one(left[0], right[1]) + one(left[1], right[0]))


def fft_list(items, sign):
    count = len(items)
    if count == 1:
        return items
    even = fft_list(items[0::2], sign)
    odd = fft_list(items[1::2], sign)
    low, high = [], []
    for k in range(count // 2):
        re, im = odd[k]
        if k == 0:
            t_re, t_im = re, im
        elif 4 * k == count:
            t_re, t_im = (im, -re) if sign < 0 else (-im, re)
        else:
            angle = sign * 2.0 * math.pi * k / count
            c, s = math.cos(angle), math.sin(angle)
            t_re, t_im = re * c - im * s, re * s + im * c
        e_re, e_im = even[k]
        low.append((e_re + t_re, e_im + t_im))
        high.append((e_re - t_re, e_im - t_im))
    return low + high


AHEAD = 4
NEEDED = ((0, 3, 4, 1, 5), (2, 3, 6, 7))
HBM_SPEC = pl.BlockSpec(memory_space=pltpu.HBM)
NT = ((1,), (1,))
NN = ((1,), (0,))


def turn(re, im, c, s):
    return re * c - im * s, re * s + im * c


def swap_halves(x0, x1):
    half = x0.shape[1] // 2
    left = lax.broadcasted_iota(jnp.int32, x0.shape, 1) < half
    return (
        jnp.where(left, x0, pltpu.roll(x1, half, 1)),
        jnp.where(left, pltpu.roll(x0, half, 1), x1),
    )


def move(table, parts, dims=NN):
    def one(part):
        return lax.dot_general(table, part, (dims, ((), ())), preferred_element_type=F32)

    return one(parts[0]) + one(parts[1])


def bit_of(p, bit):
    return lax.rem(lax.div(p, 2**bit), 2)


def walk(z, w):
    odd = lax.rem(w, 2)
    return 4 * w + z + odd * (3 - 2 * z)


def chip_of(p):
    x, y = bit_of(p, 2), bit_of(p, 0)
    return walk(lax.div(p, 8), 3 * x + y - 2 * x * y), bit_of(p, 1)


def device_of(chip, core):
    w, at = lax.div(chip, 4), lax.rem(chip, 4)
    odd = lax.rem(w, 2)
    z = at + odd * (3 - 2 * at)
    x = lax.div(w, 2)
    y = odd + x - 2 * x * odd
    return ((z * 2 + x) * 2 + core) * 2 + y


def crossed(p, step, bits):
    value = p + step
    for bit in range(bits):
        value = value - 2 ** (bit + 1) * bit_of(p, bit) * bit_of(step, bit)
    return value


def turned_block(block):
    rows, lanes = block.shape

    def anti(size):
        total = lax.broadcasted_iota(jnp.int32, (size, size), 0) + lax.broadcasted_iota(
            jnp.int32, (size, size), 1
        )
        return (total == size - 1).astype(F32).astype(BF16)

    half = move(anti(rows), halves(block))
    high, low = halves(half)
    table = anti(lanes)

    def one(part):
        return jnp.dot(part, table, preferred_element_type=F32)

    return one(high) + one(low)


def lanes_of(shape):
    return lax.broadcasted_iota(jnp.int32, shape, 1)


def onto_first(low, high):
    lane = lanes_of((low.shape[0], 128))
    column = lane & 7
    high = [pltpu.roll(high[:, at : at + 128], 9, 1) for at in (0, 128)]
    low = [pltpu.roll(low[:, at : at + 128], 1, 1) for at in (0, 128)]
    left = jnp.where(
        column > 0,
        jnp.where(lane < 8, high[1], high[0]),
        jnp.where(lane < 8, low[1], low[0]),
    )
    right = jnp.where(
        column > 0,
        jnp.where(lane < 8, high[0], high[1]),
        jnp.where(lane < 8, low[0], low[1]),
    )
    left = jnp.where(lane >= 8, left, pltpu.roll(left, 1, 0))
    return jnp.concatenate([left, right], axis=1)


def onto_second(low, high):
    rows = low.shape[0]
    lane = lanes_of((rows, 128))
    column = lane & 7
    low = [pltpu.roll(low[:, at : at + 128], 119, 1) for at in (0, 128)]
    high = [pltpu.roll(high[:, at : at + 128], 127, 1) for at in (0, 128)]
    left = jnp.where(
        column < 7,
        jnp.where(lane >= 120, low[1], low[0]),
        jnp.where(lane >= 120, high[1], high[0]),
    )
    right = jnp.where(
        column < 7,
        jnp.where(lane >= 120, low[0], low[1]),
        jnp.where(lane >= 120, high[0], high[1]),
    )
    right = jnp.where(lane < 120, right, pltpu.roll(right, rows - 1, 0))
    return jnp.concatenate([left, right], axis=1)


def main_kernel(
    n,
    n_chan,
    image_hbm,
    w_hbm,
    weight_hbm,
    count_hbm,
    tile_hbm,
    turns_hbm,
    square_hbm,
    tct_hbm,
    row_f_hbm,
    row_i_hbm,
    y_ref,
    norm_ref,
    image,
    tall_ref,
    weight_ref,
    count_ref,
    tile_ref,
    turns,
    square,
    tct,
    row_f,
    row_i,
    x_ref,
    b_ref,
    send1,
    recv1,
    send2,
    recv2,
    recv_w,
    recv_x,
    mark_send,
    mark_recv,
    wh,
    wl,
    th,
    tl,
    wm,
    oh,
    oht,
    own_h,
    own_l,
    g_h,
    g_l,
    h_h,
    h_l,
    grid,
    came,
    edge_send,
    edge_last,
    ring_send,
    ring_came,
    u_ref,
    w_send,
    w_recv,
    x_sem,
    d1_sem,
    d2_sem,
    m_sem,
    core_sem,
    ring_sem,
    own_sem,
):
    base, chan = lax.axis_index("base"), lax.axis_index("chan")
    me = base * n_chan + chan
    chip, core = chip_of(me)
    chips = n // 2
    rows = 32
    partner = device_of(chip, 1 - core)
    around = device_of(lax.rem(chip + chips + 2 * core - 1, chips), 1 - core)
    first_edge = jnp.logical_and(core == 0, chip == 0)
    last_edge = jnp.logical_and(core == 1, chip == chips - 1)

    def place(p):
        return (lax.div(p, n_chan), lax.rem(p, n_chan))

    def remote(src, dst, sems, out_index, in_index, peer):
        return pltpu.make_async_remote_copy(
            src_ref=src,
            dst_ref=dst,
            send_sem=sems.at[out_index],
            recv_sem=sems.at[in_index],
            device_id=place(peer),
            device_id_type=pl.DeviceIdType.MESH,
        )

    def block_of(p):
        its_chip, its_core = chip_of(p)
        return its_chip + its_core * (n - 1 - 2 * its_chip)

    def weights_to(p, arrives):
        return pltpu.make_async_remote_copy(
            src_ref=w_hbm.at[block_of(p)],
            dst_ref=recv_w.at[arrives],
            send_sem=w_send.at[0],
            recv_sem=w_recv.at[arrives],
            device_id=place(p),
            device_id_type=pl.DeviceIdType.MESH,
        )

    def extras_to(p, arrives):
        return remote(x_ref.at[block_of(p)], recv_x.at[arrives], x_sem, 0, 1, p)

    def first_to(p, arrives):
        its_chip, its_core = chip_of(p)
        return remote(send1.at[its_chip * 2 + its_core], recv1.at[arrives], d1_sem, 0, 1, p)

    def second_to(p, arrives):
        its_chip, its_core = chip_of(arrives)
        return remote(send2.at[p], recv2.at[its_chip * 2 + its_core], d2_sem, 0, 1, p)

    def mark_to(k):
        return lambda p, arrives: remote(
            mark_send.at[k], mark_recv.at[k, arrives], m_sem, (k, 0), (k, 1), p
        )

    def start_all(make, low=1, high=n):
        def body(step, carry):
            make(crossed(me, step, 5), me).start()
            return carry

        lax.fori_loop(low, high, body, 0)

    others = pl.ds(0, n - 1)

    def all_of(sent, landed, sems, out_index, in_index):
        return remote(sent.at[others], landed.at[others], sems, out_index, in_index, partner)

    all_weights = pltpu.make_async_remote_copy(
        src_ref=w_hbm.at[others],
        dst_ref=recv_w.at[others],
        send_sem=w_send.at[0],
        recv_sem=w_recv.at[0],
        device_id=place(partner),
        device_id_type=pl.DeviceIdType.MESH,
    )
    all_extras = all_of(x_ref, recv_x, x_sem, 0, 1)
    all_first = all_of(send1, recv1, d1_sem, 0, 1)
    all_second = all_of(send2, recv2, d2_sem, 0, 1)

    def all_marks(k):
        return all_of(mark_recv.at[k], mark_recv.at[k], m_sem, (k, 0), (k, 1))

    def put_mark(k, total):
        mark_send[k] = total
        mark_recv[k, me] = total
        start_all(mark_to(k))

    def get_mark(k):
        all_marks(k).wait_recv()
        return jnp.sqrt(jnp.sum(mark_recv[k], axis=0))

    def spread_sum(value):
        return jnp.full((1, 128), jnp.sum(value), F32)

    own_w = pltpu.make_async_copy(w_hbm.at[block_of(me)], recv_w.at[me], own_sem.at[0])
    loads = [
        pltpu.make_async_copy(src, dst, own_sem.at[1 + at])
        for at, (src, dst) in enumerate(
            (
                (image_hbm, image),
                (row_f_hbm, row_f),
                (turns_hbm, turns),
                (weight_hbm, weight_ref),
                (count_hbm, count_ref),
                (tile_hbm, tile_ref),
                (square_hbm, square),
                (tct_hbm, tct),
                (row_i_hbm, row_i),
            )
        )
    ]
    for load in loads:
        load.start()
    own_w.start()
    barrier = pltpu.get_barrier_semaphore()

    def greet(step, carry):
        peer = crossed(me, step, 5)
        pl.semaphore_signal(
            barrier, inc=1, device_id=place(peer), device_id_type=pl.DeviceIdType.MESH
        )
        return carry

    lax.fori_loop(1, n, greet, 0)
    rtc, rts = turns.at[0], turns.at[1]
    tc, ts = tct.at[0], tct.at[1]
    cfh, cfl = square.at[0], square.at[1]
    cih, cil = cfh, cfl

    loads[0].wait()
    loads[1].wait()
    total = jnp.zeros((8, 128), F32)
    for lane in range(0, image.shape[1], 128):
        part = image[:, lane : lane + 128]
        tall_ref[lane : lane + 128, :] = part.T
        square_of = part * part
        for row in range(0, 64, 8):
            total = total + square_of[row : row + 8]
    for at in range(0, n, 8):
        part = jnp.concatenate(
            [tall_ref[pl.ds(at + q, 64, stride=n), :] for q in range(8)], axis=1
        )
        b_ref[:, at * 64 : at * 64 + 512] = triple_dot((row_f[0], row_f[1]), halves(part), NN)

    def row_chunk(i, carry):
        at = pl.multiple_of(i * 8, 8)
        items = [[None, None] for _ in range(n)]
        for pair in range(n // 2):
            lanes = slice(pair * 128, (pair + 1) * 128)
            for part in range(2):
                x0 = b_ref[pl.ds(at + part * 64, 8), lanes]
                x1 = b_ref[pl.ds(at + part * 64 + rows, 8), lanes]
                items[2 * pair][part], items[2 * pair + 1][part] = swap_halves(x0, x1)
        items = [
            turn(*items[q], tc_q, ts_q)
            for q, (tc_q, ts_q) in enumerate(
                (rtc[q, pl.ds(at, 8), :], rts[q, pl.ds(at, 8), :]) for q in range(n)
            )
        ]
        items = fft_list(items, -1.0)
        row = lax.broadcasted_iota(jnp.int32, (8, 128), 0) + at
        lane = lanes_of((8, 128))
        alone = jnp.logical_and(row == 0, lane < 64)
        items[0] = (items[0][0], jnp.where(alone, items[n // 2][0], items[0][1]))
        its_core = lax.div(i, 2)
        to = pl.multiple_of(lax.rem(i, 2) * 8, 8)
        for o in range(n // 2):
            send1[o * 2 + its_core, pl.ds(to, 8), :] = items[o][0]
            send1[o * 2 + its_core, pl.ds(to + 16, 8), :] = items[o][1]
        return carry

    for load in loads[2:]:
        load.wait()
    vis = lax.broadcasted_iota(jnp.int32, (8, 256), 0)
    live = jnp.where(vis < count_ref[...], weight_ref[...], 0.0)
    tile = jnp.broadcast_to(tile_ref[...].astype(F32), (8, 256))
    squares = jnp.full((8, 256), jnp.sum(total), F32)
    slots = jnp.concatenate([live, tile, squares, jnp.zeros((104, 256), F32)], axis=0).T
    x_ref[...] = slots.reshape(n, 8, 128)
    recv_x[me] = x_ref[block_of(me)]
    lax.fori_loop(0, 4, row_chunk, 0)
    recv1[me] = send1[chip * 2 + core]

    pl.semaphore_wait(barrier, n - 1)
    start_all(first_to)
    start_all(extras_to)
    start_all(weights_to, n // 2, n // 2 + AHEAD)

    all_extras.wait_recv()
    slots = recv_x[...].reshape(256, 128)
    inverse = jnp.full((1, 128), jnp.sum(recv_x[:, 0:1, 16:17]), F32)
    inverse = 1.0 / jnp.sqrt(inverse)
    tall = jnp.broadcast_to(slots[:, 8:9], (256, 256))
    tall = jnp.where(core == 0, tall, 511.0 - tall)
    wide = tall.T
    for at in range(0, 512, 256):
        down = (lax.broadcasted_iota(jnp.int32, (256, 256), 0) + at).astype(F32)
        along = (lanes_of((256, 256)) + at).astype(F32)
        oht[at : at + 256, :] = (wide == down).astype(F32).astype(BF16)
        oh[:, at : at + 256] = (tall == along).astype(F32).astype(BF16)
    spread = lax.broadcasted_iota(jnp.int32, (128, 256), 0) == (lanes_of((128, 256)) & 7)
    spread = spread.astype(F32).astype(BF16)
    high, low = halves(slots)
    rest = (slots - high.astype(F32) - low.astype(F32)).astype(BF16)
    value = jnp.dot(high, spread, preferred_element_type=F32) + (
        jnp.dot(low, spread, preferred_element_type=F32)
        + jnp.dot(rest, spread, preferred_element_type=F32)
    )
    slot = (lax.broadcasted_iota(jnp.int32, (256, 256), 0) & 31)
    wm[...] = jnp.where(slot == lax.shift_right_logical(lanes_of((256, 256)), 3), value, 0.0).reshape(8, 32, 256)

    all_first.wait_recv()

    def block(i, half):
        return 2 * core + i + 4 * half

    def forward(i, carry):
        at = pl.multiple_of(i * 8, 8)
        items = fft_list(
            [
                (
                    recv1[d, pl.ds(at, 8), :] * inverse,
                    recv1[d, pl.ds(at + 16, 8), :] * inverse,
                )
                for d in range(n)
            ],
            -1.0,
        )
        for k in range(n):
            re, im = turn(*items[k], tc[k : k + 1, :], ts[k : k + 1, :])
            u_ref[k * 8 : k * 8 + 8, :128] = re
            u_ref[k * 8 : k * 8 + 8, 128:] = im
        out = triple_dot((cfh[...], cfl[...]), halves(u_ref[...]), NT)
        for part in range(2):
            for half in range(2):
                start = part * 128 + half * 64
                came[0, part, block(i, half)] = out[start : start + 64]
        return carry

    lax.fori_loop(0, 2, forward, 0)

    def raised(block_before):
        return onto_first(block_before, block_before)

    @pl.when(first_edge)
    def _():
        z_re, z_im = came[0, 0, 0], came[0, 1, 0]
        f_re = raised(turned_block(z_re))
        f_im = -raised(turned_block(z_im))
        first = (lanes_of(z_re.shape) & 7) == 0
        came[0, 0, 0] = jnp.where(first, 0.5 * (z_re + f_re), z_re)
        came[0, 1, 0] = jnp.where(first, 0.5 * (z_im + f_im), z_im)
        edge_send[0] = 0.5 * (z_im - f_im)
        edge_send[1] = -0.5 * (z_re - f_re)

    @pl.when(jnp.logical_and(core == 0, chip > 0))
    def _():
        edge_send[0] = came[0, 0, 0]
        edge_send[1] = came[0, 1, 0]

    def half_copy(half, its_core, peer):
        at = pl.ds(2 * its_core + 4 * half, 2)
        return remote(
            came.at[0, :, at], came.at[0, :, at], core_sem, (0, half, 0), (0, half, 1), peer
        )

    for half in range(2):
        half_copy(half, core, partner).start()

    edge_copy = remote(edge_send, came.at[0, :, 8], ring_sem, (0, 0), (0, 1), around)

    @pl.when(core == 0)
    def _():
        edge_copy.start()

    start_all(weights_to, n // 2 + AHEAD, n - 4)
    start_all(weights_to, 1, n // 2)
    start_all(weights_to, n - 4, n)

    def keep(a, part, value):
        high, low = halves(value)
        at = pl.ds(pl.multiple_of(a * 64, 64), 64)
        own_h[part, at, :] = high
        own_l[part, at, :] = low

    for half in range(2):
        half_copy(half, 1 - core, partner).wait_recv()

    @pl.when(core == 0)
    def _():
        def one(a, carry):
            for part in range(2):
                keep(a, part, came[0, part, a])
            return carry

        lax.fori_loop(0, 8, one, 0)

    @pl.when(core == 1)
    def _():
        edge_copy.wait_recv()

        def one(a, carry):
            for part in range(2):
                keep(a, part, onto_second(came[0, part, a], came[0, part, a + 1]))
            return carry

        lax.fori_loop(0, 8, one, 0)

    def partner_copy(k, a, its_core, peer):
        return remote(
            grid.at[k, :, a],
            came.at[k + 1, :, a + its_core],
            core_sem,
            (k + 1, a, 0),
            (k + 1, a, 1),
            peer,
        )

    def partner_sent(k):
        for a in range(8):
            partner_copy(k, a, core, partner).wait_send()

    def ring_copy(k):
        return remote(
            ring_send.at[k], ring_came.at[k], ring_sem, (k + 1, 0), (k + 1, 1), around
        )

    def pack_ring(k):
        lane = lanes_of((16, 256)) & 7
        packed = jnp.zeros((16, 256), F32)
        for part in range(2):
            value = grid[k, part, 7 * core]
            for four in range(4):
                at = 2 * four + part
                turned = pltpu.roll(value[16 * four : 16 * four + 16], core * ((256 - 2 * at) % 256) + at, 1)
                packed = jnp.where(lane == core * (7 - 2 * at) + at, turned, packed)
        ring_send[k] = packed

    def unpack_ring(k):
        packed = ring_came[k]
        for part in range(2):
            for four in range(4):
                at = 2 * four + part
                came[k + 1, part, 8 * core, 16 * four : 16 * four + 16] = pltpu.roll(
                    packed, core * ((256 - 2 * at) % 256) + at, 1
                )

    def make_ready(g):
        def one(j, carry):
            d = 4 * g + j

            @pl.when(d != me)
            def _():
                weights_to(d, d).wait_recv()

            @pl.when(d == me)
            def _():
                own_w.wait()

            return carry

        lax.fori_loop(0, 4, one, 0)
        value = recv_w[pl.ds(4 * g, 4)].reshape(256, 256)
        for part, ref, flat in zip(halves(value), (wh, wl), (th, tl)):
            moved = jnp.dot(part, square[2 + core], preferred_element_type=F32)
            ref[g] = moved.astype(BF16)
            flat[g] = moved.T.astype(BF16)

    def apply(k, inverse=None):
        for part in range(2):
            for own, out in ((own_h, g_h), (own_l, g_l)):
                out[part] = jnp.dot(
                    oh[...], own[part], preferred_element_type=F32
                ).astype(BF16).reshape(8, 32, 256)

        def group(step, carry):
            g = step
            if k == 0:
                g = crossed(lax.div(me, 4), step, 3)
                make_ready(g)
            left = tuple(
                jnp.concatenate([ref[0, g], ref[1, g]], axis=0) for ref in (g_h, g_l)
            )
            weights = (wh[g], wl[g])
            seen = triple_dot(left, (th[g], tl[g]), NN)
            weight = wm[g]
            if inverse is not None:
                weight = weight * inverse * inverse
            seen = seen * jnp.concatenate([weight, weight], axis=0)
            high, low = halves(triple_dot(halves(seen), weights, NN))
            for ref, value in ((h_h, high), (h_l, low)):
                ref[0, g] = value[:32]
                ref[1, g] = value[32:]
            return carry

        lax.fori_loop(0, 8, group, 0, unroll=1 if k == 0 else 4)
        for part in range(2):
            grid[k, part] = move(
                oht[...], (h_h[part].reshape(256, 256), h_l[part].reshape(256, 256))
            ).reshape(8, 64, 256)
        if k < 2:

            def one(a, carry):
                partner_copy(k, a, core, partner).start()
                return carry

            lax.fori_loop(0, 8, one, 0)
        else:
            for its_core in range(2):

                @pl.when(core == 1 - its_core)
                def _():
                    for a in NEEDED[its_core]:
                        partner_copy(k, a, core, partner).start()

        pack_ring(k)
        ring_copy(k).start()

    def close_edge(k):
        ring_copy(k).wait_recv()
        unpack_ring(k)

        @pl.when(jnp.logical_or(first_edge, last_edge))
        def _():
            came[k + 1, 0, 8 * core] = turned_block(grid[k, 0, 7 * core])
            came[k + 1, 1, 8 * core] = -turned_block(grid[k, 1, 7 * core])

    def combine(k):
        def run(onto, start, last):
            def block(a, total):
                for part in range(2):
                    value = grid[k, part, a] + onto(came[k + 1, part, a], came[k + 1, part, a + 1])
                    value = 0.5 * value
                    keep(a, part, value)
                    if k == 0:
                        total = total + value * value
                return total

            def one(step, total):
                partner_copy(k, step + 1, 1 - core, partner).wait_recv()
                return block(step + start, total)

            partner_copy(k, 0, 1 - core, partner).wait_recv()
            total = lax.fori_loop(0, 7, one, jnp.zeros((64, 256), F32))
            close_edge(k)
            return block(last, total)

        return lax.cond(
            core == 0, lambda: run(onto_first, 1, 0), lambda: run(onto_second, 0, 7)
        )

    def two_lanes(value):
        return jnp.concatenate([value, value], axis=1)

    apply(0)
    put_mark(0, spread_sum(combine(0)))
    apply(1)
    combine(1)
    n1 = get_mark(0)
    inverse = two_lanes(1.0 / n1)
    apply(2, inverse)
    for its_core in range(2):

        @pl.when(core == its_core)
        def _():
            for a in NEEDED[its_core]:
                partner_copy(2, a, 1 - core, partner).wait_recv()

    ring_copy(2).wait_recv()
    unpack_ring(2)


    @pl.when(first_edge)
    def _():
        up = raised(came[3, 0, 0]), raised(came[3, 1, 0])
        edge_last[0] = up[0] + raised(turned_block(up[0]))
        edge_last[1] = up[1] - raised(turned_block(up[1]))

    @pl.when(first_edge)
    def _():
        came[3, 0, 0] = turned_block(grid[2, 0, 0])
        came[3, 1, 0] = -turned_block(grid[2, 1, 0])

    def last_sum(j, total):
        a = 2 * core + lax.rem(j, 2) + 4 * lax.div(j, 2)

        @pl.when(core == 0)
        def _():
            for part in range(2):
                value = grid[2, part, a] + onto_first(came[3, part, a], came[3, part, a + 1])
                grid[0, part, a] = value

        @pl.when(core == 1)
        def _():
            for part in range(2):
                value = came[3, part, a] + onto_first(grid[2, part, a - 1], grid[2, part, a])
                grid[0, part, a] = value

        for part in range(2):
            value = grid[0, part, a]
            total = total + value * value
        return total

    partner_sent(0)
    total = 0.5 * lax.fori_loop(0, 4, last_sum, jnp.zeros((64, 256), F32))
    h0_re, h0_im = grid[0, 0, 0], grid[0, 1, 0]
    alone = jnp.logical_and((lanes_of((64, 256)) & 7) == 0, first_edge)
    z_re = jnp.where(alone, 0.5 * (h0_re - edge_last[1]), h0_re)
    z_im = jnp.where(alone, 0.5 * (h0_im + edge_last[0]), h0_im)

    @pl.when(first_edge)
    def _():
        grid[0, 0, 0] = z_re
        grid[0, 1, 0] = z_im


    def backward(i, carry):
        at = pl.multiple_of(i * 8, 8)
        held = jnp.concatenate(
            [grid[0, part, block(i, half)] for part in range(2) for half in range(2)], axis=0
        )
        u_ref[...] = triple_dot(halves(held.T), (cih[...], cil[...]), NN)
        items = []
        for k in range(n):
            re = u_ref[k * 8 : k * 8 + 8, :128]
            im = u_ref[k * 8 : k * 8 + 8, 128:]
            items.append(turn(re, im, tc[k : k + 1, :], -ts[k : k + 1, :]))
        items = fft_list(items, 1.0)
        for d in range(n):
            send2[d, pl.ds(at, 8), :] = items[d][0]
            send2[d, pl.ds(at + 16, 8), :] = items[d][1]
        return carry

    lax.fori_loop(0, 2, backward, 0)
    recv2[chip * 2 + core] = send2[me]
    start_all(second_to)
    change = z_re * z_re + z_im * z_im - 0.5 * (h0_re * h0_re + h0_im * h0_im)
    third = spread_sum(total + jnp.where(alone, change, 0.0))

    def second_sum(i, sums):
        at = pl.ds(pl.multiple_of(i * 64, 64), 64)
        for part in range(2):
            value = own_h[part, at, :].astype(F32) + own_l[part, at, :].astype(F32)
            value = value * inverse
            sums = sums + value * value
        return sums

    second = spread_sum(lax.fori_loop(0, 8, second_sum, jnp.zeros((64, 256), F32)))
    put_mark(1, jnp.where(lanes_of((1, 128)) < 64, second, third))
    all_extras.wait_send()
    all_weights.wait_send()
    all_first.wait_send()
    all_marks(0).wait_send()
    for half in range(2):
        half_copy(half, core, partner).wait_send()

    @pl.when(core == 0)
    def _():
        edge_copy.wait_send()

    partner_sent(1)
    for its_core in range(2):

        @pl.when(core == 1 - its_core)
        def _():
            for a in NEEDED[its_core]:
                partner_copy(2, a, core, partner).wait_send()

    for k in range(3):
        ring_copy(k).wait_send()
    all_second.wait_recv()

    def back_chunk(i, carry):
        at = pl.multiple_of(i * 8, 8)
        its_core = lax.div(i, 2)
        to = pl.multiple_of(lax.rem(i, 2) * 8, 8)
        items = [
            (recv2[o * 2 + its_core, pl.ds(to, 8), :], recv2[o * 2 + its_core, pl.ds(to + 16, 8), :])
            for o in range(n // 2)
        ]
        row = lax.broadcasted_iota(jnp.int32, (8, 128), 0) + at
        lane = lanes_of((8, 128))
        extra = jnp.where(jnp.logical_and(row == 0, lane < 64), items[0][1], 0.0)
        even = fft_list(items, 1.0)
        odd = []
        for o, (re, im) in enumerate(items):
            angle = 2.0 * math.pi * o / n
            odd.append((re, im) if o == 0 else turn(re, im, math.cos(angle), math.sin(angle)))
        odd = fft_list(odd, 1.0)
        items = []
        for k in range(n // 2):
            items.append((even[k][0] + extra, even[k][1]))
            items.append((odd[k][0] - extra, odd[k][1]))
        items = [
            turn(*items[q], rtc[q, pl.ds(at, 8), :], -rts[q, pl.ds(at, 8), :]) for q in range(n)
        ]
        for pair in range(n // 2):
            lanes = slice(pair * 128, (pair + 1) * 128)
            for part in range(2):
                x0, x1 = swap_halves(items[2 * pair][part], items[2 * pair + 1][part])
                b_ref[pl.ds(at + part * 64, 8), lanes] = x0
                b_ref[pl.ds(at + part * 64 + rows, 8), lanes] = x1
        return carry

    lax.fori_loop(0, 4, back_chunk, 0)
    both = get_mark(1)
    n2, n3 = jnp.full((1, 128), both[0, 0], F32), jnp.full((1, 128), both[0, 64], F32)
    factor = float(image.shape[1]) / n3
    factor = jnp.concatenate([factor] * 4, axis=1)
    for at in range(0, n, 8):
        lanes = slice(at * 64, at * 64 + 512)
        part = triple_dot((row_i[0], row_i[1]), halves(b_ref[:, lanes]), NN) * factor
        for q in range(8):
            tall_ref[pl.ds(at + q, 64, stride=n), :] = part[:, q * 64 : q * 64 + 64]
    for lane in range(0, image.shape[1], 128):
        y_ref[:, lane : lane + 128] = tall_ref[lane : lane + 128, :].T
    third = n3 * n1 / n2
    for at, value in enumerate((n1, n2, third)):
        norm_ref[at] = value[0, 0]
    all_second.wait_send()
    all_marks(1).wait_send()


def tables(n, row_count, length):
    half = row_count // 2
    scale = 1.0 / math.sqrt(length)
    local = np.arange(row_count)
    angle = -2.0 * np.pi * np.outer(local, local) / row_count
    c, s = np.cos(angle) * scale, np.sin(angle) * scale
    two = np.eye(2)
    col_f = np.block([[np.kron(two, c), np.kron(two, -s)], [np.kron(two, s), np.kron(two, c)]])
    col_i = col_f
    row_f = np.concatenate([c, s], axis=0)
    row_i = np.concatenate([c, s], axis=1)
    index = np.arange(n)
    turns = -2.0 * np.pi * np.outer(index, np.tile(local, 2)) / length
    u = np.arange(half)[:, None] + half * (np.arange(2 * row_count)[None, :] // row_count)
    row_turns = -2.0 * np.pi * index[:, None, None] * u[None] / length
    return col_f, col_i, row_f, row_i, turns, row_turns


def fast_device(image0, interp, vis_weight, counts, tile_index):
    n_chan = lax.axis_size("chan")
    n = lax.axis_size("base") * n_chan
    row_count, length = image0.shape
    touch = tile_index.shape[2]
    each = touch // n
    vcap, cells = interp.shape[3:]
    col_f, col_i, row_f, row_i, turns, row_turns = tables(n, row_count, length)
    cfh, cfl = np_halves(col_f)
    rows_f, rows_i = np.stack(np_halves(row_f)), np.stack(np_halves(row_i))
    column_turns = np.stack([np.cos(turns), np.sin(turns)]).astype(np.float32)
    row_turns = np.stack([np.cos(row_turns), np.sin(row_turns)]).astype(np.float32)
    order = np.arange(cells).reshape(TILE_V, TILE_U).T.reshape(-1)
    perm = np.zeros((2, cells, cells), np.float32)
    perm[0, order, np.arange(cells)] = 1.0
    perm[1] = perm[0][:, ::-1]
    perm = perm.astype(jnp.bfloat16)
    square = np.concatenate([np.stack([cfh, cfl]), perm])
    matrices = interp.reshape(n, each * vcap, cells)
    weight = vis_weight.reshape(touch, vcap).T
    count = counts.reshape(1, touch)
    tile = tile_index.reshape(1, touch)

    def dma(*shape):
        return pltpu.SemaphoreType.DMA(shape)

    message = (n, 32, 128)
    wide = (8, 64, 256)
    image, norms = pl.pallas_call(
        lambda *refs: main_kernel(n, n_chan, *refs),
        out_shape=[
            jax.ShapeDtypeStruct((row_count, length), F32),
            jax.ShapeDtypeStruct((3,), F32),
        ],
        in_specs=[HBM_SPEC] * 10,
        out_specs=[VMEM_SPEC, SMEM_SPEC],
        scratch_shapes=[
            pltpu.VMEM((row_count, length), F32),
            pltpu.VMEM((length, row_count), F32),
            pltpu.VMEM(weight.shape, F32),
            pltpu.VMEM(count.shape, jnp.int32),
            pltpu.VMEM(tile.shape, jnp.int32),
            pltpu.VMEM(row_turns.shape, F32),
            pltpu.VMEM(square.shape, BF16),
            pltpu.VMEM(column_turns.shape, F32),
            pltpu.VMEM(rows_f.shape, BF16),
            pltpu.VMEM(rows_i.shape, BF16),
            pltpu.VMEM((n, 8, 128), F32),
            pltpu.VMEM((2 * row_count, length), F32),
            pltpu.VMEM(message, F32),
            pltpu.VMEM(message, F32),
            pltpu.VMEM(message, F32),
            pltpu.VMEM(message, F32),
            pltpu.VMEM((n, each * vcap, cells), F32),
            pltpu.VMEM((n, 8, 128), F32),
            pltpu.VMEM((2, 1, 128), F32),
            pltpu.VMEM((2, n, 1, 128), F32),
            pltpu.VMEM((8, cells, cells), BF16),
            pltpu.VMEM((8, cells, cells), BF16),
            pltpu.VMEM((8, cells, cells), BF16),
            pltpu.VMEM((8, cells, cells), BF16),
            pltpu.VMEM((8, 32, cells), F32),
            pltpu.VMEM((touch, 512), BF16),
            pltpu.VMEM((512, touch), BF16),
            pltpu.VMEM((2, 512, cells), BF16),
            pltpu.VMEM((2, 512, cells), BF16),
            pltpu.VMEM((2, 8, 32, cells), BF16),
            pltpu.VMEM((2, 8, 32, cells), BF16),
            pltpu.VMEM((2, 8, 32, cells), BF16),
            pltpu.VMEM((2, 8, 32, cells), BF16),
            pltpu.VMEM((3, 2, 8, 64, cells), F32),
            pltpu.VMEM((4, 2, 9, 64, cells), F32),
            pltpu.VMEM((2, 64, cells), F32),
            pltpu.VMEM((2, 64, cells), F32),
            pltpu.VMEM((3, 16, cells), F32),
            pltpu.VMEM((3, 16, cells), F32),
            pltpu.VMEM((256, 256), F32),
            dma(1),
            dma(n),
            dma(2),
            dma(2),
            dma(2),
            dma(4, 2),
            dma(4, 8, 2),
            dma(4, 2),
            dma(10),
        ],
        compiler_params=pltpu.CompilerParams(
            has_side_effects=True, collective_id=0, vmem_limit_bytes=67043328
        ),
    )(
        image0,
        matrices,
        weight,
        count,
        tile,
        jnp.asarray(row_turns),
        jnp.asarray(square),
        column_turns,
        rows_f,
        rows_i,
    )
    return image, norms


def per_device(image0, interp, vis_weight, counts, tile_index):
    n = lax.axis_size("base") * lax.axis_size("chan")
    row_count, length = image0.shape
    vcap, cells = interp.shape[3:]
    touch = tile_index.shape[2]
    fits = (n, row_count, length // row_count) == (TILE_U, 64, TILE_U)
    if fits and (vcap, cells, touch % 256) == (8, 256, 0) and touch // n == 8:
        return fast_device(image0, interp, vis_weight, counts, tile_index)
    return general_device(image0, interp, vis_weight, counts, tile_index)


def solution(mesh):
    placed = (
        P(("base", "chan"), None),
        P("base", "chan", None, None, None),
        P("base", "chan", None, None),
        P("base", "chan", None),
        P("base", "chan", None),
    )
    return jax.shard_map(
        per_device,
        mesh=mesh,
        in_specs=placed,
        out_specs=(P(("base", "chan"), None), P()),
        check_vma=False,
    )
```

```python
import math

import jax
import jax.numpy as jnp
import numpy as np
from jax import lax
from jax.experimental import pallas as pl
from jax.experimental.pallas import tpu as pltpu
from jax.sharding import PartitionSpec as P

TILE_V = 8
TILE_U = 32
ITERS = 3


PRECISION_LEVEL = lax.Precision.HIGHEST


def split_length(length):
    outer_len = 2 ** ((length.bit_length() - 1) // 2)
    return (outer_len, length // outer_len)


def angle_table(count_a, count_b, modulus, sign):
    left = jnp.arange(count_a, dtype=jnp.int32)[:, None]
    right = jnp.arange(count_b, dtype=jnp.int32)[None, :]
    angle = sign * 2.0 * math.pi / modulus * (left * right % modulus).astype(jnp.float32)
    return (jnp.cos(angle), jnp.sin(angle))


def transform_rows(real_part, imag_part, sign):
    row_count, length = real_part.shape
    outer_len, inner_len = split_length(length)
    cos_q, sin_q = angle_table(inner_len, inner_len, inner_len, sign)
    cos_t, sin_t = angle_table(inner_len, outer_len, length, sign)
    cos_p, sin_p = angle_table(outer_len, outer_len, outer_len, sign)
    real_in = real_part.reshape(row_count, inner_len, outer_len)
    first_re = jnp.einsum("kq,rqp->rkp", cos_q, real_in, precision=PRECISION_LEVEL)
    first_im = jnp.einsum("kq,rqp->rkp", sin_q, real_in, precision=PRECISION_LEVEL)
    if imag_part is not None:
        imag_in = imag_part.reshape(row_count, inner_len, outer_len)
        first_re = first_re - jnp.einsum("kq,rqp->rkp", sin_q, imag_in, precision=PRECISION_LEVEL)
        first_im = first_im + jnp.einsum("kq,rqp->rkp", cos_q, imag_in, precision=PRECISION_LEVEL)
    turned_re = first_re * cos_t - first_im * sin_t
    turned_im = first_re * sin_t + first_im * cos_t
    last_re = jnp.einsum("jp,rkp->rjk", cos_p, turned_re, precision=PRECISION_LEVEL) - jnp.einsum(
        "jp,rkp->rjk", sin_p, turned_im, precision=PRECISION_LEVEL
    )
    last_im = jnp.einsum("jp,rkp->rjk", cos_p, turned_im, precision=PRECISION_LEVEL) + jnp.einsum(
        "jp,rkp->rjk", sin_p, turned_re, precision=PRECISION_LEVEL
    )
    factor = 1.0 / math.sqrt(length)
    return (
        last_re.reshape(row_count, length) * factor,
        last_im.reshape(row_count, length) * factor,
    )


def transpose_global(real_part, imag_part):
    row_count, length = real_part.shape
    n_base = lax.axis_size("base")
    n_chan = lax.axis_size("chan")
    width = length // (n_base * n_chan)
    moved = (
        lax.all_to_all(
            lax.all_to_all(
                real_part.reshape(1, row_count, n_base, n_chan, width),
                "base",
                split_axis=2,
                concat_axis=0,
                tiled=True,
            ),
            "chan",
            split_axis=3,
            concat_axis=1,
            tiled=True,
        ),
        lax.all_to_all(
            lax.all_to_all(
                imag_part.reshape(1, row_count, n_base, n_chan, width),
                "base",
                split_axis=2,
                concat_axis=0,
                tiled=True,
            ),
            "chan",
            split_axis=3,
            concat_axis=1,
            tiled=True,
        ),
    )
    return (moved[0].reshape(length, width).T, moved[1].reshape(length, width).T)


def to_tiles(plane):
    row_count, length = plane.shape
    shaped = plane.reshape(row_count // TILE_V, TILE_V, length // TILE_U, TILE_U)
    return shaped.transpose(0, 2, 1, 3).reshape(-1, TILE_V * TILE_U)


def from_tiles(tiles, row_count, length):
    shaped = tiles.reshape(row_count // TILE_V, length // TILE_U, TILE_V, TILE_U)
    return shaped.transpose(0, 2, 1, 3).reshape(row_count, length)


def slot_work(sample_weights, masked_weight, sample_values):
    visible_samples = (
        jnp.einsum("gnz,gez->gen", sample_weights, sample_values, precision=PRECISION_LEVEL)
        * masked_weight[:, None, :]
    )
    return jnp.einsum("hbi,hyb->hyi", sample_weights, visible_samples, precision=PRECISION_LEVEL)


def total_squares(image):
    return lax.psum(jnp.sum(image * image), ("base", "chan"))


def general_device(image0, interp, vis_weight, counts, tile_index):
    n_base = lax.axis_size("base")
    n_chan = lax.axis_size("chan")
    row_count, length = image0.shape
    touch = tile_index.shape[2]
    slots_each = touch // (n_base * n_chan)
    vcap = interp.shape[3]
    cells = interp.shape[4]
    tiles_own = row_count // TILE_V * (length // TILE_U)
    live = (jnp.arange(vcap, dtype=jnp.int32)[None, :] < counts.reshape(touch, 1)).astype(
        jnp.float32
    )
    masked_weight = vis_weight.reshape(touch, vcap) * live
    sample_weights = interp.reshape(touch, vcap, cells)
    wanted = lax.all_to_all(
        lax.all_to_all(
            tile_index.reshape(n_base, n_chan, slots_each),
            "base",
            split_axis=0,
            concat_axis=0,
            tiled=True,
        ),
        "chan",
        split_axis=1,
        concat_axis=1,
        tiled=True,
    ).reshape(touch)
    onehot = (jnp.arange(tiles_own, dtype=jnp.int32)[:, None] == wanted[None, :]).astype(
        jnp.float32
    )
    moved = (
        lax.all_to_all(
            lax.all_to_all(
                sample_weights.reshape(n_base, n_chan, slots_each, vcap, cells),
                "base",
                split_axis=0,
                concat_axis=0,
                tiled=True,
            ),
            "chan",
            split_axis=1,
            concat_axis=1,
            tiled=True,
        ),
        lax.all_to_all(
            lax.all_to_all(
                masked_weight.reshape(n_base, n_chan, slots_each, vcap),
                "base",
                split_axis=0,
                concat_axis=0,
                tiled=True,
            ),
            "chan",
            split_axis=1,
            concat_axis=1,
            tiled=True,
        ),
    )
    sample_weights = moved[0].reshape(touch, vcap, cells)
    masked_weight = moved[1].reshape(touch, vcap)
    found = []
    current = image0 / jnp.sqrt(total_squares(image0))
    for iteration in range(ITERS):
        real_part, imag_part = transform_rows(current, None, -1.0)
        real_part, imag_part = transpose_global(real_part, imag_part)
        real_part, imag_part = transform_rows(real_part, imag_part, -1.0)
        tiles = jnp.stack([to_tiles(real_part), to_tiles(imag_part)], axis=1)
        sample_values = jnp.take(tiles, wanted, axis=0)
        gridded_plane = slot_work(sample_weights, masked_weight, sample_values)
        summed = jnp.einsum("ts,skc->tkc", onehot, gridded_plane, precision=PRECISION_LEVEL)
        real_part = from_tiles(summed[:, 0, :], row_count, length)
        imag_part = from_tiles(summed[:, 1, :], row_count, length)
        real_part, imag_part = transform_rows(real_part, imag_part, 1.0)
        real_part, imag_part = transpose_global(real_part, imag_part)
        real_part, imag_part = transform_rows(real_part, imag_part, 1.0)
        norm_value = jnp.sqrt(total_squares(real_part))
        found.append(norm_value)
        current = real_part / norm_value
    return (float(length) * current, jnp.stack(found))


F32 = jnp.float32
BF16 = jnp.bfloat16
VMEM_SPEC = pl.BlockSpec(memory_space=pltpu.VMEM)
SMEM_SPEC = pl.BlockSpec(memory_space=pltpu.SMEM)
BIG = pltpu.CompilerParams(vmem_limit_bytes=48 * 1024 * 1024)


def halves(value):
    high = value.astype(BF16)
    return high, (value - high.astype(F32)).astype(BF16)


def np_halves(table):
    high = np.asarray(table, np.float32).astype(jnp.bfloat16)
    low = (np.asarray(table, np.float64) - high.astype(np.float64)).astype(jnp.bfloat16)
    return high, low


def triple_dot(left, right, dims):
    def one(a, b):
        return lax.dot_general(a, b, (dims, ((), ())), preferred_element_type=F32)

    return one(left[0], right[0]) + (one(left[0], right[1]) + one(left[1], right[0]))


def fft_list(items, sign):
    count = len(items)
    if count == 1:
        return items
    even = fft_list(items[0::2], sign)
    odd = fft_list(items[1::2], sign)
    low, high = [], []
    for k in range(count // 2):
        re, im = odd[k]
        if k == 0:
            t_re, t_im = re, im
        elif 4 * k == count:
            t_re, t_im = (im, -re) if sign < 0 else (-im, re)
        else:
            angle = sign * 2.0 * math.pi * k / count
            c, s = math.cos(angle), math.sin(angle)
            t_re, t_im = re * c - im * s, re * s + im * c
        e_re, e_im = even[k]
        low.append((e_re + t_re, e_im + t_im))
        high.append((e_re - t_re, e_im - t_im))
    return low + high


AHEAD = 4
NEEDED = ((0, 3, 4, 1, 5), (2, 3, 6, 7))
HBM_SPEC = pl.BlockSpec(memory_space=pltpu.HBM)
NT = ((1,), (1,))
NN = ((1,), (0,))


def turn(re, im, c, s):
    return re * c - im * s, re * s + im * c


def swap_halves(x0, x1):
    half = x0.shape[1] // 2
    left = lax.broadcasted_iota(jnp.int32, x0.shape, 1) < half
    return (
        jnp.where(left, x0, pltpu.roll(x1, half, 1)),
        jnp.where(left, pltpu.roll(x0, half, 1), x1),
    )


def move(table, parts, dims=NN):
    def one(part):
        return lax.dot_general(table, part, (dims, ((), ())), preferred_element_type=F32)

    return one(parts[0]) + one(parts[1])


def bit_of(p, bit):
    return lax.rem(lax.div(p, 2**bit), 2)


def walk(z, w):
    odd = lax.rem(w, 2)
    return 4 * w + z + odd * (3 - 2 * z)


def chip_of(p):
    x, y = bit_of(p, 2), bit_of(p, 0)
    return walk(lax.div(p, 8), 3 * x + y - 2 * x * y), bit_of(p, 1)


def device_of(chip, core):
    w, at = lax.div(chip, 4), lax.rem(chip, 4)
    odd = lax.rem(w, 2)
    z = at + odd * (3 - 2 * at)
    x = lax.div(w, 2)
    y = odd + x - 2 * x * odd
    return ((z * 2 + x) * 2 + core) * 2 + y


def crossed(p, step, bits):
    value = p + step
    for bit in range(bits):
        value = value - 2 ** (bit + 1) * bit_of(p, bit) * bit_of(step, bit)
    return value


def turned_block(block):
    rows, lanes = block.shape

    def anti(size):
        total = lax.broadcasted_iota(jnp.int32, (size, size), 0) + lax.broadcasted_iota(
            jnp.int32, (size, size), 1
        )
        return (total == size - 1).astype(F32).astype(BF16)

    half = move(anti(rows), halves(block))
    high, low = halves(half)
    table = anti(lanes)

    def one(part):
        return jnp.dot(part, table, preferred_element_type=F32)

    return one(high) + one(low)


def lanes_of(shape):
    return lax.broadcasted_iota(jnp.int32, shape, 1)


def onto_first(low, high):
    lane = lanes_of((low.shape[0], 128))
    column = lane & 7
    high = [pltpu.roll(high[:, at : at + 128], 9, 1) for at in (0, 128)]
    low = [pltpu.roll(low[:, at : at + 128], 1, 1) for at in (0, 128)]
    left = jnp.where(
        column > 0,
        jnp.where(lane < 8, high[1], high[0]),
        jnp.where(lane < 8, low[1], low[0]),
    )
    right = jnp.where(
        column > 0,
        jnp.where(lane < 8, high[0], high[1]),
        jnp.where(lane < 8, low[0], low[1]),
    )
    left = jnp.where(lane >= 8, left, pltpu.roll(left, 1, 0))
    return jnp.concatenate([left, right], axis=1)


def onto_second(low, high):
    rows = low.shape[0]
    lane = lanes_of((rows, 128))
    column = lane & 7
    low = [pltpu.roll(low[:, at : at + 128], 119, 1) for at in (0, 128)]
    high = [pltpu.roll(high[:, at : at + 128], 127, 1) for at in (0, 128)]
    left = jnp.where(
        column < 7,
        jnp.where(lane >= 120, low[1], low[0]),
        jnp.where(lane >= 120, high[1], high[0]),
    )
    right = jnp.where(
        column < 7,
        jnp.where(lane >= 120, low[0], low[1]),
        jnp.where(lane >= 120, high[0], high[1]),
    )
    right = jnp.where(lane < 120, right, pltpu.roll(right, rows - 1, 0))
    return jnp.concatenate([left, right], axis=1)


def main_kernel(
    n,
    n_chan,
    image_hbm,
    w_hbm,
    weight_hbm,
    count_hbm,
    tile_hbm,
    turns_hbm,
    square_hbm,
    tct_hbm,
    row_f_hbm,
    row_i_hbm,
    y_ref,
    norm_ref,
    image,
    tall_ref,
    weight_ref,
    count_ref,
    tile_ref,
    turns,
    square,
    tct,
    row_f,
    row_i,
    x_ref,
    b_ref,
    send1,
    recv1,
    send2,
    recv2,
    recv_w,
    recv_x,
    mark_send,
    mark_recv,
    wh,
    wl,
    th,
    tl,
    wm,
    oh,
    oht,
    own_h,
    own_l,
    g_h,
    g_l,
    h_h,
    h_l,
    grid,
    came,
    edge_send,
    edge_last,
    ring_send,
    ring_came,
    u_ref,
    w_send,
    w_recv,
    x_sem,
    d1_sem,
    d2_sem,
    m_sem,
    core_sem,
    ring_sem,
    own_sem,
):
    base, chan = lax.axis_index("base"), lax.axis_index("chan")
    me = base * n_chan + chan
    chip, core = chip_of(me)
    chips = n // 2
    rows = 32
    partner = device_of(chip, 1 - core)
    around = device_of(lax.rem(chip + chips + 2 * core - 1, chips), 1 - core)
    first_edge = jnp.logical_and(core == 0, chip == 0)
    last_edge = jnp.logical_and(core == 1, chip == chips - 1)

    def place(p):
        return (lax.div(p, n_chan), lax.rem(p, n_chan))

    def remote(src, dst, sems, out_index, in_index, peer):
        return pltpu.make_async_remote_copy(
            src_ref=src,
            dst_ref=dst,
            send_sem=sems.at[out_index],
            recv_sem=sems.at[in_index],
            device_id=place(peer),
            device_id_type=pl.DeviceIdType.MESH,
        )

    def block_of(p):
        its_chip, its_core = chip_of(p)
        return its_chip + its_core * (n - 1 - 2 * its_chip)

    def weights_to(p, arrives):
        return pltpu.make_async_remote_copy(
            src_ref=w_hbm.at[block_of(p)],
            dst_ref=recv_w.at[arrives],
            send_sem=w_send.at[0],
            recv_sem=w_recv.at[arrives],
            device_id=place(p),
            device_id_type=pl.DeviceIdType.MESH,
        )

    def extras_to(p, arrives):
        return remote(x_ref.at[block_of(p)], recv_x.at[arrives], x_sem, 0, 1, p)

    def first_to(p, arrives):
        its_chip, its_core = chip_of(p)
        return remote(send1.at[its_chip * 2 + its_core], recv1.at[arrives], d1_sem, 0, 1, p)

    def second_to(p, arrives):
        its_chip, its_core = chip_of(arrives)
        return remote(send2.at[p], recv2.at[its_chip * 2 + its_core], d2_sem, 0, 1, p)

    def mark_to(k):
        return lambda p, arrives: remote(
            mark_send.at[k], mark_recv.at[k, arrives], m_sem, (k, 0), (k, 1), p
        )

    def start_all(make, low=1, high=n):
        def body(step, carry):
            make(crossed(me, step, 5), me).start()
            return carry

        lax.fori_loop(low, high, body, 0)

    others = pl.ds(0, n - 1)

    def all_of(sent, landed, sems, out_index, in_index):
        return remote(sent.at[others], landed.at[others], sems, out_index, in_index, partner)

    all_weights = pltpu.make_async_remote_copy(
        src_ref=w_hbm.at[others],
        dst_ref=recv_w.at[others],
        send_sem=w_send.at[0],
        recv_sem=w_recv.at[0],
        device_id=place(partner),
        device_id_type=pl.DeviceIdType.MESH,
    )
    all_extras = all_of(x_ref, recv_x, x_sem, 0, 1)
    all_first = all_of(send1, recv1, d1_sem, 0, 1)
    all_second = all_of(send2, recv2, d2_sem, 0, 1)

    def all_marks(k):
        return all_of(mark_recv.at[k], mark_recv.at[k], m_sem, (k, 0), (k, 1))

    def put_mark(k, total):
        mark_send[k] = total
        mark_recv[k, me] = total
        start_all(mark_to(k))

    def get_mark(k):
        all_marks(k).wait_recv()
        return jnp.sqrt(jnp.sum(mark_recv[k], axis=0))

    def spread_sum(value):
        return jnp.full((1, 128), jnp.sum(value), F32)

    own_w = pltpu.make_async_copy(w_hbm.at[block_of(me)], recv_w.at[me], own_sem.at[0])
    loads = [
        pltpu.make_async_copy(src, dst, own_sem.at[1 + at])
        for at, (src, dst) in enumerate(
            (
                (image_hbm, image),
                (row_f_hbm, row_f),
                (turns_hbm, turns),
                (weight_hbm, weight_ref),
                (count_hbm, count_ref),
                (tile_hbm, tile_ref),
                (square_hbm, square),
                (tct_hbm, tct),
                (row_i_hbm, row_i),
            )
        )
    ]
    for load in loads:
        load.start()
    own_w.start()
    barrier = pltpu.get_barrier_semaphore()

    def greet(step, carry):
        peer = crossed(me, step, 5)
        pl.semaphore_signal(
            barrier, inc=1, device_id=place(peer), device_id_type=pl.DeviceIdType.MESH
        )
        return carry

    lax.fori_loop(1, n, greet, 0)
    rtc, rts = turns.at[0], turns.at[1]
    tc, ts = tct.at[0], tct.at[1]
    cfh, cfl = square.at[0], square.at[1]
    cih, cil = cfh, cfl

    loads[0].wait()
    loads[1].wait()
    total = jnp.zeros((8, 128), F32)
    for lane in range(0, image.shape[1], 128):
        part = image[:, lane : lane + 128]
        tall_ref[lane : lane + 128, :] = part.T
        square_of = part * part
        for row in range(0, 64, 8):
            total = total + square_of[row : row + 8]
    for at in range(0, n, 8):
        part = jnp.concatenate(
            [tall_ref[pl.ds(at + q, 64, stride=n), :] for q in range(8)], axis=1
        )
        b_ref[:, at * 64 : at * 64 + 512] = triple_dot((row_f[0], row_f[1]), halves(part), NN)

    def row_chunk(i, carry):
        at = pl.multiple_of(i * 8, 8)
        items = [[None, None] for _ in range(n)]
        for pair in range(n // 2):
            lanes = slice(pair * 128, (pair + 1) * 128)
            for part in range(2):
                x0 = b_ref[pl.ds(at + part * 64, 8), lanes]
                x1 = b_ref[pl.ds(at + part * 64 + rows, 8), lanes]
                items[2 * pair][part], items[2 * pair + 1][part] = swap_halves(x0, x1)
        items = [
            turn(*items[q], tc_q, ts_q)
            for q, (tc_q, ts_q) in enumerate(
                (rtc[q, pl.ds(at, 8), :], rts[q, pl.ds(at, 8), :]) for q in range(n)
            )
        ]
        items = fft_list(items, -1.0)
        row = lax.broadcasted_iota(jnp.int32, (8, 128), 0) + at
        lane = lanes_of((8, 128))
        alone = jnp.logical_and(row == 0, lane < 64)
        items[0] = (items[0][0], jnp.where(alone, items[n // 2][0], items[0][1]))
        its_core = lax.div(i, 2)
        to = pl.multiple_of(lax.rem(i, 2) * 8, 8)
        for o in range(n // 2):
            send1[o * 2 + its_core, pl.ds(to, 8), :] = items[o][0]
            send1[o * 2 + its_core, pl.ds(to + 16, 8), :] = items[o][1]
        return carry

    for load in loads[2:]:
        load.wait()
    vis = lax.broadcasted_iota(jnp.int32, (8, 256), 0)
    live = jnp.where(vis < count_ref[...], weight_ref[...], 0.0)
    tile = jnp.broadcast_to(tile_ref[...].astype(F32), (8, 256))
    squares = jnp.full((8, 256), jnp.sum(total), F32)
    slots = jnp.concatenate([live, tile, squares, jnp.zeros((104, 256), F32)], axis=0).T
    x_ref[...] = slots.reshape(n, 8, 128)
    recv_x[me] = x_ref[block_of(me)]
    lax.fori_loop(0, 4, row_chunk, 0)
    recv1[me] = send1[chip * 2 + core]

    pl.semaphore_wait(barrier, n - 1)
    start_all(first_to)
    start_all(extras_to)
    start_all(weights_to, n // 2, n // 2 + AHEAD)

    all_extras.wait_recv()
    slots = recv_x[...].reshape(256, 128)
    inverse = jnp.full((1, 128), jnp.sum(recv_x[:, 0:1, 16:17]), F32)
    inverse = 1.0 / jnp.sqrt(inverse)
    tall = jnp.broadcast_to(slots[:, 8:9], (256, 256))
    tall = jnp.where(core == 0, tall, 511.0 - tall)
    wide = tall.T
    for at in range(0, 512, 256):
        down = (lax.broadcasted_iota(jnp.int32, (256, 256), 0) + at).astype(F32)
        along = (lanes_of((256, 256)) + at).astype(F32)
        oht[at : at + 256, :] = (wide == down).astype(F32).astype(BF16)
        oh[:, at : at + 256] = (tall == along).astype(F32).astype(BF16)
    spread = lax.broadcasted_iota(jnp.int32, (128, 256), 0) == (lanes_of((128, 256)) & 7)
    spread = spread.astype(F32).astype(BF16)
    high, low = halves(slots)
    rest = (slots - high.astype(F32) - low.astype(F32)).astype(BF16)
    value = jnp.dot(high, spread, preferred_element_type=F32) + (
        jnp.dot(low, spread, preferred_element_type=F32)
        + jnp.dot(rest, spread, preferred_element_type=F32)
    )
    slot = (lax.broadcasted_iota(jnp.int32, (256, 256), 0) & 31)
    wm[...] = jnp.where(slot == lax.shift_right_logical(lanes_of((256, 256)), 3), value, 0.0).reshape(8, 32, 256)

    all_first.wait_recv()

    def block(i, half):
        return 2 * core + i + 4 * half

    def forward(i, carry):
        at = pl.multiple_of(i * 8, 8)
        items = fft_list(
            [
                (
                    recv1[d, pl.ds(at, 8), :] * inverse,
                    recv1[d, pl.ds(at + 16, 8), :] * inverse,
                )
                for d in range(n)
            ],
            -1.0,
        )
        for k in range(n):
            re, im = turn(*items[k], tc[k : k + 1, :], ts[k : k + 1, :])
            u_ref[k * 8 : k * 8 + 8, :128] = re
            u_ref[k * 8 : k * 8 + 8, 128:] = im
        out = triple_dot((cfh[...], cfl[...]), halves(u_ref[...]), NT)
        for part in range(2):
            for half in range(2):
                start = part * 128 + half * 64
                came[0, part, block(i, half)] = out[start : start + 64]
        return carry

    lax.fori_loop(0, 2, forward, 0)

    def raised(block_before):
        return onto_first(block_before, block_before)

    @pl.when(first_edge)
    def _():
        z_re, z_im = came[0, 0, 0], came[0, 1, 0]
        f_re = raised(turned_block(z_re))
        f_im = -raised(turned_block(z_im))
        first = (lanes_of(z_re.shape) & 7) == 0
        came[0, 0, 0] = jnp.where(first, 0.5 * (z_re + f_re), z_re)
        came[0, 1, 0] = jnp.where(first, 0.5 * (z_im + f_im), z_im)
        edge_send[0] = 0.5 * (z_im - f_im)
        edge_send[1] = -0.5 * (z_re - f_re)

    @pl.when(jnp.logical_and(core == 0, chip > 0))
    def _():
        edge_send[0] = came[0, 0, 0]
        edge_send[1] = came[0, 1, 0]

    def half_copy(half, its_core, peer):
        at = pl.ds(2 * its_core + 4 * half, 2)
        return remote(
            came.at[0, :, at], came.at[0, :, at], core_sem, (0, half, 0), (0, half, 1), peer
        )

    for half in range(2):
        half_copy(half, core, partner).start()

    edge_copy = remote(edge_send, came.at[0, :, 8], ring_sem, (0, 0), (0, 1), around)

    @pl.when(core == 0)
    def _():
        edge_copy.start()

    start_all(weights_to, n // 2 + AHEAD, n - 4)
    start_all(weights_to, 1, n // 2)
    start_all(weights_to, n - 4, n)

    def keep(a, part, value):
        high, low = halves(value)
        at = pl.ds(pl.multiple_of(a * 64, 64), 64)
        own_h[part, at, :] = high
        own_l[part, at, :] = low

    for half in range(2):
        half_copy(half, 1 - core, partner).wait_recv()

    @pl.when(core == 0)
    def _():
        def one(a, carry):
            for part in range(2):
                keep(a, part, came[0, part, a])
            return carry

        lax.fori_loop(0, 8, one, 0)

    @pl.when(core == 1)
    def _():
        edge_copy.wait_recv()

        def one(a, carry):
            for part in range(2):
                keep(a, part, onto_second(came[0, part, a], came[0, part, a + 1]))
            return carry

        lax.fori_loop(0, 8, one, 0)

    def partner_copy(k, a, its_core, peer):
        return remote(
            grid.at[k, :, a],
            came.at[k + 1, :, a + its_core],
            core_sem,
            (k + 1, a, 0),
            (k + 1, a, 1),
            peer,
        )

    def partner_sent(k):
        for a in range(8):
            partner_copy(k, a, core, partner).wait_send()

    def ring_copy(k):
        return remote(
            ring_send.at[k], ring_came.at[k], ring_sem, (k + 1, 0), (k + 1, 1), around
        )

    def pack_ring(k):
        lane = lanes_of((16, 256)) & 7
        packed = jnp.zeros((16, 256), F32)
        for part in range(2):
            value = grid[k, part, 7 * core]
            for four in range(4):
                at = 2 * four + part
                turned = pltpu.roll(value[16 * four : 16 * four + 16], core * ((256 - 2 * at) % 256) + at, 1)
                packed = jnp.where(lane == core * (7 - 2 * at) + at, turned, packed)
        ring_send[k] = packed

    def unpack_ring(k):
        packed = ring_came[k]
        for part in range(2):
            for four in range(4):
                at = 2 * four + part
                came[k + 1, part, 8 * core, 16 * four : 16 * four + 16] = pltpu.roll(
                    packed, core * ((256 - 2 * at) % 256) + at, 1
                )

    def make_ready(g):
        def one(j, carry):
            d = 4 * g + j

            @pl.when(d != me)
            def _():
                weights_to(d, d).wait_recv()

            @pl.when(d == me)
            def _():
                own_w.wait()

            return carry

        lax.fori_loop(0, 4, one, 0)
        value = recv_w[pl.ds(4 * g, 4)].reshape(256, 256)
        for part, ref, flat in zip(halves(value), (wh, wl), (th, tl)):
            moved = jnp.dot(part, square[2 + core], preferred_element_type=F32)
            ref[g] = moved.astype(BF16)
            flat[g] = moved.T.astype(BF16)

    def apply(k, inverse=None):
        for part in range(2):
            for own, out in ((own_h, g_h), (own_l, g_l)):
                out[part] = jnp.dot(
                    oh[...], own[part], preferred_element_type=F32
                ).astype(BF16).reshape(8, 32, 256)

        def group(step, carry):
            g = step
            if k == 0:
                g = crossed(lax.div(me, 4), step, 3)
                make_ready(g)
            left = tuple(
                jnp.concatenate([ref[0, g], ref[1, g]], axis=0) for ref in (g_h, g_l)
            )
            weights = (wh[g], wl[g])
            seen = triple_dot(left, (th[g], tl[g]), NN)
            weight = wm[g]
            if inverse is not None:
                weight = weight * inverse * inverse
            seen = seen * jnp.concatenate([weight, weight], axis=0)
            high, low = halves(triple_dot(halves(seen), weights, NN))
            for ref, value in ((h_h, high), (h_l, low)):
                ref[0, g] = value[:32]
                ref[1, g] = value[32:]
            return carry

        lax.fori_loop(0, 8, group, 0, unroll=1 if k == 0 else 8)
        for at in range(0, 8, 4):
            for part in range(2):
                grid[k, part, at : at + 4] = move(
                    oht[at * 64 : at * 64 + 256, :],
                    (h_h[part].reshape(256, 256), h_l[part].reshape(256, 256)),
                ).reshape(4, 64, 256)
            if k < 2:
                for a in range(at, at + 4):
                    partner_copy(k, a, core, partner).start()
        if k == 2:
            for its_core in range(2):

                @pl.when(core == 1 - its_core)
                def _():
                    for a in NEEDED[its_core]:
                        partner_copy(k, a, core, partner).start()

        pack_ring(k)
        ring_copy(k).start()

    def close_edge(k):
        ring_copy(k).wait_recv()
        unpack_ring(k)

        @pl.when(jnp.logical_or(first_edge, last_edge))
        def _():
            came[k + 1, 0, 8 * core] = turned_block(grid[k, 0, 7 * core])
            came[k + 1, 1, 8 * core] = -turned_block(grid[k, 1, 7 * core])

    def combine(k):
        def run(onto, start, last):
            def block(a, total):
                for part in range(2):
                    value = grid[k, part, a] + onto(came[k + 1, part, a], came[k + 1, part, a + 1])
                    value = 0.5 * value
                    keep(a, part, value)
                    if k == 0:
                        total = total + value * value
                return total

            def one(step, total):
                partner_copy(k, step + 1, 1 - core, partner).wait_recv()
                return block(step + start, total)

            partner_copy(k, 0, 1 - core, partner).wait_recv()
            total = lax.fori_loop(0, 7, one, jnp.zeros((64, 256), F32))
            close_edge(k)
            return block(last, total)

        return lax.cond(
            core == 0, lambda: run(onto_first, 1, 0), lambda: run(onto_second, 0, 7)
        )

    def two_lanes(value):
        return jnp.concatenate([value, value], axis=1)

    apply(0)
    put_mark(0, spread_sum(combine(0)))
    apply(1)
    combine(1)
    n1 = get_mark(0)
    inverse = two_lanes(1.0 / n1)
    apply(2, inverse)
    for its_core in range(2):

        @pl.when(core == its_core)
        def _():
            for a in NEEDED[its_core]:
                partner_copy(2, a, 1 - core, partner).wait_recv()

    ring_copy(2).wait_recv()
    unpack_ring(2)


    @pl.when(first_edge)
    def _():
        up = raised(came[3, 0, 0]), raised(came[3, 1, 0])
        edge_last[0] = up[0] + raised(turned_block(up[0]))
        edge_last[1] = up[1] - raised(turned_block(up[1]))

    @pl.when(first_edge)
    def _():
        came[3, 0, 0] = turned_block(grid[2, 0, 0])
        came[3, 1, 0] = -turned_block(grid[2, 1, 0])

    def last_sum(j, total):
        a = 2 * core + lax.rem(j, 2) + 4 * lax.div(j, 2)

        @pl.when(core == 0)
        def _():
            for part in range(2):
                value = grid[2, part, a] + onto_first(came[3, part, a], came[3, part, a + 1])
                grid[0, part, a] = value

        @pl.when(core == 1)
        def _():
            for part in range(2):
                value = came[3, part, a] + onto_first(grid[2, part, a - 1], grid[2, part, a])
                grid[0, part, a] = value

        for part in range(2):
            value = grid[0, part, a]
            total = total + value * value
        return total

    partner_sent(0)
    total = 0.5 * lax.fori_loop(0, 4, last_sum, jnp.zeros((64, 256), F32))
    h0_re, h0_im = grid[0, 0, 0], grid[0, 1, 0]
    alone = jnp.logical_and((lanes_of((64, 256)) & 7) == 0, first_edge)
    z_re = jnp.where(alone, 0.5 * (h0_re - edge_last[1]), h0_re)
    z_im = jnp.where(alone, 0.5 * (h0_im + edge_last[0]), h0_im)

    @pl.when(first_edge)
    def _():
        grid[0, 0, 0] = z_re
        grid[0, 1, 0] = z_im


    def backward(i, carry):
        at = pl.multiple_of(i * 8, 8)
        held = jnp.concatenate(
            [grid[0, part, block(i, half)] for part in range(2) for half in range(2)], axis=0
        )
        u_ref[...] = triple_dot(halves(held.T), (cih[...], cil[...]), NN)
        items = []
        for k in range(n):
            re = u_ref[k * 8 : k * 8 + 8, :128]
            im = u_ref[k * 8 : k * 8 + 8, 128:]
            items.append(turn(re, im, tc[k : k + 1, :], -ts[k : k + 1, :]))
        items = fft_list(items, 1.0)
        for d in range(n):
            send2[d, pl.ds(at, 8), :] = items[d][0]
            send2[d, pl.ds(at + 16, 8), :] = items[d][1]
        return carry

    lax.fori_loop(0, 2, backward, 0, unroll=2)
    recv2[chip * 2 + core] = send2[me]
    start_all(second_to)
    change = z_re * z_re + z_im * z_im - 0.5 * (h0_re * h0_re + h0_im * h0_im)
    third = spread_sum(total + jnp.where(alone, change, 0.0))

    def second_sum(i, sums):
        at = pl.ds(pl.multiple_of(i * 64, 64), 64)
        for part in range(2):
            value = own_h[part, at, :].astype(F32) + own_l[part, at, :].astype(F32)
            value = value * inverse
            sums = sums + value * value
        return sums

    second = spread_sum(lax.fori_loop(0, 8, second_sum, jnp.zeros((64, 256), F32)))
    put_mark(1, jnp.where(lanes_of((1, 128)) < 64, second, third))
    all_extras.wait_send()
    all_weights.wait_send()
    all_first.wait_send()
    all_marks(0).wait_send()
    for half in range(2):
        half_copy(half, core, partner).wait_send()

    @pl.when(core == 0)
    def _():
        edge_copy.wait_send()

    partner_sent(1)
    for its_core in range(2):

        @pl.when(core == 1 - its_core)
        def _():
            for a in NEEDED[its_core]:
                partner_copy(2, a, core, partner).wait_send()

    for k in range(3):
        ring_copy(k).wait_send()
    all_second.wait_recv()

    def back_chunk(i, carry):
        at = pl.multiple_of(i * 8, 8)
        its_core = lax.div(i, 2)
        to = pl.multiple_of(lax.rem(i, 2) * 8, 8)
        items = [
            (recv2[o * 2 + its_core, pl.ds(to, 8), :], recv2[o * 2 + its_core, pl.ds(to + 16, 8), :])
            for o in range(n // 2)
        ]
        row = lax.broadcasted_iota(jnp.int32, (8, 128), 0) + at
        lane = lanes_of((8, 128))
        extra = jnp.where(jnp.logical_and(row == 0, lane < 64), items[0][1], 0.0)
        even = fft_list(items, 1.0)
        odd = []
        for o, (re, im) in enumerate(items):
            angle = 2.0 * math.pi * o / n
            odd.append((re, im) if o == 0 else turn(re, im, math.cos(angle), math.sin(angle)))
        odd = fft_list(odd, 1.0)
        items = []
        for k in range(n // 2):
            items.append((even[k][0] + extra, even[k][1]))
            items.append((odd[k][0] - extra, odd[k][1]))
        items = [
            turn(*items[q], rtc[q, pl.ds(at, 8), :], -rts[q, pl.ds(at, 8), :]) for q in range(n)
        ]
        for pair in range(n // 2):
            lanes = slice(pair * 128, (pair + 1) * 128)
            for part in range(2):
                x0, x1 = swap_halves(items[2 * pair][part], items[2 * pair + 1][part])
                b_ref[pl.ds(at + part * 64, 8), lanes] = x0
                b_ref[pl.ds(at + part * 64 + rows, 8), lanes] = x1
        return carry

    lax.fori_loop(0, 4, back_chunk, 0, unroll=2)
    both = get_mark(1)
    n2, n3 = jnp.full((1, 128), both[0, 0], F32), jnp.full((1, 128), both[0, 64], F32)
    factor = float(image.shape[1]) / n3
    factor = jnp.concatenate([factor] * 4, axis=1)
    for at in range(0, n, 8):
        lanes = slice(at * 64, at * 64 + 512)
        part = triple_dot((row_i[0], row_i[1]), halves(b_ref[:, lanes]), NN) * factor
        for q in range(8):
            tall_ref[pl.ds(at + q, 64, stride=n), :] = part[:, q * 64 : q * 64 + 64]
    for lane in range(0, image.shape[1], 128):
        y_ref[:, lane : lane + 128] = tall_ref[lane : lane + 128, :].T
    third = n3 * n1 / n2
    for at, value in enumerate((n1, n2, third)):
        norm_ref[at] = value[0, 0]
    all_second.wait_send()
    all_marks(1).wait_send()


def tables(n, row_count, length):
    half = row_count // 2
    scale = 1.0 / math.sqrt(length)
    local = np.arange(row_count)
    angle = -2.0 * np.pi * np.outer(local, local) / row_count
    c, s = np.cos(angle) * scale, np.sin(angle) * scale
    two = np.eye(2)
    col_f = np.block([[np.kron(two, c), np.kron(two, -s)], [np.kron(two, s), np.kron(two, c)]])
    col_i = col_f
    row_f = np.concatenate([c, s], axis=0)
    row_i = np.concatenate([c, s], axis=1)
    index = np.arange(n)
    turns = -2.0 * np.pi * np.outer(index, np.tile(local, 2)) / length
    u = np.arange(half)[:, None] + half * (np.arange(2 * row_count)[None, :] // row_count)
    row_turns = -2.0 * np.pi * index[:, None, None] * u[None] / length
    return col_f, col_i, row_f, row_i, turns, row_turns


def fast_device(image0, interp, vis_weight, counts, tile_index):
    n_chan = lax.axis_size("chan")
    n = lax.axis_size("base") * n_chan
    row_count, length = image0.shape
    touch = tile_index.shape[2]
    each = touch // n
    vcap, cells = interp.shape[3:]
    col_f, col_i, row_f, row_i, turns, row_turns = tables(n, row_count, length)
    cfh, cfl = np_halves(col_f)
    rows_f, rows_i = np.stack(np_halves(row_f)), np.stack(np_halves(row_i))
    column_turns = np.stack([np.cos(turns), np.sin(turns)]).astype(np.float32)
    row_turns = np.stack([np.cos(row_turns), np.sin(row_turns)]).astype(np.float32)
    order = np.arange(cells).reshape(TILE_V, TILE_U).T.reshape(-1)
    perm = np.zeros((2, cells, cells), np.float32)
    perm[0, order, np.arange(cells)] = 1.0
    perm[1] = perm[0][:, ::-1]
    perm = perm.astype(jnp.bfloat16)
    square = np.concatenate([np.stack([cfh, cfl]), perm])
    matrices = interp.reshape(n, each * vcap, cells)
    weight = vis_weight.reshape(touch, vcap).T
    count = counts.reshape(1, touch)
    tile = tile_index.reshape(1, touch)

    def dma(*shape):
        return pltpu.SemaphoreType.DMA(shape)

    message = (n, 32, 128)
    wide = (8, 64, 256)
    image, norms = pl.pallas_call(
        lambda *refs: main_kernel(n, n_chan, *refs),
        out_shape=[
            jax.ShapeDtypeStruct((row_count, length), F32),
            jax.ShapeDtypeStruct((3,), F32),
        ],
        in_specs=[HBM_SPEC] * 10,
        out_specs=[VMEM_SPEC, SMEM_SPEC],
        scratch_shapes=[
            pltpu.VMEM((row_count, length), F32),
            pltpu.VMEM((length, row_count), F32),
            pltpu.VMEM(weight.shape, F32),
            pltpu.VMEM(count.shape, jnp.int32),
            pltpu.VMEM(tile.shape, jnp.int32),
            pltpu.VMEM(row_turns.shape, F32),
            pltpu.VMEM(square.shape, BF16),
            pltpu.VMEM(column_turns.shape, F32),
            pltpu.VMEM(rows_f.shape, BF16),
            pltpu.VMEM(rows_i.shape, BF16),
            pltpu.VMEM((n, 8, 128), F32),
            pltpu.VMEM((2 * row_count, length), F32),
            pltpu.VMEM(message, F32),
            pltpu.VMEM(message, F32),
            pltpu.VMEM(message, F32),
            pltpu.VMEM(message, F32),
            pltpu.VMEM((n, each * vcap, cells), F32),
            pltpu.VMEM((n, 8, 128), F32),
            pltpu.VMEM((2, 1, 128), F32),
            pltpu.VMEM((2, n, 1, 128), F32),
            pltpu.VMEM((8, cells, cells), BF16),
            pltpu.VMEM((8, cells, cells), BF16),
            pltpu.VMEM((8, cells, cells), BF16),
            pltpu.VMEM((8, cells, cells), BF16),
            pltpu.VMEM((8, 32, cells), F32),
            pltpu.VMEM((touch, 512), BF16),
            pltpu.VMEM((512, touch), BF16),
            pltpu.VMEM((2, 512, cells), BF16),
            pltpu.VMEM((2, 512, cells), BF16),
            pltpu.VMEM((2, 8, 32, cells), BF16),
            pltpu.VMEM((2, 8, 32, cells), BF16),
            pltpu.VMEM((2, 8, 32, cells), BF16),
            pltpu.VMEM((2, 8, 32, cells), BF16),
            pltpu.VMEM((3, 2, 8, 64, cells), F32),
            pltpu.VMEM((4, 2, 9, 64, cells), F32),
            pltpu.VMEM((2, 64, cells), F32),
            pltpu.VMEM((2, 64, cells), F32),
            pltpu.VMEM((3, 16, cells), F32),
            pltpu.VMEM((3, 16, cells), F32),
            pltpu.VMEM((256, 256), F32),
            dma(1),
            dma(n),
            dma(2),
            dma(2),
            dma(2),
            dma(4, 2),
            dma(4, 8, 2),
            dma(4, 2),
            dma(10),
        ],
        compiler_params=pltpu.CompilerParams(
            has_side_effects=True, collective_id=0, vmem_limit_bytes=67043328
        ),
    )(
        image0,
        matrices,
        weight,
        count,
        tile,
        jnp.asarray(row_turns),
        jnp.asarray(square),
        column_turns,
        rows_f,
        rows_i,
    )
    return image, norms


def per_device(image0, interp, vis_weight, counts, tile_index):
    n = lax.axis_size("base") * lax.axis_size("chan")
    row_count, length = image0.shape
    vcap, cells = interp.shape[3:]
    touch = tile_index.shape[2]
    fits = (n, row_count, length // row_count) == (TILE_U, 64, TILE_U)
    if fits and (vcap, cells, touch % 256) == (8, 256, 0) and touch // n == 8:
        return fast_device(image0, interp, vis_weight, counts, tile_index)
    return general_device(image0, interp, vis_weight, counts, tile_index)


def solution(mesh):
    placed = (
        P(("base", "chan"), None),
        P("base", "chan", None, None, None),
        P("base", "chan", None, None),
        P("base", "chan", None),
        P("base", "chan", None),
    )
    return jax.shard_map(
        per_device,
        mesh=mesh,
        in_specs=placed,
        out_specs=(P(("base", "chan"), None), P()),
        check_vma=False,
    )
```

```python
import math

import jax
import jax.numpy as jnp
import numpy as np
from jax import lax
from jax.experimental import pallas as pl
from jax.experimental.pallas import tpu as pltpu
from jax.sharding import PartitionSpec as P

TILE_V = 8
TILE_U = 32
ITERS = 3


PRECISION_LEVEL = lax.Precision.HIGHEST


def split_length(length):
    outer_len = 2 ** ((length.bit_length() - 1) // 2)
    return (outer_len, length // outer_len)


def angle_table(count_a, count_b, modulus, sign):
    left = jnp.arange(count_a, dtype=jnp.int32)[:, None]
    right = jnp.arange(count_b, dtype=jnp.int32)[None, :]
    angle = sign * 2.0 * math.pi / modulus * (left * right % modulus).astype(jnp.float32)
    return (jnp.cos(angle), jnp.sin(angle))


def transform_rows(real_part, imag_part, sign):
    row_count, length = real_part.shape
    outer_len, inner_len = split_length(length)
    cos_q, sin_q = angle_table(inner_len, inner_len, inner_len, sign)
    cos_t, sin_t = angle_table(inner_len, outer_len, length, sign)
    cos_p, sin_p = angle_table(outer_len, outer_len, outer_len, sign)
    real_in = real_part.reshape(row_count, inner_len, outer_len)
    first_re = jnp.einsum("kq,rqp->rkp", cos_q, real_in, precision=PRECISION_LEVEL)
    first_im = jnp.einsum("kq,rqp->rkp", sin_q, real_in, precision=PRECISION_LEVEL)
    if imag_part is not None:
        imag_in = imag_part.reshape(row_count, inner_len, outer_len)
        first_re = first_re - jnp.einsum("kq,rqp->rkp", sin_q, imag_in, precision=PRECISION_LEVEL)
        first_im = first_im + jnp.einsum("kq,rqp->rkp", cos_q, imag_in, precision=PRECISION_LEVEL)
    turned_re = first_re * cos_t - first_im * sin_t
    turned_im = first_re * sin_t + first_im * cos_t
    last_re = jnp.einsum("jp,rkp->rjk", cos_p, turned_re, precision=PRECISION_LEVEL) - jnp.einsum(
        "jp,rkp->rjk", sin_p, turned_im, precision=PRECISION_LEVEL
    )
    last_im = jnp.einsum("jp,rkp->rjk", cos_p, turned_im, precision=PRECISION_LEVEL) + jnp.einsum(
        "jp,rkp->rjk", sin_p, turned_re, precision=PRECISION_LEVEL
    )
    factor = 1.0 / math.sqrt(length)
    return (
        last_re.reshape(row_count, length) * factor,
        last_im.reshape(row_count, length) * factor,
    )


def transpose_global(real_part, imag_part):
    row_count, length = real_part.shape
    n_base = lax.axis_size("base")
    n_chan = lax.axis_size("chan")
    width = length // (n_base * n_chan)
    moved = (
        lax.all_to_all(
            lax.all_to_all(
                real_part.reshape(1, row_count, n_base, n_chan, width),
                "base",
                split_axis=2,
                concat_axis=0,
                tiled=True,
            ),
            "chan",
            split_axis=3,
            concat_axis=1,
            tiled=True,
        ),
        lax.all_to_all(
            lax.all_to_all(
                imag_part.reshape(1, row_count, n_base, n_chan, width),
                "base",
                split_axis=2,
                concat_axis=0,
                tiled=True,
            ),
            "chan",
            split_axis=3,
            concat_axis=1,
            tiled=True,
        ),
    )
    return (moved[0].reshape(length, width).T, moved[1].reshape(length, width).T)


def to_tiles(plane):
    row_count, length = plane.shape
    shaped = plane.reshape(row_count // TILE_V, TILE_V, length // TILE_U, TILE_U)
    return shaped.transpose(0, 2, 1, 3).reshape(-1, TILE_V * TILE_U)


def from_tiles(tiles, row_count, length):
    shaped = tiles.reshape(row_count // TILE_V, length // TILE_U, TILE_V, TILE_U)
    return shaped.transpose(0, 2, 1, 3).reshape(row_count, length)


def slot_work(sample_weights, masked_weight, sample_values):
    visible_samples = (
        jnp.einsum("gnz,gez->gen", sample_weights, sample_values, precision=PRECISION_LEVEL)
        * masked_weight[:, None, :]
    )
    return jnp.einsum("hbi,hyb->hyi", sample_weights, visible_samples, precision=PRECISION_LEVEL)


def total_squares(image):
    return lax.psum(jnp.sum(image * image), ("base", "chan"))


def general_device(image0, interp, vis_weight, counts, tile_index):
    n_base = lax.axis_size("base")
    n_chan = lax.axis_size("chan")
    row_count, length = image0.shape
    touch = tile_index.shape[2]
    slots_each = touch // (n_base * n_chan)
    vcap = interp.shape[3]
    cells = interp.shape[4]
    tiles_own = row_count // TILE_V * (length // TILE_U)
    live = (jnp.arange(vcap, dtype=jnp.int32)[None, :] < counts.reshape(touch, 1)).astype(
        jnp.float32
    )
    masked_weight = vis_weight.reshape(touch, vcap) * live
    sample_weights = interp.reshape(touch, vcap, cells)
    wanted = lax.all_to_all(
        lax.all_to_all(
            tile_index.reshape(n_base, n_chan, slots_each),
            "base",
            split_axis=0,
            concat_axis=0,
            tiled=True,
        ),
        "chan",
        split_axis=1,
        concat_axis=1,
        tiled=True,
    ).reshape(touch)
    onehot = (jnp.arange(tiles_own, dtype=jnp.int32)[:, None] == wanted[None, :]).astype(
        jnp.float32
    )
    moved = (
        lax.all_to_all(
            lax.all_to_all(
                sample_weights.reshape(n_base, n_chan, slots_each, vcap, cells),
                "base",
                split_axis=0,
                concat_axis=0,
                tiled=True,
            ),
            "chan",
            split_axis=1,
            concat_axis=1,
            tiled=True,
        ),
        lax.all_to_all(
            lax.all_to_all(
                masked_weight.reshape(n_base, n_chan, slots_each, vcap),
                "base",
                split_axis=0,
                concat_axis=0,
                tiled=True,
            ),
            "chan",
            split_axis=1,
            concat_axis=1,
            tiled=True,
        ),
    )
    sample_weights = moved[0].reshape(touch, vcap, cells)
    masked_weight = moved[1].reshape(touch, vcap)
    found = []
    current = image0 / jnp.sqrt(total_squares(image0))
    for iteration in range(ITERS):
        real_part, imag_part = transform_rows(current, None, -1.0)
        real_part, imag_part = transpose_global(real_part, imag_part)
        real_part, imag_part = transform_rows(real_part, imag_part, -1.0)
        tiles = jnp.stack([to_tiles(real_part), to_tiles(imag_part)], axis=1)
        sample_values = jnp.take(tiles, wanted, axis=0)
        gridded_plane = slot_work(sample_weights, masked_weight, sample_values)
        summed = jnp.einsum("ts,skc->tkc", onehot, gridded_plane, precision=PRECISION_LEVEL)
        real_part = from_tiles(summed[:, 0, :], row_count, length)
        imag_part = from_tiles(summed[:, 1, :], row_count, length)
        real_part, imag_part = transform_rows(real_part, imag_part, 1.0)
        real_part, imag_part = transpose_global(real_part, imag_part)
        real_part, imag_part = transform_rows(real_part, imag_part, 1.0)
        norm_value = jnp.sqrt(total_squares(real_part))
        found.append(norm_value)
        current = real_part / norm_value
    return (float(length) * current, jnp.stack(found))


F32 = jnp.float32
BF16 = jnp.bfloat16
VMEM_SPEC = pl.BlockSpec(memory_space=pltpu.VMEM)
SMEM_SPEC = pl.BlockSpec(memory_space=pltpu.SMEM)
BIG = pltpu.CompilerParams(vmem_limit_bytes=48 * 1024 * 1024)


def halves(value):
    high = value.astype(BF16)
    return high, (value - high.astype(F32)).astype(BF16)


def np_halves(table):
    high = np.asarray(table, np.float32).astype(jnp.bfloat16)
    low = (np.asarray(table, np.float64) - high.astype(np.float64)).astype(jnp.bfloat16)
    return high, low


def triple_dot(left, right, dims):
    def one(a, b):
        return lax.dot_general(a, b, (dims, ((), ())), preferred_element_type=F32)

    return one(left[0], right[0]) + (one(left[0], right[1]) + one(left[1], right[0]))


def fft_list(items, sign):
    count = len(items)
    if count == 1:
        return items
    even = fft_list(items[0::2], sign)
    odd = fft_list(items[1::2], sign)
    low, high = [], []
    for k in range(count // 2):
        re, im = odd[k]
        if k == 0:
            t_re, t_im = re, im
        elif 4 * k == count:
            t_re, t_im = (im, -re) if sign < 0 else (-im, re)
        else:
            angle = sign * 2.0 * math.pi * k / count
            c, s = math.cos(angle), math.sin(angle)
            t_re, t_im = re * c - im * s, re * s + im * c
        e_re, e_im = even[k]
        low.append((e_re + t_re, e_im + t_im))
        high.append((e_re - t_re, e_im - t_im))
    return low + high


AHEAD = 4
NEEDED = ((0, 3, 4, 1, 5), (2, 3, 6, 7))
HBM_SPEC = pl.BlockSpec(memory_space=pltpu.HBM)
NT = ((1,), (1,))
NN = ((1,), (0,))


def turn(re, im, c, s):
    return re * c - im * s, re * s + im * c


def swap_halves(x0, x1):
    half = x0.shape[1] // 2
    left = lax.broadcasted_iota(jnp.int32, x0.shape, 1) < half
    return (
        jnp.where(left, x0, pltpu.roll(x1, half, 1)),
        jnp.where(left, pltpu.roll(x0, half, 1), x1),
    )


def move(table, parts, dims=NN):
    def one(part):
        return lax.dot_general(table, part, (dims, ((), ())), preferred_element_type=F32)

    return one(parts[0]) + one(parts[1])


def bit_of(p, bit):
    return lax.rem(lax.div(p, 2**bit), 2)


def walk(z, w):
    odd = lax.rem(w, 2)
    return 4 * w + z + odd * (3 - 2 * z)


def chip_of(p):
    x, y = bit_of(p, 2), bit_of(p, 0)
    return walk(lax.div(p, 8), 3 * x + y - 2 * x * y), bit_of(p, 1)


def device_of(chip, core):
    w, at = lax.div(chip, 4), lax.rem(chip, 4)
    odd = lax.rem(w, 2)
    z = at + odd * (3 - 2 * at)
    x = lax.div(w, 2)
    y = odd + x - 2 * x * odd
    return ((z * 2 + x) * 2 + core) * 2 + y


def crossed(p, step, bits):
    value = p + step
    for bit in range(bits):
        value = value - 2 ** (bit + 1) * bit_of(p, bit) * bit_of(step, bit)
    return value


def turned_block(block):
    rows, lanes = block.shape

    def anti(size):
        total = lax.broadcasted_iota(jnp.int32, (size, size), 0) + lax.broadcasted_iota(
            jnp.int32, (size, size), 1
        )
        return (total == size - 1).astype(F32).astype(BF16)

    half = move(anti(rows), halves(block))
    high, low = halves(half)
    table = anti(lanes)

    def one(part):
        return jnp.dot(part, table, preferred_element_type=F32)

    return one(high) + one(low)


def lanes_of(shape):
    return lax.broadcasted_iota(jnp.int32, shape, 1)


def onto_first(low, high):
    lane = lanes_of((low.shape[0], 128))
    column = lane & 7
    high = [pltpu.roll(high[:, at : at + 128], 9, 1) for at in (0, 128)]
    low = [pltpu.roll(low[:, at : at + 128], 1, 1) for at in (0, 128)]
    left = jnp.where(
        column > 0,
        jnp.where(lane < 8, high[1], high[0]),
        jnp.where(lane < 8, low[1], low[0]),
    )
    right = jnp.where(
        column > 0,
        jnp.where(lane < 8, high[0], high[1]),
        jnp.where(lane < 8, low[0], low[1]),
    )
    left = jnp.where(lane >= 8, left, pltpu.roll(left, 1, 0))
    return jnp.concatenate([left, right], axis=1)


def onto_second(low, high):
    rows = low.shape[0]
    lane = lanes_of((rows, 128))
    column = lane & 7
    low = [pltpu.roll(low[:, at : at + 128], 119, 1) for at in (0, 128)]
    high = [pltpu.roll(high[:, at : at + 128], 127, 1) for at in (0, 128)]
    left = jnp.where(
        column < 7,
        jnp.where(lane >= 120, low[1], low[0]),
        jnp.where(lane >= 120, high[1], high[0]),
    )
    right = jnp.where(
        column < 7,
        jnp.where(lane >= 120, low[0], low[1]),
        jnp.where(lane >= 120, high[0], high[1]),
    )
    right = jnp.where(lane < 120, right, pltpu.roll(right, rows - 1, 0))
    return jnp.concatenate([left, right], axis=1)


def main_kernel(
    n,
    n_chan,
    image_hbm,
    w_hbm,
    weight_hbm,
    count_hbm,
    tile_hbm,
    turns_hbm,
    square_hbm,
    tct_hbm,
    row_f_hbm,
    row_i_hbm,
    y_ref,
    norm_ref,
    image,
    tall_ref,
    weight_ref,
    count_ref,
    tile_ref,
    turns,
    square,
    tct,
    row_f,
    row_i,
    x_ref,
    b_ref,
    send1,
    recv1,
    send2,
    recv2,
    recv_w,
    recv_x,
    mark_send,
    mark_recv,
    wh,
    wl,
    th,
    tl,
    wm,
    oh,
    oht,
    own_h,
    own_l,
    g_h,
    g_l,
    h_h,
    h_l,
    grid,
    came,
    edge_send,
    edge_last,
    ring_send,
    ring_came,
    u_ref,
    w_send,
    w_recv,
    x_sem,
    d1_sem,
    d2_sem,
    m_sem,
    core_sem,
    ring_sem,
    own_sem,
):
    base, chan = lax.axis_index("base"), lax.axis_index("chan")
    me = base * n_chan + chan
    chip, core = chip_of(me)
    chips = n // 2
    rows = 32
    partner = device_of(chip, 1 - core)
    around = device_of(lax.rem(chip + chips + 2 * core - 1, chips), 1 - core)
    first_edge = jnp.logical_and(core == 0, chip == 0)
    last_edge = jnp.logical_and(core == 1, chip == chips - 1)

    def place(p):
        return (lax.div(p, n_chan), lax.rem(p, n_chan))

    def remote(src, dst, sems, out_index, in_index, peer):
        return pltpu.make_async_remote_copy(
            src_ref=src,
            dst_ref=dst,
            send_sem=sems.at[out_index],
            recv_sem=sems.at[in_index],
            device_id=place(peer),
            device_id_type=pl.DeviceIdType.MESH,
        )

    def block_of(p):
        its_chip, its_core = chip_of(p)
        return its_chip + its_core * (n - 1 - 2 * its_chip)

    def weights_to(p, arrives):
        return pltpu.make_async_remote_copy(
            src_ref=w_hbm.at[block_of(p)],
            dst_ref=recv_w.at[arrives],
            send_sem=w_send.at[0],
            recv_sem=w_recv.at[arrives],
            device_id=place(p),
            device_id_type=pl.DeviceIdType.MESH,
        )

    def extras_to(p, arrives):
        return remote(x_ref.at[block_of(p)], recv_x.at[arrives], x_sem, 0, 1, p)

    def first_to(p, arrives):
        its_chip, its_core = chip_of(p)
        return remote(send1.at[its_chip * 2 + its_core], recv1.at[arrives], d1_sem, 0, 1, p)

    def second_to(p, arrives):
        its_chip, its_core = chip_of(arrives)
        return remote(send2.at[p], recv2.at[its_chip * 2 + its_core], d2_sem, 0, 1, p)

    def mark_to(k):
        return lambda p, arrives: remote(
            mark_send.at[k], mark_recv.at[k, arrives], m_sem, (k, 0), (k, 1), p
        )

    def start_all(make, low=1, high=n):
        def body(step, carry):
            make(crossed(me, step, 5), me).start()
            return carry

        lax.fori_loop(low, high, body, 0)

    others = pl.ds(0, n - 1)

    def all_of(sent, landed, sems, out_index, in_index):
        return remote(sent.at[others], landed.at[others], sems, out_index, in_index, partner)

    all_weights = pltpu.make_async_remote_copy(
        src_ref=w_hbm.at[others],
        dst_ref=recv_w.at[others],
        send_sem=w_send.at[0],
        recv_sem=w_recv.at[0],
        device_id=place(partner),
        device_id_type=pl.DeviceIdType.MESH,
    )
    all_extras = all_of(x_ref, recv_x, x_sem, 0, 1)
    all_first = all_of(send1, recv1, d1_sem, 0, 1)
    all_second = all_of(send2, recv2, d2_sem, 0, 1)

    def all_marks(k):
        return all_of(mark_recv.at[k], mark_recv.at[k], m_sem, (k, 0), (k, 1))

    def put_mark(k, total):
        mark_send[k] = total
        mark_recv[k, me] = total

        def body(step, carry):
            mark_to(k)(lax.rem(me + step, n), me).start()
            return carry

        lax.fori_loop(1, n, body, 0)

    def get_mark(k):
        all_marks(k).wait_recv()
        return jnp.sqrt(jnp.sum(mark_recv[k], axis=0))

    def spread_sum(value):
        return jnp.full((1, 128), jnp.sum(value), F32)

    own_w = pltpu.make_async_copy(w_hbm.at[block_of(me)], recv_w.at[me], own_sem.at[0])
    loads = [
        pltpu.make_async_copy(src, dst, own_sem.at[1 + at])
        for at, (src, dst) in enumerate(
            (
                (image_hbm, image),
                (row_f_hbm, row_f),
                (turns_hbm, turns),
                (weight_hbm, weight_ref),
                (count_hbm, count_ref),
                (tile_hbm, tile_ref),
                (square_hbm, square),
                (tct_hbm, tct),
                (row_i_hbm, row_i),
            )
        )
    ]
    for load in loads:
        load.start()
    own_w.start()
    barrier = pltpu.get_barrier_semaphore()

    def greet(step, carry):
        peer = lax.rem(me + step, n)
        pl.semaphore_signal(
            barrier, inc=1, device_id=place(peer), device_id_type=pl.DeviceIdType.MESH
        )
        return carry

    lax.fori_loop(1, n, greet, 0)
    rtc, rts = turns.at[0], turns.at[1]
    tc, ts = tct.at[0], tct.at[1]
    cfh, cfl = square.at[0], square.at[1]
    cih, cil = cfh, cfl

    loads[0].wait()
    loads[1].wait()
    total = jnp.zeros((8, 128), F32)
    for lane in range(0, image.shape[1], 128):
        part = image[:, lane : lane + 128]
        tall_ref[lane : lane + 128, :] = part.T
        square_of = part * part
        for row in range(0, 64, 8):
            total = total + square_of[row : row + 8]
    for at in range(0, n, 8):
        part = jnp.concatenate(
            [tall_ref[pl.ds(at + q, 64, stride=n), :] for q in range(8)], axis=1
        )
        b_ref[:, at * 64 : at * 64 + 512] = triple_dot((row_f[0], row_f[1]), halves(part), NN)

    def row_chunk(i, carry):
        at = pl.multiple_of(i * 8, 8)
        items = [[None, None] for _ in range(n)]
        for pair in range(n // 2):
            lanes = slice(pair * 128, (pair + 1) * 128)
            for part in range(2):
                x0 = b_ref[pl.ds(at + part * 64, 8), lanes]
                x1 = b_ref[pl.ds(at + part * 64 + rows, 8), lanes]
                items[2 * pair][part], items[2 * pair + 1][part] = swap_halves(x0, x1)
        items = [
            turn(*items[q], tc_q, ts_q)
            for q, (tc_q, ts_q) in enumerate(
                (rtc[q, pl.ds(at, 8), :], rts[q, pl.ds(at, 8), :]) for q in range(n)
            )
        ]
        items = fft_list(items, -1.0)
        row = lax.broadcasted_iota(jnp.int32, (8, 128), 0) + at
        lane = lanes_of((8, 128))
        alone = jnp.logical_and(row == 0, lane < 64)
        items[0] = (items[0][0], jnp.where(alone, items[n // 2][0], items[0][1]))
        its_core = lax.div(i, 2)
        to = pl.multiple_of(lax.rem(i, 2) * 8, 8)
        for o in range(n // 2):
            send1[o * 2 + its_core, pl.ds(to, 8), :] = items[o][0]
            send1[o * 2 + its_core, pl.ds(to + 16, 8), :] = items[o][1]
        return carry

    for load in loads[2:]:
        load.wait()
    vis = lax.broadcasted_iota(jnp.int32, (8, 256), 0)
    live = jnp.where(vis < count_ref[...], weight_ref[...], 0.0)
    tile = jnp.broadcast_to(tile_ref[...].astype(F32), (8, 256))
    squares = jnp.full((8, 256), jnp.sum(total), F32)
    slots = jnp.concatenate([live, tile, squares, jnp.zeros((104, 256), F32)], axis=0).T
    x_ref[...] = slots.reshape(n, 8, 128)
    recv_x[me] = x_ref[block_of(me)]
    lax.fori_loop(0, 4, row_chunk, 0)
    recv1[me] = send1[chip * 2 + core]

    pl.semaphore_wait(barrier, n - 1)
    start_all(first_to)
    start_all(extras_to)
    start_all(weights_to, n // 2, n // 2 + AHEAD)

    all_extras.wait_recv()
    slots = recv_x[...].reshape(256, 128)
    inverse = jnp.full((1, 128), jnp.sum(recv_x[:, 0:1, 16:17]), F32)
    inverse = 1.0 / jnp.sqrt(inverse)
    tall = jnp.broadcast_to(slots[:, 8:9], (256, 256))
    tall = jnp.where(core == 0, tall, 511.0 - tall)
    wide = tall.T
    for at in range(0, 512, 256):
        down = (lax.broadcasted_iota(jnp.int32, (256, 256), 0) + at).astype(F32)
        along = (lanes_of((256, 256)) + at).astype(F32)
        oht[at : at + 256, :] = (wide == down).astype(F32).astype(BF16)
        oh[:, at : at + 256] = (tall == along).astype(F32).astype(BF16)
    spread = lax.broadcasted_iota(jnp.int32, (128, 256), 0) == (lanes_of((128, 256)) & 7)
    spread = spread.astype(F32).astype(BF16)
    high, low = halves(slots)
    rest = (slots - high.astype(F32) - low.astype(F32)).astype(BF16)
    value = jnp.dot(high, spread, preferred_element_type=F32) + (
        jnp.dot(low, spread, preferred_element_type=F32)
        + jnp.dot(rest, spread, preferred_element_type=F32)
    )
    slot = (lax.broadcasted_iota(jnp.int32, (256, 256), 0) & 31)
    wm[...] = jnp.where(slot == lax.shift_right_logical(lanes_of((256, 256)), 3), value, 0.0).reshape(8, 32, 256)

    all_first.wait_recv()

    def block(i, half):
        return 2 * core + i + 4 * half

    def forward(i, carry):
        at = pl.multiple_of(i * 8, 8)
        items = fft_list(
            [
                (
                    recv1[d, pl.ds(at, 8), :] * inverse,
                    recv1[d, pl.ds(at + 16, 8), :] * inverse,
                )
                for d in range(n)
            ],
            -1.0,
        )
        for k in range(n):
            re, im = turn(*items[k], tc[k : k + 1, :], ts[k : k + 1, :])
            u_ref[k * 8 : k * 8 + 8, :128] = re
            u_ref[k * 8 : k * 8 + 8, 128:] = im
        out = triple_dot((cfh[...], cfl[...]), halves(u_ref[...]), NT)
        for part in range(2):
            for half in range(2):
                start = part * 128 + half * 64
                came[0, part, block(i, half)] = out[start : start + 64]
        return carry

    lax.fori_loop(0, 2, forward, 0)

    def raised(block_before):
        return onto_first(block_before, block_before)

    @pl.when(first_edge)
    def _():
        z_re, z_im = came[0, 0, 0], came[0, 1, 0]
        f_re = raised(turned_block(z_re))
        f_im = -raised(turned_block(z_im))
        first = (lanes_of(z_re.shape) & 7) == 0
        came[0, 0, 0] = jnp.where(first, 0.5 * (z_re + f_re), z_re)
        came[0, 1, 0] = jnp.where(first, 0.5 * (z_im + f_im), z_im)
        edge_send[0] = 0.5 * (z_im - f_im)
        edge_send[1] = -0.5 * (z_re - f_re)

    @pl.when(jnp.logical_and(core == 0, chip > 0))
    def _():
        edge_send[0] = came[0, 0, 0]
        edge_send[1] = came[0, 1, 0]

    def half_copy(half, its_core, peer):
        at = pl.ds(2 * its_core + 4 * half, 2)
        return remote(
            came.at[0, :, at], came.at[0, :, at], core_sem, (0, half, 0), (0, half, 1), peer
        )

    for half in range(2):
        half_copy(half, core, partner).start()

    edge_copy = remote(edge_send, came.at[0, :, 8], ring_sem, (0, 0), (0, 1), around)

    @pl.when(core == 0)
    def _():
        edge_copy.start()

    start_all(weights_to, n // 2 + AHEAD, n - 4)
    start_all(weights_to, 1, n // 2)
    start_all(weights_to, n - 4, n)

    def keep(a, part, value):
        high, low = halves(value)
        at = pl.ds(pl.multiple_of(a * 64, 64), 64)
        own_h[part, at, :] = high
        own_l[part, at, :] = low

    for half in range(2):
        half_copy(half, 1 - core, partner).wait_recv()

    @pl.when(core == 0)
    def _():
        def one(a, carry):
            for part in range(2):
                keep(a, part, came[0, part, a])
            return carry

        lax.fori_loop(0, 8, one, 0)

    @pl.when(core == 1)
    def _():
        edge_copy.wait_recv()

        def one(a, carry):
            for part in range(2):
                keep(a, part, onto_second(came[0, part, a], came[0, part, a + 1]))
            return carry

        lax.fori_loop(0, 8, one, 0)

    def partner_copy(k, a, its_core, peer):
        return remote(
            grid.at[k, :, a],
            came.at[k + 1, :, a + its_core],
            core_sem,
            (k + 1, a, 0),
            (k + 1, a, 1),
            peer,
        )

    def partner_sent(k):
        for a in range(8):
            partner_copy(k, a, core, partner).wait_send()

    def ring_copy(k):
        return remote(
            ring_send.at[k], ring_came.at[k], ring_sem, (k + 1, 0), (k + 1, 1), around
        )

    def pack_ring(k):
        lane = lanes_of((16, 256)) & 7
        packed = jnp.zeros((16, 256), F32)
        for part in range(2):
            value = grid[k, part, 7 * core]
            for four in range(4):
                at = 2 * four + part
                turned = pltpu.roll(value[16 * four : 16 * four + 16], core * ((256 - 2 * at) % 256) + at, 1)
                packed = jnp.where(lane == core * (7 - 2 * at) + at, turned, packed)
        ring_send[k] = packed

    def unpack_ring(k):
        packed = ring_came[k]
        for part in range(2):
            for four in range(4):
                at = 2 * four + part
                came[k + 1, part, 8 * core, 16 * four : 16 * four + 16] = pltpu.roll(
                    packed, core * ((256 - 2 * at) % 256) + at, 1
                )

    def make_ready(g):
        def one(j, carry):
            d = 4 * g + j

            @pl.when(d != me)
            def _():
                weights_to(d, d).wait_recv()

            @pl.when(d == me)
            def _():
                own_w.wait()

            return carry

        lax.fori_loop(0, 4, one, 0)
        value = recv_w[pl.ds(4 * g, 4)].reshape(256, 256)
        for part, ref, flat in zip(halves(value), (wh, wl), (th, tl)):
            moved = jnp.dot(part, square[2 + core], preferred_element_type=F32)
            ref[g] = moved.astype(BF16)
            flat[g] = moved.T.astype(BF16)

    def apply(k, inverse=None):
        for part in range(2):
            for own, out in ((own_h, g_h), (own_l, g_l)):
                out[part] = jnp.dot(
                    oh[...], own[part], preferred_element_type=F32
                ).astype(BF16).reshape(8, 32, 256)

        def group(step, carry):
            g = step
            if k == 0:
                g = crossed(lax.div(me, 4), step, 3)
                make_ready(g)
            left = tuple(
                jnp.concatenate([ref[0, g], ref[1, g]], axis=0) for ref in (g_h, g_l)
            )
            weights = (wh[g], wl[g])
            seen = triple_dot(left, (th[g], tl[g]), NN)
            weight = wm[g]
            if inverse is not None:
                weight = weight * inverse * inverse
            seen = seen * jnp.concatenate([weight, weight], axis=0)
            high, low = halves(triple_dot(halves(seen), weights, NN))
            for ref, value in ((h_h, high), (h_l, low)):
                ref[0, g] = value[:32]
                ref[1, g] = value[32:]
            return carry

        lax.fori_loop(0, 8, group, 0, unroll=1 if k == 0 else 8)
        for at in range(0, 8, 4):
            for part in range(2):
                grid[k, part, at : at + 4] = move(
                    oht[at * 64 : at * 64 + 256, :],
                    (h_h[part].reshape(256, 256), h_l[part].reshape(256, 256)),
                ).reshape(4, 64, 256)
            if k < 2:
                for a in range(at, at + 4):
                    partner_copy(k, a, core, partner).start()
        if k == 2:
            for its_core in range(2):

                @pl.when(core == 1 - its_core)
                def _():
                    for a in NEEDED[its_core]:
                        partner_copy(k, a, core, partner).start()

        pack_ring(k)
        ring_copy(k).start()

    def close_edge(k):
        ring_copy(k).wait_recv()
        unpack_ring(k)

        @pl.when(jnp.logical_or(first_edge, last_edge))
        def _():
            came[k + 1, 0, 8 * core] = turned_block(grid[k, 0, 7 * core])
            came[k + 1, 1, 8 * core] = -turned_block(grid[k, 1, 7 * core])

    def combine(k):
        def run(onto, start, last):
            def block(a, total):
                for part in range(2):
                    value = grid[k, part, a] + onto(came[k + 1, part, a], came[k + 1, part, a + 1])
                    value = 0.5 * value
                    keep(a, part, value)
                    if k == 0:
                        total = total + value * value
                return total

            def one(step, total):
                partner_copy(k, step + 1, 1 - core, partner).wait_recv()
                return block(step + start, total)

            partner_copy(k, 0, 1 - core, partner).wait_recv()
            total = lax.fori_loop(0, 7, one, jnp.zeros((64, 256), F32))
            close_edge(k)
            return block(last, total)

        return lax.cond(
            core == 0, lambda: run(onto_first, 1, 0), lambda: run(onto_second, 0, 7)
        )

    def two_lanes(value):
        return jnp.concatenate([value, value], axis=1)

    apply(0)
    put_mark(0, spread_sum(combine(0)))
    apply(1)
    combine(1)
    n1 = get_mark(0)
    inverse = two_lanes(1.0 / n1)
    apply(2, inverse)
    for its_core in range(2):

        @pl.when(core == its_core)
        def _():
            for a in NEEDED[its_core]:
                partner_copy(2, a, 1 - core, partner).wait_recv()

    ring_copy(2).wait_recv()
    unpack_ring(2)


    @pl.when(first_edge)
    def _():
        up = raised(came[3, 0, 0]), raised(came[3, 1, 0])
        edge_last[0] = up[0] + raised(turned_block(up[0]))
        edge_last[1] = up[1] - raised(turned_block(up[1]))

    @pl.when(first_edge)
    def _():
        came[3, 0, 0] = turned_block(grid[2, 0, 0])
        came[3, 1, 0] = -turned_block(grid[2, 1, 0])

    def last_sum(j, total):
        a = 2 * core + lax.rem(j, 2) + 4 * lax.div(j, 2)

        @pl.when(core == 0)
        def _():
            for part in range(2):
                value = grid[2, part, a] + onto_first(came[3, part, a], came[3, part, a + 1])
                grid[0, part, a] = value

        @pl.when(core == 1)
        def _():
            for part in range(2):
                value = came[3, part, a] + onto_first(grid[2, part, a - 1], grid[2, part, a])
                grid[0, part, a] = value

        for part in range(2):
            value = grid[0, part, a]
            total = total + value * value
        return total

    partner_sent(0)
    total = 0.5 * lax.fori_loop(0, 4, last_sum, jnp.zeros((64, 256), F32))
    h0_re, h0_im = grid[0, 0, 0], grid[0, 1, 0]
    alone = jnp.logical_and((lanes_of((64, 256)) & 7) == 0, first_edge)
    z_re = jnp.where(alone, 0.5 * (h0_re - edge_last[1]), h0_re)
    z_im = jnp.where(alone, 0.5 * (h0_im + edge_last[0]), h0_im)

    @pl.when(first_edge)
    def _():
        grid[0, 0, 0] = z_re
        grid[0, 1, 0] = z_im


    def backward(i, carry):
        at = pl.multiple_of(i * 8, 8)
        held = jnp.concatenate(
            [grid[0, part, block(i, half)] for part in range(2) for half in range(2)], axis=0
        )
        u_ref[...] = triple_dot(halves(held.T), (cih[...], cil[...]), NN)
        items = []
        for k in range(n):
            re = u_ref[k * 8 : k * 8 + 8, :128]
            im = u_ref[k * 8 : k * 8 + 8, 128:]
            items.append(turn(re, im, tc[k : k + 1, :], -ts[k : k + 1, :]))
        items = fft_list(items, 1.0)
        for d in range(n):
            send2[d, pl.ds(at, 8), :] = items[d][0]
            send2[d, pl.ds(at + 16, 8), :] = items[d][1]
        return carry

    lax.fori_loop(0, 2, backward, 0, unroll=2)
    recv2[chip * 2 + core] = send2[me]
    start_all(second_to)
    change = z_re * z_re + z_im * z_im - 0.5 * (h0_re * h0_re + h0_im * h0_im)
    third = spread_sum(total + jnp.where(alone, change, 0.0))

    def second_sum(i, sums):
        at = pl.ds(pl.multiple_of(i * 64, 64), 64)
        for part in range(2):
            value = own_h[part, at, :].astype(F32) + own_l[part, at, :].astype(F32)
            value = value * inverse
            sums = sums + value * value
        return sums

    second = spread_sum(lax.fori_loop(0, 8, second_sum, jnp.zeros((64, 256), F32)))
    put_mark(1, jnp.where(lanes_of((1, 128)) < 64, second, third))
    all_extras.wait_send()
    all_weights.wait_send()
    all_first.wait_send()
    all_marks(0).wait_send()
    for half in range(2):
        half_copy(half, core, partner).wait_send()

    @pl.when(core == 0)
    def _():
        edge_copy.wait_send()

    partner_sent(1)
    for its_core in range(2):

        @pl.when(core == 1 - its_core)
        def _():
            for a in NEEDED[its_core]:
                partner_copy(2, a, core, partner).wait_send()

    for k in range(3):
        ring_copy(k).wait_send()
    all_second.wait_recv()

    def back_chunk(i, carry):
        at = pl.multiple_of(i * 8, 8)
        its_core = lax.div(i, 2)
        to = pl.multiple_of(lax.rem(i, 2) * 8, 8)
        items = [
            (recv2[o * 2 + its_core, pl.ds(to, 8), :], recv2[o * 2 + its_core, pl.ds(to + 16, 8), :])
            for o in range(n // 2)
        ]
        row = lax.broadcasted_iota(jnp.int32, (8, 128), 0) + at
        lane = lanes_of((8, 128))
        extra = jnp.where(jnp.logical_and(row == 0, lane < 64), items[0][1], 0.0)
        even = fft_list(items, 1.0)
        odd = []
        for o, (re, im) in enumerate(items):
            angle = 2.0 * math.pi * o / n
            odd.append((re, im) if o == 0 else turn(re, im, math.cos(angle), math.sin(angle)))
        odd = fft_list(odd, 1.0)
        items = []
        for k in range(n // 2):
            items.append((even[k][0] + extra, even[k][1]))
            items.append((odd[k][0] - extra, odd[k][1]))
        items = [
            turn(*items[q], rtc[q, pl.ds(at, 8), :], -rts[q, pl.ds(at, 8), :]) for q in range(n)
        ]
        for pair in range(n // 2):
            lanes = slice(pair * 128, (pair + 1) * 128)
            for part in range(2):
                x0, x1 = swap_halves(items[2 * pair][part], items[2 * pair + 1][part])
                b_ref[pl.ds(at + part * 64, 8), lanes] = x0
                b_ref[pl.ds(at + part * 64 + rows, 8), lanes] = x1
        return carry

    lax.fori_loop(0, 4, back_chunk, 0, unroll=2)
    both = get_mark(1)
    n2, n3 = jnp.full((1, 128), both[0, 0], F32), jnp.full((1, 128), both[0, 64], F32)
    factor = float(image.shape[1]) / n3
    factor = jnp.concatenate([factor] * 4, axis=1)
    for at in range(0, n, 8):
        lanes = slice(at * 64, at * 64 + 512)
        part = triple_dot((row_i[0], row_i[1]), halves(b_ref[:, lanes]), NN) * factor
        for q in range(8):
            tall_ref[pl.ds(at + q, 64, stride=n), :] = part[:, q * 64 : q * 64 + 64]
    for lane in range(0, image.shape[1], 128):
        y_ref[:, lane : lane + 128] = tall_ref[lane : lane + 128, :].T
    third = n3 * n1 / n2
    for at, value in enumerate((n1, n2, third)):
        norm_ref[at] = value[0, 0]
    all_second.wait_send()
    all_marks(1).wait_send()


def tables(n, row_count, length):
    half = row_count // 2
    scale = 1.0 / math.sqrt(length)
    local = np.arange(row_count)
    angle = -2.0 * np.pi * np.outer(local, local) / row_count
    c, s = np.cos(angle) * scale, np.sin(angle) * scale
    two = np.eye(2)
    col_f = np.block([[np.kron(two, c), np.kron(two, -s)], [np.kron(two, s), np.kron(two, c)]])
    col_i = col_f
    row_f = np.concatenate([c, s], axis=0)
    row_i = np.concatenate([c, s], axis=1)
    index = np.arange(n)
    turns = -2.0 * np.pi * np.outer(index, np.tile(local, 2)) / length
    u = np.arange(half)[:, None] + half * (np.arange(2 * row_count)[None, :] // row_count)
    row_turns = -2.0 * np.pi * index[:, None, None] * u[None] / length
    return col_f, col_i, row_f, row_i, turns, row_turns


def fast_device(image0, interp, vis_weight, counts, tile_index):
    n_chan = lax.axis_size("chan")
    n = lax.axis_size("base") * n_chan
    row_count, length = image0.shape
    touch = tile_index.shape[2]
    each = touch // n
    vcap, cells = interp.shape[3:]
    col_f, col_i, row_f, row_i, turns, row_turns = tables(n, row_count, length)
    cfh, cfl = np_halves(col_f)
    rows_f, rows_i = np.stack(np_halves(row_f)), np.stack(np_halves(row_i))
    column_turns = np.stack([np.cos(turns), np.sin(turns)]).astype(np.float32)
    row_turns = np.stack([np.cos(row_turns), np.sin(row_turns)]).astype(np.float32)
    order = np.arange(cells).reshape(TILE_V, TILE_U).T.reshape(-1)
    perm = np.zeros((2, cells, cells), np.float32)
    perm[0, order, np.arange(cells)] = 1.0
    perm[1] = perm[0][:, ::-1]
    perm = perm.astype(jnp.bfloat16)
    square = np.concatenate([np.stack([cfh, cfl]), perm])
    matrices = interp.reshape(n, each * vcap, cells)
    weight = vis_weight.reshape(touch, vcap).T
    count = counts.reshape(1, touch)
    tile = tile_index.reshape(1, touch)

    def dma(*shape):
        return pltpu.SemaphoreType.DMA(shape)

    message = (n, 32, 128)
    wide = (8, 64, 256)
    image, norms = pl.pallas_call(
        lambda *refs: main_kernel(n, n_chan, *refs),
        out_shape=[
            jax.ShapeDtypeStruct((row_count, length), F32),
            jax.ShapeDtypeStruct((3,), F32),
        ],
        in_specs=[HBM_SPEC] * 10,
        out_specs=[VMEM_SPEC, SMEM_SPEC],
        scratch_shapes=[
            pltpu.VMEM((row_count, length), F32),
            pltpu.VMEM((length, row_count), F32),
            pltpu.VMEM(weight.shape, F32),
            pltpu.VMEM(count.shape, jnp.int32),
            pltpu.VMEM(tile.shape, jnp.int32),
            pltpu.VMEM(row_turns.shape, F32),
            pltpu.VMEM(square.shape, BF16),
            pltpu.VMEM(column_turns.shape, F32),
            pltpu.VMEM(rows_f.shape, BF16),
            pltpu.VMEM(rows_i.shape, BF16),
            pltpu.VMEM((n, 8, 128), F32),
            pltpu.VMEM((2 * row_count, length), F32),
            pltpu.VMEM(message, F32),
            pltpu.VMEM(message, F32),
            pltpu.VMEM(message, F32),
            pltpu.VMEM(message, F32),
            pltpu.VMEM((n, each * vcap, cells), F32),
            pltpu.VMEM((n, 8, 128), F32),
            pltpu.VMEM((2, 1, 128), F32),
            pltpu.VMEM((2, n, 1, 128), F32),
            pltpu.VMEM((8, cells, cells), BF16),
            pltpu.VMEM((8, cells, cells), BF16),
            pltpu.VMEM((8, cells, cells), BF16),
            pltpu.VMEM((8, cells, cells), BF16),
            pltpu.VMEM((8, 32, cells), F32),
            pltpu.VMEM((touch, 512), BF16),
            pltpu.VMEM((512, touch), BF16),
            pltpu.VMEM((2, 512, cells), BF16),
            pltpu.VMEM((2, 512, cells), BF16),
            pltpu.VMEM((2, 8, 32, cells), BF16),
            pltpu.VMEM((2, 8, 32, cells), BF16),
            pltpu.VMEM((2, 8, 32, cells), BF16),
            pltpu.VMEM((2, 8, 32, cells), BF16),
            pltpu.VMEM((3, 2, 8, 64, cells), F32),
            pltpu.VMEM((4, 2, 9, 64, cells), F32),
            pltpu.VMEM((2, 64, cells), F32),
            pltpu.VMEM((2, 64, cells), F32),
            pltpu.VMEM((3, 16, cells), F32),
            pltpu.VMEM((3, 16, cells), F32),
            pltpu.VMEM((256, 256), F32),
            dma(1),
            dma(n),
            dma(2),
            dma(2),
            dma(2),
            dma(4, 2),
            dma(4, 8, 2),
            dma(4, 2),
            dma(10),
        ],
        compiler_params=pltpu.CompilerParams(
            has_side_effects=True, collective_id=0, vmem_limit_bytes=67043328
        ),
    )(
        image0,
        matrices,
        weight,
        count,
        tile,
        jnp.asarray(row_turns),
        jnp.asarray(square),
        column_turns,
        rows_f,
        rows_i,
    )
    return image, norms


def per_device(image0, interp, vis_weight, counts, tile_index):
    n = lax.axis_size("base") * lax.axis_size("chan")
    row_count, length = image0.shape
    vcap, cells = interp.shape[3:]
    touch = tile_index.shape[2]
    fits = (n, row_count, length // row_count) == (TILE_U, 64, TILE_U)
    if fits and (vcap, cells, touch % 256) == (8, 256, 0) and touch // n == 8:
        return fast_device(image0, interp, vis_weight, counts, tile_index)
    return general_device(image0, interp, vis_weight, counts, tile_index)


def solution(mesh):
    placed = (
        P(("base", "chan"), None),
        P("base", "chan", None, None, None),
        P("base", "chan", None, None),
        P("base", "chan", None),
        P("base", "chan", None),
    )
    return jax.shard_map(
        per_device,
        mesh=mesh,
        in_specs=placed,
        out_specs=(P(("base", "chan"), None), P()),
        check_vma=False,
    )
```
